16 devices in a mesh: model: 2 (over z), data: 8 (over y, x, core).
Axes of the slice: x: 2, y: 2, z: 2, core: 2. Of those that a mesh axis runs over, the one named last changes fastest.
Arguments:
- local_grads: bfloat16 [8, 384, 65536], P('data', None, 'model')
- master: float32 [384, 65536], P(None, ('model', 'data'))
- moment_one: float32 [384, 65536], P(None, ('model', 'data'))
- moment_two: float32 [384, 65536], P(None, ('model', 'data'))
Outputs:
- output 1: bfloat16 [384, 65536], P(None, 'model')
- output 2: float32 [384, 65536], P(None, ('model', 'data'))
- output 3: float32 [384, 65536], P(None, ('model', 'data'))
- output 4: float32 [384, 65536], P(None, ('model', 'data'))
All inputs are finite; a program needn't handle non-finite values.
Results may differ from the reference program's by a relative error of at most 0.001.
Values are sent between devices in bfloat16 or wider.
A program may use at most 1 GiB of HBM per device.

```python
import jax
import jax.numpy as jnp
from jax import lax

D = 256
LAYERS = 32
DATA = 8
STEP = 4
BLOCKS = 12 * LAYERS
BLOCK_SIZE = D * D
LEARN_RATE = 0.08
BETA_ONE = 0.9
BETA_TWO = 0.999
EPSILON = 1e-6
WEIGHT_DECAY = 0.01
MAX_NORM = 1.0
CORR_ONE = 1.0 - BETA_ONE ** STEP
CORR_TWO = 1.0 - BETA_TWO ** STEP


def tensor_sums(block_values):
    return jnp.stack([block_values[..., 0:3].sum(axis=-1), block_values[..., 3], block_values[..., 4:8].sum(axis=-1), block_values[..., 8:12].sum(axis=-1)], axis=-1)


def spread_tensors(tensor_values):
    lead_shape = tensor_values.shape[:-1]
    pieces = [jnp.broadcast_to(tensor_values[..., tensor_pos:tensor_pos + 1], lead_shape + (block_count,)) for tensor_pos, block_count in enumerate((3, 1, 4, 4))]
    return jnp.concatenate(pieces, axis=-1)


def setup_inputs(seed: int = 0) -> dict:
    key_list = jax.random.split(jax.random.key(seed), 8)
    fan_scale = jnp.concatenate([jnp.full((8,), D ** -0.5, jnp.float32), jnp.full((4,), (4 * D) ** -0.5, jnp.float32)])
    weight_factor = jnp.exp(jax.random.uniform(key_list[0], (LAYERS, 4), jnp.float32, minval=-0.8, maxval=0.8))
    weight_scale = (spread_tensors(weight_factor) * fan_scale).reshape(BLOCKS, 1)
    weight_slope = spread_tensors(jax.random.uniform(key_list[1], (LAYERS, 4), jnp.float32, minval=1.5, maxval=2.5)).reshape(BLOCKS, 1)
    position = jnp.arange(BLOCK_SIZE, dtype=jnp.float32) / BLOCK_SIZE - 0.5
    grad_factor = spread_tensors(jnp.exp(jax.random.uniform(key_list[2], (LAYERS, 4), jnp.float32, minval=-1.0, maxval=1.0))).reshape(BLOCKS, 1)
    grad_sigma = grad_factor * (3.0 * MAX_NORM) / jnp.sqrt(BLOCK_SIZE * jnp.sum(grad_factor * grad_factor))
    unit_scale = grad_sigma / jnp.sqrt(2.0)
    shared = jax.random.normal(key_list[3], (BLOCKS, BLOCK_SIZE), jnp.float32)

    def one_replica(replica):
        replica_noise = jax.random.normal(jax.random.fold_in(key_list[4], replica), (BLOCKS, BLOCK_SIZE), jnp.float32)
        return (unit_scale * (shared + DATA ** 0.5 * replica_noise)).astype(jnp.bfloat16)

    local_grads = lax.map(one_replica, jnp.arange(DATA))
    step_sigma = grad_sigma / 3.0
    master = weight_scale * jnp.exp(weight_slope * position) * jax.random.normal(key_list[5], (BLOCKS, BLOCK_SIZE), jnp.float32)
    moment_one = 0.1 * step_sigma * jax.random.normal(key_list[6], (BLOCKS, BLOCK_SIZE), jnp.float32)
    moment_two = 0.003 * step_sigma * step_sigma * jax.random.uniform(key_list[7], (BLOCKS, BLOCK_SIZE), jnp.float32, minval=0.5, maxval=1.5)
    return {'local_grads': local_grads, 'master': master, 'moment_one': moment_one, 'moment_two': moment_two}


def reference(local_grads, master, moment_one, moment_two):
    grad_mean = jnp.sum(local_grads, axis=0, dtype=jnp.float32) / DATA
    clip_scale = jnp.minimum(1.0, MAX_NORM / jnp.sqrt(jnp.sum(grad_mean * grad_mean)))
    scaled = clip_scale * grad_mean
    new_one = BETA_ONE * moment_one + (1.0 - BETA_ONE) * scaled
    new_two = BETA_TWO * moment_two + (1.0 - BETA_TWO) * scaled * scaled
    direction = (new_one / CORR_ONE) / (jnp.sqrt(new_two / CORR_TWO) + EPSILON) + WEIGHT_DECAY * master
    norm_sq = jnp.stack([jnp.sum(master * master, axis=1), jnp.sum(direction * direction, axis=1)])
    tensor_norms = jnp.sqrt(tensor_sums(norm_sq.reshape(2, LAYERS, 12)))
    block_ratio = spread_tensors(tensor_norms[0] / tensor_norms[1]).reshape(BLOCKS, 1)
    new_master = master - LEARN_RATE * block_ratio * direction
    return new_master.astype(jnp.bfloat16), new_master, new_one, new_two
```

```python
import jax
import jax.numpy as jnp
from jax import lax
from jax.experimental import pallas as pl
from jax.experimental.pallas import tpu as pltpu
from jax.sharding import PartitionSpec as P

STEP = 4
LEARN_RATE = 0.08
BETA_ONE = 0.9
BETA_TWO = 0.999
EPSILON = 1e-6
WEIGHT_DECAY = 0.01
MAX_NORM = 1.0
CORR_ONE = 1.0 - BETA_ONE ** STEP
CORR_TWO = 1.0 - BETA_TWO ** STEP

ROWS = 384
HALF = 192
COLS = 4096
DATA = 8
DEVICES = 16
PIECE = 1024
PIECES = COLS // PIECE

RS_SIZES = (48, 48, 48, 32, 16)
RS_CHUNKS = len(RS_SIZES)
RS_STARTS = tuple(sum(RS_SIZES[:i]) for i in range(RS_CHUNKS))
AG_SIZES = (16,) + (32,) * 11 + (16,)
AG_CHUNKS = len(AG_SIZES)
AG_STARTS = tuple(sum(AG_SIZES[:i]) for i in range(AG_CHUNKS))
NORM_CHUNKS = ((0, 16), (16, 112), (112, 384))
OUT_PARTS = 4

MESH = pl.DeviceIdType.MESH
F32 = jnp.float32
BF16 = jnp.bfloat16


def fold_lanes(values):
    total = values[:, 0:128]
    for group in range(1, values.shape[1] // 128):
        total = total + values[:, group * 128:(group + 1) * 128]
    return total


def tensor_total(tile):
    row = [tile[s:s + 1, :] for s in range(8)]
    first3 = row[0] + row[1] + row[2]
    first4 = first3 + row[3]
    mid3 = row[4] + row[5] + row[6]
    last4 = mid3 + row[7]
    sub = lax.broadcasted_iota(jnp.int32, (8, 128), 0)
    kind = lax.broadcasted_iota(jnp.int32, (8, 128), 1) % 3
    full = lambda value: jnp.broadcast_to(value, (8, 128))
    low = jnp.where(kind == 0, jnp.where(sub == 3, full(row[3]), full(first3)), full(first4))
    high = jnp.where(kind == 1, jnp.where(sub == 7, full(row[7]), full(mid3)), full(last4))
    return jnp.where(sub < 4, low, high)


def first_totals(row):
    lane = lax.broadcasted_iota(jnp.int32, (8, 128), 1)
    sub = lax.broadcasted_iota(jnp.int32, (8, 128), 0)
    tile = jnp.zeros((8, 128), F32)
    for group in range(NORM_CHUNKS[0][1] // 8):
        low, high = ((3, 4), (4, 7), (4, 8))[group % 3]
        part = lambda s: (s >= low).astype(jnp.int32) + (s >= high).astype(jnp.int32)
        same = (lane // 8 == group) & (part(sub) == part(lane % 8))
        total = jnp.sum(jnp.where(same, jnp.broadcast_to(row, (8, 128)), 0.0), axis=1, keepdims=True)
        tile = jnp.where(lane == group, total, tile)
    return tile


def kernel(grad_ref, master_ref, one_ref, two_ref, params, master, one, two, relay, grad, weight_buf, norm_buf, first_buf, sq_buf,
           load_sem, rs_recv, rs_send, hop_recv, hop_send, ex_recv, ex_send, ag_x, ag_y, ag_d, ag_o, ag_send):
    model = lax.axis_index("model")
    me = lax.axis_index("data")
    linear = model * DATA + me
    core = me % 2
    x = (me // 2) % 2
    y = me // 4
    to_core = 1 - 2 * core
    near_x = me + 2 - 4 * x
    near_y = me + 4 - 8 * y
    diag = near_x + 4 - 8 * y
    other = me + to_core
    peer = lambda index: {"model": model, "data": index}
    block = lambda index: pl.ds(pl.multiple_of(index * COLS, COLS), COLS)

    loads = [pltpu.make_async_copy(source, target, load_sem.at[i])
             for i, (source, target) in enumerate(((master_ref, master), (one_ref, one), (two_ref, two)))]

    first = (near_x, near_y)
    second = (near_y, near_x)

    def rows_of(half, chunk):
        return pl.ds(half * HALF + RS_STARTS[chunk], RS_SIZES[chunk])

    barrier = pltpu.get_barrier_semaphore()

    @pl.loop(1, DEVICES)
    def _(offset):
        index = (linear + offset) % DEVICES
        pl.semaphore_signal(barrier, inc=1, device_id={"model": index // DATA, "data": index % DATA}, device_id_type=MESH)

    for chunk in range(RS_CHUNKS):
        for half in range(2):
            rows = rows_of(half, chunk)
            for part, owner in enumerate((me, second[half])):
                pltpu.make_async_copy(grad_ref.at[0, rows, block(owner)], params.at[rows, pl.ds(part * COLS, COLS)], rs_recv.at[half, chunk]).start()
    for load in loads:
        load.start()

    pl.semaphore_wait(barrier, DEVICES - 1)

    def remote(source, target, send, recv, index):
        return pltpu.make_async_remote_copy(src_ref=source, dst_ref=target, send_sem=send, recv_sem=recv,
                                            device_id=peer(index), device_id_type=MESH)

    for chunk in range(RS_CHUNKS):
        for half in range(2):
            rows = rows_of(half, chunk)
            recv = rs_recv.at[half, chunk]
            send = rs_send.at[half]
            for turn in range(2):
                shift = turn * to_core
                for part, owner in enumerate((first[half] + shift, diag + shift)):
                    remote(grad_ref.at[0, rows, block(owner)], params.at[rows, pl.ds((4 + 2 * turn + part) * COLS, COLS)], send, recv, first[half] + shift).start()
            for part, owner in enumerate((other, second[half] + to_core)):
                remote(grad_ref.at[0, rows, block(owner)], params.at[rows, pl.ds((2 + part) * COLS, COLS)], send, recv, other).start()

    for load in loads:
        load.wait()

    lane = lax.broadcasted_iota(jnp.int32, (8, 128), 1)
    sub = lax.broadcasted_iota(jnp.int32, (8, 128), 0)

    def weight_rows(group, tile):
        rows = pl.ds(pl.multiple_of(group * 8, 8), 8)

        def piece(i, total):
            value = master[rows, pl.ds(pl.multiple_of(i * PIECE, PIECE), PIECE)]
            return total + fold_lanes(value * value)

        total = lax.fori_loop(0, PIECES, piece, jnp.zeros((8, 128), F32))
        return jnp.where(lane == group, jnp.sum(total, axis=1, keepdims=True), tile)

    weight_buf[linear] = lax.fori_loop(0, ROWS // 8, weight_rows, jnp.zeros((8, 128), F32))

    def exchange(buf, number):
        @pl.loop(1, DEVICES)
        def _(offset):
            index = (linear + offset) % DEVICES
            pltpu.make_async_remote_copy(src_ref=buf.at[linear], dst_ref=buf.at[linear], send_sem=ex_send.at[number], recv_sem=ex_recv.at[number],
                                         device_id={"model": index // DATA, "data": index % DATA}, device_id_type=MESH).start()

    def exchange_wait(buf, sem):
        others = buf.at[pl.ds(0, DEVICES - 1)]
        pltpu.make_async_copy(others, others, sem).wait()

    def gathered(buf):
        total = buf[0]
        for index in range(1, DEVICES):
            total = total + buf[index]
        return total

    EX_WEIGHT, EX_GRAD, EX_FIRST = range(3)

    def four(rows, cols_at, part):
        total = params[rows, pl.ds(pl.multiple_of(part * COLS + cols_at, PIECE), PIECE)].astype(F32)
        for source in range(1, 4):
            total = total + params[rows, pl.ds(pl.multiple_of((2 * source + part) * COLS + cols_at, PIECE), PIECE)].astype(F32)
        return total

    def hop(half, chunk):
        rows = rows_of(half, chunk)
        return remote(relay.at[rows], grad.at[rows], hop_send.at[half], hop_recv.at[half, chunk], second[half])

    for chunk in range(RS_CHUNKS):
        for half in range(2):
            rows = rows_of(half, chunk)
            whole = params.at[rows]
            pltpu.make_async_copy(whole, whole, rs_recv.at[half, chunk]).wait()

            @pl.loop(0, RS_SIZES[chunk] // 16 * PIECES)
            def _(step):
                tile_rows = pl.ds(pl.multiple_of(half * HALF + RS_STARTS[chunk] + step // PIECES * 16, 16), 16)
                cols_at = step % PIECES * PIECE
                relay[tile_rows, pl.ds(pl.multiple_of(cols_at, PIECE), PIECE)] = four(tile_rows, cols_at, 1)

            hop(half, chunk).start()
        if chunk == 0:
            exchange(weight_buf, EX_WEIGHT)

    square = jnp.zeros((8, 128), F32)
    for chunk in range(RS_CHUNKS):
        for half in range(2):
            hop(half, chunk).wait_recv()

            def finish(step, total):
                tile_rows = pl.ds(pl.multiple_of(half * HALF + RS_STARTS[chunk] + step // PIECES * 16, 16), 16)
                cols_at = step % PIECES * PIECE
                cols = pl.ds(pl.multiple_of(cols_at, PIECE), PIECE)
                value = (grad[tile_rows, cols] + four(tile_rows, cols_at, 0)) * (1.0 / DATA)
                grad[tile_rows, cols] = value
                folded = fold_lanes(value * value)
                return total + (folded[0:8] + folded[8:16])

            square = lax.fori_loop(0, RS_SIZES[chunk] // 16 * PIECES, finish, square)

    norm_buf[linear] = jnp.sum(square, axis=0, keepdims=True)
    exchange_wait(weight_buf, ex_recv.at[EX_WEIGHT])
    weight_norm = jnp.sqrt(tensor_total(gathered(weight_buf)))
    exchange(norm_buf, EX_GRAD)
    for half in range(2):
        rows = pl.ds(half * HALF, HALF)
        pltpu.make_async_copy(relay.at[rows], relay.at[rows], hop_send.at[half]).wait()
    exchange_wait(norm_buf, ex_recv.at[EX_GRAD])
    grad_norm = jnp.sqrt(jnp.sum(gathered(norm_buf), axis=1, keepdims=True))
    clip = jnp.minimum(1.0, MAX_NORM / grad_norm)

    def adam_row_sums(group):
        rows = pl.ds(pl.multiple_of(group * 8, 8), 8)

        def piece(i, total):
            cols = pl.ds(pl.multiple_of(i * PIECE, PIECE), PIECE)
            scaled = grad[rows, cols] * clip
            new_one = BETA_ONE * one[rows, cols] + (1.0 - BETA_ONE) * scaled
            new_two = BETA_TWO * two[rows, cols] + (1.0 - BETA_TWO) * (scaled * scaled)
            one[rows, cols] = new_one
            two[rows, cols] = new_two
            direction = (new_one * (1.0 / CORR_ONE)) / (jnp.sqrt(new_two * (1.0 / CORR_TWO)) + EPSILON) + WEIGHT_DECAY * master[rows, cols]
            relay[rows, cols] = direction
            return total + fold_lanes(direction * direction)

        total = lax.fori_loop(0, PIECES, piece, jnp.zeros((8, 128), F32))
        return jnp.sum(total, axis=1, keepdims=True)

    def adam_rows(group, tile):
        return jnp.where(lane == group, adam_row_sums(group), tile)

    def adam_first(group, tile):
        return jnp.where(lane == 8 * group + sub, adam_row_sums(group), tile)

    def step_rates(number):
        if number == 0:
            exchange_wait(first_buf, ex_recv.at[EX_FIRST])
            total = first_totals(gathered(first_buf))
        else:
            exchange_wait(sq_buf.at[number - 1], ex_recv.at[EX_FIRST + number])
            total = tensor_total(gathered(sq_buf.at[number - 1]))
        return weight_norm / jnp.sqrt(total) * LEARN_RATE

    def ag_rows(chunk):
        return pl.ds(AG_STARTS[chunk], AG_SIZES[chunk])

    def update(number, rates):
        start, stop = NORM_CHUNKS[number]
        for chunk in range(AG_CHUNKS):
            if not start <= AG_STARTS[chunk] < stop:
                continue

            @pl.loop(0, AG_SIZES[chunk] // 16)
            def _(tile):
                group = AG_STARTS[chunk] // 8 + 2 * tile
                rows = pl.ds(pl.multiple_of(AG_STARTS[chunk] + tile * 16, 16), 16)
                rate = jnp.concatenate([jnp.sum(jnp.where(lane == group + i, rates, 0.0), axis=1, keepdims=True) for i in range(2)], axis=0)

                @pl.loop(0, PIECES)
                def _(i):
                    cols = pl.ds(pl.multiple_of(i * PIECE, PIECE), PIECE)
                    value = master[rows, cols] - rate * relay[rows, cols]
                    master[rows, cols] = value
                    params[rows, pl.ds(pl.multiple_of(me * COLS + i * PIECE, PIECE), PIECE)] = value.astype(BF16)

            rows = ag_rows(chunk)
            own = params.at[rows, block(me)]
            remote(own, own, ag_send.at[0], ag_x.at[chunk], near_x).start()
            remote(own, own, ag_send.at[1], ag_y.at[chunk], near_y).start()
            remote(own, own, ag_send.at[2], ag_o, other).start()

    groups = [(start // 8, stop // 8) for start, stop in NORM_CHUNKS]
    zero_tile = jnp.zeros((8, 128), F32)
    first_buf[linear] = jnp.sum(lax.fori_loop(*groups[0], adam_first, zero_tile), axis=0, keepdims=True)
    tile = lax.fori_loop(groups[1][0], groups[1][0] + 1, adam_rows, zero_tile)
    exchange(first_buf, EX_FIRST)
    sq_buf[0, linear] = lax.fori_loop(groups[1][0] + 1, groups[1][1], adam_rows, tile)
    tile = lax.fori_loop(groups[2][0], groups[2][0] + 1, adam_rows, zero_tile)
    exchange(sq_buf.at[0], EX_FIRST + 1)
    update(0, step_rates(0))
    update(1, step_rates(1))
    sq_buf[1, linear] = lax.fori_loop(groups[2][0] + 1, groups[2][1], adam_rows, tile)
    exchange(sq_buf.at[1], EX_FIRST + 2)
    update(2, step_rates(2))

    def arrived(sem, source, rows):
        view = params.at[rows, block(source)]
        pltpu.make_async_copy(view, view, sem).wait()
        return view

    for chunk in range(AG_CHUNKS):
        rows = ag_rows(chunk)
        view = arrived(ag_x.at[chunk], near_x, rows)
        if chunk % 2 == 0:
            remote(view, view, ag_send.at[1], ag_d.at[chunk], near_y).start()
        remote(view, view, ag_send.at[2], ag_o, other).start()
        view = arrived(ag_y.at[chunk], near_y, rows)
        if chunk % 2 == 1:
            remote(view, view, ag_send.at[0], ag_d.at[chunk], near_x).start()
        remote(view, view, ag_send.at[2], ag_o, other).start()

    for chunk in range(AG_CHUNKS):
        view = arrived(ag_d.at[chunk], diag, ag_rows(chunk))
        remote(view, view, ag_send.at[2], ag_o, other).start()

    half_cols = params.at[:, pl.ds(0, DATA // 2 * COLS)]
    pltpu.make_async_copy(half_cols, half_cols, ag_o).wait()
    pltpu.make_async_copy(half_cols, half_cols, ag_send.at[2]).wait()
    for direction in range(2):
        for part in (pl.ds(0, ROWS), pl.ds(0, HALF)):
            view = params.at[part, pl.ds(0, COLS)]
            pltpu.make_async_copy(view, view, ag_send.at[direction]).wait()
    for half in range(2):
        view = params.at[pl.ds(0, HALF), pl.ds(0, 6 * COLS)]
        pltpu.make_async_copy(view, view, rs_send.at[half]).wait()
    exchange_wait(weight_buf, ex_send.at[EX_WEIGHT])
    exchange_wait(norm_buf, ex_send.at[EX_GRAD])
    exchange_wait(first_buf, ex_send.at[EX_FIRST])
    for number in range(2):
        exchange_wait(sq_buf.at[number], ex_send.at[EX_FIRST + 1 + number])


def write_out(*refs):
    count = len(refs) // 2
    sem = refs[-1]
    copies = []
    for source, target in zip(refs[:count], refs[count:-1]):
        for part in range(OUT_PARTS):
            rows = pl.ds(part * (ROWS // OUT_PARTS), ROWS // OUT_PARTS)
            copies.append(pltpu.make_async_copy(source.at[rows], target.at[rows], sem.at[len(copies)]))
    for copy in copies:
        copy.start()
    for copy in copies:
        copy.wait()


def solution(mesh):
    def device_step(local_grads, master, moment_one, moment_two):
        any_spec = pl.BlockSpec(memory_space=pl.ANY)
        vmem_spec = pl.BlockSpec(memory_space=pltpu.VMEM)
        state = pltpu.VMEM((ROWS, COLS), F32)
        dma = pltpu.SemaphoreType.DMA
        results = pl.pallas_call(
            kernel,
            name="lamb",
            out_shape=(pltpu.VMEM((ROWS, DATA * COLS), BF16), state, state, state),
            in_specs=[any_spec] * 4,
            out_specs=[vmem_spec] * 4,
            scratch_shapes=[
                pltpu.VMEM((ROWS, COLS), F32),
                pltpu.VMEM((ROWS, COLS), F32),
                pltpu.VMEM((DEVICES, 8, 128), F32),
                pltpu.VMEM((DEVICES, 1, 128), F32),
                pltpu.VMEM((DEVICES, 1, 128), F32),
                pltpu.VMEM((2, DEVICES, 8, 128), F32),
                dma((3,)),
                dma((2, RS_CHUNKS)),
                dma((2,)),
                dma((2, RS_CHUNKS)),
                dma((2,)),
                dma((5,)),
                dma((5,)),
                dma((AG_CHUNKS,)),
                dma((AG_CHUNKS,)),
                dma((AG_CHUNKS,)),
                dma,
                dma((3,)),
            ],
            compiler_params=pltpu.CompilerParams(collective_id=0, has_side_effects=True, vmem_limit_bytes=16 << 20),
        )(local_grads, master, moment_one, moment_two)
        written = []
        for group in (results[:1], results[1:]):
            written += pl.pallas_call(
                write_out,
                name="write_out",
                out_shape=[jax.ShapeDtypeStruct(value.shape, value.dtype) for value in group],
                in_specs=[vmem_spec] * len(group),
                out_specs=[any_spec] * len(group),
                scratch_shapes=[dma((len(group) * OUT_PARTS,))],
                compiler_params=pltpu.CompilerParams(vmem_limit_bytes=1 << 20),
            )(*group)
        return tuple(written)

    state_spec = P(None, ('model', 'data'))
    return jax.shard_map(device_step, mesh=mesh, in_specs=(P('data', None, 'model'), state_spec, state_spec, state_spec), out_specs=(P(None, 'model'), state_spec, state_spec, state_spec), check_vma=False)
```

```python
import jax
import jax.numpy as jnp
from jax import lax
from jax.experimental import pallas as pl
from jax.experimental.pallas import tpu as pltpu
from jax.sharding import PartitionSpec as P

STEP = 4
LEARN_RATE = 0.08
BETA_ONE = 0.9
BETA_TWO = 0.999
EPSILON = 1e-6
WEIGHT_DECAY = 0.01
MAX_NORM = 1.0
CORR_ONE = 1.0 - BETA_ONE ** STEP
CORR_TWO = 1.0 - BETA_TWO ** STEP

ROWS = 384
HALF = 192
COLS = 4096
DATA = 8
DEVICES = 16
PIECE = 1024
PIECES = COLS // PIECE

RS_SIZES = (48, 48, 48, 32, 16)
RS_CHUNKS = len(RS_SIZES)
RS_STARTS = tuple(sum(RS_SIZES[:i]) for i in range(RS_CHUNKS))
AG_SIZES = (16,) + (32,) * 11 + (16,)
AG_CHUNKS = len(AG_SIZES)
AG_STARTS = tuple(sum(AG_SIZES[:i]) for i in range(AG_CHUNKS))
NORM_CHUNKS = ((0, 16), (16, 112), (112, 384))
OUT_PARTS = 4

MESH = pl.DeviceIdType.MESH
F32 = jnp.float32
BF16 = jnp.bfloat16


def fold_lanes(values):
    total = values[:, 0:128]
    for group in range(1, values.shape[1] // 128):
        total = total + values[:, group * 128:(group + 1) * 128]
    return total


def tensor_total(tile):
    row = [tile[s:s + 1, :] for s in range(8)]
    first3 = row[0] + row[1] + row[2]
    first4 = first3 + row[3]
    mid3 = row[4] + row[5] + row[6]
    last4 = mid3 + row[7]
    sub = lax.broadcasted_iota(jnp.int32, (8, 128), 0)
    kind = lax.broadcasted_iota(jnp.int32, (8, 128), 1) % 3
    full = lambda value: jnp.broadcast_to(value, (8, 128))
    low = jnp.where(kind == 0, jnp.where(sub == 3, full(row[3]), full(first3)), full(first4))
    high = jnp.where(kind == 1, jnp.where(sub == 7, full(row[7]), full(mid3)), full(last4))
    return jnp.where(sub < 4, low, high)


def first_totals(row):
    lane = lax.broadcasted_iota(jnp.int32, (8, 128), 1)
    sub = lax.broadcasted_iota(jnp.int32, (8, 128), 0)
    tile = jnp.zeros((8, 128), F32)
    for group in range(NORM_CHUNKS[0][1] // 8):
        low, high = ((3, 4), (4, 7), (4, 8))[group % 3]
        part = lambda s: (s >= low).astype(jnp.int32) + (s >= high).astype(jnp.int32)
        same = (lane // 8 == group) & (part(sub) == part(lane % 8))
        total = jnp.sum(jnp.where(same, jnp.broadcast_to(row, (8, 128)), 0.0), axis=1, keepdims=True)
        tile = jnp.where(lane == group, total, tile)
    return tile


def kernel(grad_ref, master_ref, one_ref, two_ref, params, master, one, two, relay, grad, weight_buf, norm_buf, first_buf, sq_buf,
           load_sem, rs_recv, rs_send, hop_recv, hop_send, ex_recv, ex_send, ag_x, ag_y, ag_d, ag_o, ag_send):
    model = lax.axis_index("model")
    me = lax.axis_index("data")
    linear = model * DATA + me
    core = me % 2
    x = (me // 2) % 2
    y = me // 4
    to_core = 1 - 2 * core
    near_x = me + 2 - 4 * x
    near_y = me + 4 - 8 * y
    diag = near_x + 4 - 8 * y
    other = me + to_core
    peer = lambda index: {"model": model, "data": index}
    block = lambda index: pl.ds(pl.multiple_of(index * COLS, COLS), COLS)

    loads = [pltpu.make_async_copy(source, target, load_sem.at[i])
             for i, (source, target) in enumerate(((master_ref, master), (one_ref, one), (two_ref, two)))]

    first = (near_x, near_y)
    second = (near_y, near_x)

    def rows_of(half, chunk):
        return pl.ds(half * HALF + RS_STARTS[chunk], RS_SIZES[chunk])

    barrier = pltpu.get_barrier_semaphore()

    @pl.loop(1, DEVICES)
    def _(offset):
        index = (linear + offset) % DEVICES
        pl.semaphore_signal(barrier, inc=1, device_id={"model": index // DATA, "data": index % DATA}, device_id_type=MESH)

    pl.semaphore_wait(barrier, DEVICES - 1)

    def remote(source, target, send, recv, index):
        return pltpu.make_async_remote_copy(src_ref=source, dst_ref=target, send_sem=send, recv_sem=recv,
                                            device_id=peer(index), device_id_type=MESH)

    for chunk in range(RS_CHUNKS):
        for half in range(2):
            rows = rows_of(half, chunk)
            recv = rs_recv.at[half, chunk]
            send = rs_send.at[half]
            for turn in range(2):
                shift = turn * to_core
                for part, owner in enumerate((first[half] + shift, diag + shift)):
                    remote(grad_ref.at[0, rows, block(owner)], params.at[rows, pl.ds((4 + 2 * turn + part) * COLS, COLS)], send, recv, first[half] + shift).start()
            for part, owner in enumerate((other, second[half] + to_core)):
                remote(grad_ref.at[0, rows, block(owner)], params.at[rows, pl.ds((2 + part) * COLS, COLS)], send, recv, other).start()

    def load_own(chunk):
        for half in range(2):
            rows = rows_of(half, chunk)
            for part, owner in enumerate((me, second[half])):
                pltpu.make_async_copy(grad_ref.at[0, rows, block(owner)], params.at[rows, pl.ds(part * COLS, COLS)], rs_recv.at[half, chunk]).start()

    load_own(0)

    lane = lax.broadcasted_iota(jnp.int32, (8, 128), 1)
    sub = lax.broadcasted_iota(jnp.int32, (8, 128), 0)

    def weight_rows(group, tile):
        rows = pl.ds(pl.multiple_of(group * 8, 8), 8)

        def piece(i, total):
            value = master[rows, pl.ds(pl.multiple_of(i * PIECE, PIECE), PIECE)]
            return total + fold_lanes(value * value)

        total = lax.fori_loop(0, PIECES, piece, jnp.zeros((8, 128), F32))
        return jnp.where(lane == group, jnp.sum(total, axis=1, keepdims=True), tile)


    def exchange(buf, number):
        @pl.loop(1, DEVICES)
        def _(offset):
            index = (linear + offset) % DEVICES
            pltpu.make_async_remote_copy(src_ref=buf.at[linear], dst_ref=buf.at[linear], send_sem=ex_send.at[number], recv_sem=ex_recv.at[number],
                                         device_id={"model": index // DATA, "data": index % DATA}, device_id_type=MESH).start()

    def exchange_wait(buf, sem):
        others = buf.at[pl.ds(0, DEVICES - 1)]
        pltpu.make_async_copy(others, others, sem).wait()

    def gathered(buf):
        total = buf[0]
        for index in range(1, DEVICES):
            total = total + buf[index]
        return total

    EX_WEIGHT, EX_GRAD, EX_FIRST = range(3)

    def four(rows, cols_at, part):
        total = params[rows, pl.ds(pl.multiple_of(part * COLS + cols_at, PIECE), PIECE)].astype(F32)
        for source in range(1, 4):
            total = total + params[rows, pl.ds(pl.multiple_of((2 * source + part) * COLS + cols_at, PIECE), PIECE)].astype(F32)
        return total

    def hop(half, chunk):
        rows = rows_of(half, chunk)
        return remote(relay.at[rows], grad.at[rows], hop_send.at[half], hop_recv.at[half, chunk], second[half])

    for chunk in range(RS_CHUNKS):
        for half in range(2):
            rows = rows_of(half, chunk)
            whole = params.at[rows]
            pltpu.make_async_copy(whole, whole, rs_recv.at[half, chunk]).wait()

            @pl.loop(0, RS_SIZES[chunk] // 16 * PIECES)
            def _(step):
                tile_rows = pl.ds(pl.multiple_of(half * HALF + RS_STARTS[chunk] + step // PIECES * 16, 16), 16)
                cols_at = step % PIECES * PIECE
                relay[tile_rows, pl.ds(pl.multiple_of(cols_at, PIECE), PIECE)] = four(tile_rows, cols_at, 1)

            hop(half, chunk).start()
        if chunk + 1 < RS_CHUNKS:
            load_own(chunk + 1)
        if chunk < 3:
            loads[chunk].start()
        if chunk == 1:
            loads[0].wait()
            weight_buf[linear] = lax.fori_loop(0, ROWS // 8, weight_rows, jnp.zeros((8, 128), F32))
        if chunk == 2:
            exchange(weight_buf, EX_WEIGHT)

    square = jnp.zeros((8, 128), F32)
    for chunk in range(RS_CHUNKS):
        for half in range(2):
            hop(half, chunk).wait_recv()

            def finish(step, total):
                tile_rows = pl.ds(pl.multiple_of(half * HALF + RS_STARTS[chunk] + step // PIECES * 16, 16), 16)
                cols_at = step % PIECES * PIECE
                cols = pl.ds(pl.multiple_of(cols_at, PIECE), PIECE)
                value = (grad[tile_rows, cols] + four(tile_rows, cols_at, 0)) * (1.0 / DATA)
                grad[tile_rows, cols] = value
                folded = fold_lanes(value * value)
                return total + (folded[0:8] + folded[8:16])

            square = lax.fori_loop(0, RS_SIZES[chunk] // 16 * PIECES, finish, square)

    norm_buf[linear] = jnp.sum(square, axis=0, keepdims=True)
    exchange_wait(weight_buf, ex_recv.at[EX_WEIGHT])
    weight_norm = jnp.sqrt(tensor_total(gathered(weight_buf)))
    exchange(norm_buf, EX_GRAD)
    for half in range(2):
        rows = pl.ds(half * HALF, HALF)
        pltpu.make_async_copy(relay.at[rows], relay.at[rows], hop_send.at[half]).wait()
    for load in loads[1:]:
        load.wait()
    exchange_wait(norm_buf, ex_recv.at[EX_GRAD])
    grad_norm = jnp.sqrt(jnp.sum(gathered(norm_buf), axis=1, keepdims=True))
    clip = jnp.minimum(1.0, MAX_NORM / grad_norm)

    def adam_row_sums(group):
        rows = pl.ds(pl.multiple_of(group * 8, 8), 8)

        def piece(i, total):
            cols = pl.ds(pl.multiple_of(i * PIECE, PIECE), PIECE)
            scaled = grad[rows, cols] * clip
            new_one = BETA_ONE * one[rows, cols] + (1.0 - BETA_ONE) * scaled
            new_two = BETA_TWO * two[rows, cols] + (1.0 - BETA_TWO) * (scaled * scaled)
            one[rows, cols] = new_one
            two[rows, cols] = new_two
            direction = (new_one * (1.0 / CORR_ONE)) / (jnp.sqrt(new_two * (1.0 / CORR_TWO)) + EPSILON) + WEIGHT_DECAY * master[rows, cols]
            relay[rows, cols] = direction
            return total + fold_lanes(direction * direction)

        total = lax.fori_loop(0, PIECES, piece, jnp.zeros((8, 128), F32))
        return jnp.sum(total, axis=1, keepdims=True)

    def adam_rows(group, tile):
        return jnp.where(lane == group, adam_row_sums(group), tile)

    def adam_first(group, tile):
        return jnp.where(lane == 8 * group + sub, adam_row_sums(group), tile)

    def step_rates(number):
        if number == 0:
            exchange_wait(first_buf, ex_recv.at[EX_FIRST])
            total = first_totals(gathered(first_buf))
        else:
            exchange_wait(sq_buf.at[number - 1], ex_recv.at[EX_FIRST + number])
            total = tensor_total(gathered(sq_buf.at[number - 1]))
        return weight_norm / jnp.sqrt(total) * LEARN_RATE

    def ag_rows(chunk):
        return pl.ds(AG_STARTS[chunk], AG_SIZES[chunk])

    def update(number, rates):
        start, stop = NORM_CHUNKS[number]
        for chunk in range(AG_CHUNKS):
            if not start <= AG_STARTS[chunk] < stop:
                continue

            @pl.loop(0, AG_SIZES[chunk] // 16)
            def _(tile):
                group = AG_STARTS[chunk] // 8 + 2 * tile
                rows = pl.ds(pl.multiple_of(AG_STARTS[chunk] + tile * 16, 16), 16)
                rate = jnp.concatenate([jnp.sum(jnp.where(lane == group + i, rates, 0.0), axis=1, keepdims=True) for i in range(2)], axis=0)

                @pl.loop(0, PIECES)
                def _(i):
                    cols = pl.ds(pl.multiple_of(i * PIECE, PIECE), PIECE)
                    value = master[rows, cols] - rate * relay[rows, cols]
                    master[rows, cols] = value
                    params[rows, pl.ds(pl.multiple_of(me * COLS + i * PIECE, PIECE), PIECE)] = value.astype(BF16)

            rows = ag_rows(chunk)
            own = params.at[rows, block(me)]
            remote(own, own, ag_send.at[0], ag_x.at[chunk], near_x).start()
            remote(own, own, ag_send.at[1], ag_y.at[chunk], near_y).start()
            remote(own, own, ag_send.at[2], ag_o, other).start()

    groups = [(start // 8, stop // 8) for start, stop in NORM_CHUNKS]
    zero_tile = jnp.zeros((8, 128), F32)
    first_buf[linear] = jnp.sum(lax.fori_loop(*groups[0], adam_first, zero_tile), axis=0, keepdims=True)
    tile = lax.fori_loop(groups[1][0], groups[1][0] + 1, adam_rows, zero_tile)
    exchange(first_buf, EX_FIRST)
    sq_buf[0, linear] = lax.fori_loop(groups[1][0] + 1, groups[1][1], adam_rows, tile)
    tile = lax.fori_loop(groups[2][0], groups[2][0] + 1, adam_rows, zero_tile)
    exchange(sq_buf.at[0], EX_FIRST + 1)
    update(0, step_rates(0))
    update(1, step_rates(1))
    sq_buf[1, linear] = lax.fori_loop(groups[2][0] + 1, groups[2][1], adam_rows, tile)
    exchange(sq_buf.at[1], EX_FIRST + 2)
    update(2, step_rates(2))

    def arrived(sem, source, rows):
        view = params.at[rows, block(source)]
        pltpu.make_async_copy(view, view, sem).wait()
        return view

    for chunk in range(AG_CHUNKS):
        rows = ag_rows(chunk)
        view = arrived(ag_x.at[chunk], near_x, rows)
        if chunk % 2 == 0:
            remote(view, view, ag_send.at[1], ag_d.at[chunk], near_y).start()
        remote(view, view, ag_send.at[2], ag_o, other).start()
        view = arrived(ag_y.at[chunk], near_y, rows)
        if chunk % 2 == 1:
            remote(view, view, ag_send.at[0], ag_d.at[chunk], near_x).start()
        remote(view, view, ag_send.at[2], ag_o, other).start()

    for chunk in range(AG_CHUNKS):
        view = arrived(ag_d.at[chunk], diag, ag_rows(chunk))
        remote(view, view, ag_send.at[2], ag_o, other).start()

    half_cols = params.at[:, pl.ds(0, DATA // 2 * COLS)]
    pltpu.make_async_copy(half_cols, half_cols, ag_o).wait()
    pltpu.make_async_copy(half_cols, half_cols, ag_send.at[2]).wait()
    for direction in range(2):
        for part in (pl.ds(0, ROWS), pl.ds(0, HALF)):
            view = params.at[part, pl.ds(0, COLS)]
            pltpu.make_async_copy(view, view, ag_send.at[direction]).wait()
    for half in range(2):
        view = params.at[pl.ds(0, HALF), pl.ds(0, 6 * COLS)]
        pltpu.make_async_copy(view, view, rs_send.at[half]).wait()
    exchange_wait(weight_buf, ex_send.at[EX_WEIGHT])
    exchange_wait(norm_buf, ex_send.at[EX_GRAD])
    exchange_wait(first_buf, ex_send.at[EX_FIRST])
    for number in range(2):
        exchange_wait(sq_buf.at[number], ex_send.at[EX_FIRST + 1 + number])


def write_out(*refs):
    count = len(refs) // 2
    sem = refs[-1]
    copies = []
    for source, target in zip(refs[:count], refs[count:-1]):
        for part in range(OUT_PARTS):
            rows = pl.ds(part * (ROWS // OUT_PARTS), ROWS // OUT_PARTS)
            copies.append(pltpu.make_async_copy(source.at[rows], target.at[rows], sem.at[len(copies)]))
    for copy in copies:
        copy.start()
    for copy in copies:
        copy.wait()


def solution(mesh):
    def device_step(local_grads, master, moment_one, moment_two):
        any_spec = pl.BlockSpec(memory_space=pl.ANY)
        vmem_spec = pl.BlockSpec(memory_space=pltpu.VMEM)
        state = pltpu.VMEM((ROWS, COLS), F32)
        dma = pltpu.SemaphoreType.DMA
        results = pl.pallas_call(
            kernel,
            name="lamb",
            out_shape=(pltpu.VMEM((ROWS, DATA * COLS), BF16), state, state, state),
            in_specs=[any_spec] * 4,
            out_specs=[vmem_spec] * 4,
            scratch_shapes=[
                pltpu.VMEM((ROWS, COLS), F32),
                pltpu.VMEM((ROWS, COLS), F32),
                pltpu.VMEM((DEVICES, 8, 128), F32),
                pltpu.VMEM((DEVICES, 1, 128), F32),
                pltpu.VMEM((DEVICES, 1, 128), F32),
                pltpu.VMEM((2, DEVICES, 8, 128), F32),
                dma((3,)),
                dma((2, RS_CHUNKS)),
                dma((2,)),
                dma((2, RS_CHUNKS)),
                dma((2,)),
                dma((5,)),
                dma((5,)),
                dma((AG_CHUNKS,)),
                dma((AG_CHUNKS,)),
                dma((AG_CHUNKS,)),
                dma,
                dma((3,)),
            ],
            compiler_params=pltpu.CompilerParams(collective_id=0, has_side_effects=True, vmem_limit_bytes=16 << 20),
        )(local_grads, master, moment_one, moment_two)
        written = []
        for group in (results[:1], results[1:]):
            written += pl.pallas_call(
                write_out,
                name="write_out",
                out_shape=[jax.ShapeDtypeStruct(value.shape, value.dtype) for value in group],
                in_specs=[vmem_spec] * len(group),
                out_specs=[any_spec] * len(group),
                scratch_shapes=[dma((len(group) * OUT_PARTS,))],
                compiler_params=pltpu.CompilerParams(vmem_limit_bytes=1 << 20),
            )(*group)
        return tuple(written)

    state_spec = P(None, ('model', 'data'))
    return jax.shard_map(device_step, mesh=mesh, in_specs=(P('data', None, 'model'), state_spec, state_spec, state_spec), out_specs=(P(None, 'model'), state_spec, state_spec, state_spec), check_vma=False)
```

```python
import jax
import jax.numpy as jnp
from jax import lax
from jax.experimental import pallas as pl
from jax.experimental.pallas import tpu as pltpu
from jax.sharding import PartitionSpec as P

STEP = 4
LEARN_RATE = 0.08
BETA_ONE = 0.9
BETA_TWO = 0.999
EPSILON = 1e-6
WEIGHT_DECAY = 0.01
MAX_NORM = 1.0
CORR_ONE = 1.0 - BETA_ONE ** STEP
CORR_TWO = 1.0 - BETA_TWO ** STEP

ROWS = 384
HALF = 192
COLS = 4096
DATA = 8
DEVICES = 16
PIECE = 1024
PIECES = COLS // PIECE

RS_SIZES = (48, 48, 48, 32, 16)
RS_CHUNKS = len(RS_SIZES)
RS_STARTS = tuple(sum(RS_SIZES[:i]) for i in range(RS_CHUNKS))
AG_SIZES = (32,) * 10 + (16,) * 4
AG_CHUNKS = len(AG_SIZES)
AG_STARTS = tuple(sum(AG_SIZES[:i]) for i in range(AG_CHUNKS))
NORM_CHUNKS = ((0, 32), (32, 224), (224, 384))
OUT_PARTS = 4

MESH = pl.DeviceIdType.MESH
F32 = jnp.float32
BF16 = jnp.bfloat16


def fold_lanes(values):
    total = values[:, 0:128]
    for group in range(1, values.shape[1] // 128):
        total = total + values[:, group * 128:(group + 1) * 128]
    return total


def tensor_total(tile):
    row = [tile[s:s + 1, :] for s in range(8)]
    first3 = row[0] + row[1] + row[2]
    first4 = first3 + row[3]
    mid3 = row[4] + row[5] + row[6]
    last4 = mid3 + row[7]
    sub = lax.broadcasted_iota(jnp.int32, (8, 128), 0)
    kind = lax.broadcasted_iota(jnp.int32, (8, 128), 1) % 3
    full = lambda value: jnp.broadcast_to(value, (8, 128))
    low = jnp.where(kind == 0, jnp.where(sub == 3, full(row[3]), full(first3)), full(first4))
    high = jnp.where(kind == 1, jnp.where(sub == 7, full(row[7]), full(mid3)), full(last4))
    return jnp.where(sub < 4, low, high)


def first_totals(row):
    lane = lax.broadcasted_iota(jnp.int32, (8, 128), 1)
    sub = lax.broadcasted_iota(jnp.int32, (8, 128), 0)
    tile = jnp.zeros((8, 128), F32)
    for group in range(NORM_CHUNKS[0][1] // 8):
        low, high = ((3, 4), (4, 7), (4, 8))[group % 3]
        part = lambda s: (s >= low).astype(jnp.int32) + (s >= high).astype(jnp.int32)
        same = (lane // 8 == group) & (part(sub) == part(lane % 8))
        total = jnp.sum(jnp.where(same, jnp.broadcast_to(row, (8, 128)), 0.0), axis=1, keepdims=True)
        tile = jnp.where(lane == group, total, tile)
    return tile


def kernel(grad_ref, master_ref, one_ref, two_ref, params, master, one, two, relay, grad, weight_buf, norm_buf, first_buf, sq_buf,
           load_sem, rs_recv, rs_send, hop_recv, hop_send, ex_recv, ex_send, ag_x, ag_y, ag_d, ag_o, ag_send):
    model = lax.axis_index("model")
    me = lax.axis_index("data")
    linear = model * DATA + me
    core = me % 2
    x = (me // 2) % 2
    y = me // 4
    to_core = 1 - 2 * core
    near_x = me + 2 - 4 * x
    near_y = me + 4 - 8 * y
    diag = near_x + 4 - 8 * y
    other = me + to_core
    peer = lambda index: {"model": model, "data": index}
    block = lambda index: pl.ds(pl.multiple_of(index * COLS, COLS), COLS)

    loads = [pltpu.make_async_copy(source, target, load_sem.at[i])
             for i, (source, target) in enumerate(((master_ref, master), (one_ref, one), (two_ref, two)))]

    first = (near_x, near_y)
    second = (near_y, near_x)

    def rows_of(half, chunk):
        return pl.ds(half * HALF + RS_STARTS[chunk], RS_SIZES[chunk])

    barrier = pltpu.get_barrier_semaphore()

    @pl.loop(1, DEVICES)
    def _(offset):
        index = (linear + offset) % DEVICES
        pl.semaphore_signal(barrier, inc=1, device_id={"model": index // DATA, "data": index % DATA}, device_id_type=MESH)

    pl.semaphore_wait(barrier, DEVICES - 1)

    def remote(source, target, send, recv, index):
        return pltpu.make_async_remote_copy(src_ref=source, dst_ref=target, send_sem=send, recv_sem=recv,
                                            device_id=peer(index), device_id_type=MESH)

    for chunk in range(RS_CHUNKS):
        for half in range(2):
            rows = rows_of(half, chunk)
            recv = rs_recv.at[half, chunk]
            send = rs_send.at[half]
            for turn in range(2):
                shift = turn * to_core
                for part, owner in enumerate((first[half] + shift, diag + shift)):
                    remote(grad_ref.at[0, rows, block(owner)], params.at[rows, pl.ds((4 + 2 * turn + part) * COLS, COLS)], send, recv, first[half] + shift).start()
            for part, owner in enumerate((other, second[half] + to_core)):
                remote(grad_ref.at[0, rows, block(owner)], params.at[rows, pl.ds((2 + part) * COLS, COLS)], send, recv, other).start()

    def load_own(chunk):
        for half in range(2):
            rows = rows_of(half, chunk)
            for part, owner in enumerate((me, second[half])):
                pltpu.make_async_copy(grad_ref.at[0, rows, block(owner)], params.at[rows, pl.ds(part * COLS, COLS)], rs_recv.at[half, chunk]).start()

    load_own(0)

    lane = lax.broadcasted_iota(jnp.int32, (8, 128), 1)
    sub = lax.broadcasted_iota(jnp.int32, (8, 128), 0)

    def weight_rows(group, tile):
        rows = pl.ds(pl.multiple_of(group * 8, 8), 8)

        def piece(i, total):
            value = master[rows, pl.ds(pl.multiple_of(i * PIECE, PIECE), PIECE)]
            return total + fold_lanes(value * value)

        total = lax.fori_loop(0, PIECES, piece, jnp.zeros((8, 128), F32))
        return jnp.where(lane == group, jnp.sum(total, axis=1, keepdims=True), tile)


    def exchange(buf, number):
        @pl.loop(1, DEVICES)
        def _(offset):
            index = (linear + offset) % DEVICES
            pltpu.make_async_remote_copy(src_ref=buf.at[linear], dst_ref=buf.at[linear], send_sem=ex_send.at[number], recv_sem=ex_recv.at[number],
                                         device_id={"model": index // DATA, "data": index % DATA}, device_id_type=MESH).start()

    def exchange_wait(buf, sem):
        others = buf.at[pl.ds(0, DEVICES - 1)]
        pltpu.make_async_copy(others, others, sem).wait()

    def gathered(buf):
        total = buf[0]
        for index in range(1, DEVICES):
            total = total + buf[index]
        return total

    EX_WEIGHT, EX_GRAD, EX_FIRST = range(3)

    def four(rows, cols_at, part):
        total = params[rows, pl.ds(pl.multiple_of(part * COLS + cols_at, PIECE), PIECE)].astype(F32)
        for source in range(1, 4):
            total = total + params[rows, pl.ds(pl.multiple_of((2 * source + part) * COLS + cols_at, PIECE), PIECE)].astype(F32)
        return total

    def hop(half, chunk):
        rows = rows_of(half, chunk)
        return remote(relay.at[rows], grad.at[rows], hop_send.at[half], hop_recv.at[half, chunk], second[half])

    for chunk in range(RS_CHUNKS):
        for half in range(2):
            rows = rows_of(half, chunk)
            whole = params.at[rows]
            pltpu.make_async_copy(whole, whole, rs_recv.at[half, chunk]).wait()

            @pl.loop(0, RS_SIZES[chunk] // 16 * PIECES)
            def _(step):
                tile_rows = pl.ds(pl.multiple_of(half * HALF + RS_STARTS[chunk] + step // PIECES * 16, 16), 16)
                cols_at = step % PIECES * PIECE
                relay[tile_rows, pl.ds(pl.multiple_of(cols_at, PIECE), PIECE)] = four(tile_rows, cols_at, 1)

            hop(half, chunk).start()
        if chunk + 1 < RS_CHUNKS:
            load_own(chunk + 1)
        if chunk < 3:
            loads[chunk].start()
        if chunk == 1:
            loads[0].wait()
            weight_buf[linear] = lax.fori_loop(0, ROWS // 8, weight_rows, jnp.zeros((8, 128), F32))
        if chunk == 2:
            exchange(weight_buf, EX_WEIGHT)

    square = jnp.zeros((8, 128), F32)
    for chunk in range(RS_CHUNKS):
        for half in range(2):
            hop(half, chunk).wait_recv()

            def finish(step, total):
                tile_rows = pl.ds(pl.multiple_of(half * HALF + RS_STARTS[chunk] + step // PIECES * 16, 16), 16)
                cols_at = step % PIECES * PIECE
                cols = pl.ds(pl.multiple_of(cols_at, PIECE), PIECE)
                value = (grad[tile_rows, cols] + four(tile_rows, cols_at, 0)) * (1.0 / DATA)
                grad[tile_rows, cols] = value
                folded = fold_lanes(value * value)
                return total + (folded[0:8] + folded[8:16])

            square = lax.fori_loop(0, RS_SIZES[chunk] // 16 * PIECES, finish, square)

    norm_buf[linear] = jnp.sum(square, axis=0, keepdims=True)
    exchange(norm_buf, EX_GRAD)
    for half in range(2):
        rows = pl.ds(half * HALF, HALF)
        pltpu.make_async_copy(relay.at[rows], relay.at[rows], hop_send.at[half]).wait()
    for load in loads[1:]:
        load.wait()
    exchange_wait(weight_buf, ex_recv.at[EX_WEIGHT])
    weight_norm = jnp.sqrt(tensor_total(gathered(weight_buf)))
    exchange_wait(norm_buf, ex_recv.at[EX_GRAD])
    grad_norm = jnp.sqrt(jnp.sum(gathered(norm_buf), axis=1, keepdims=True))
    clip = jnp.minimum(1.0, MAX_NORM / grad_norm)

    def adam_row_sums(group):
        rows = pl.ds(pl.multiple_of(group * 8, 8), 8)

        def piece(i, total):
            cols = pl.ds(pl.multiple_of(i * PIECE, PIECE), PIECE)
            scaled = grad[rows, cols] * clip
            new_one = BETA_ONE * one[rows, cols] + (1.0 - BETA_ONE) * scaled
            new_two = BETA_TWO * two[rows, cols] + (1.0 - BETA_TWO) * (scaled * scaled)
            one[rows, cols] = new_one
            two[rows, cols] = new_two
            direction = (new_one * (1.0 / CORR_ONE)) / (jnp.sqrt(new_two * (1.0 / CORR_TWO)) + EPSILON) + WEIGHT_DECAY * master[rows, cols]
            relay[rows, cols] = direction
            return total + fold_lanes(direction * direction)

        total = lax.fori_loop(0, PIECES, piece, jnp.zeros((8, 128), F32))
        return jnp.sum(total, axis=1, keepdims=True)

    def adam_rows(group, tile):
        return jnp.where(lane == group, adam_row_sums(group), tile)

    def adam_first(group, tile):
        return jnp.where(lane == 8 * group + sub, adam_row_sums(group), tile)

    def step_rates(number):
        if number == 0:
            exchange_wait(first_buf, ex_recv.at[EX_FIRST])
            total = first_totals(gathered(first_buf))
        else:
            exchange_wait(sq_buf.at[number - 1], ex_recv.at[EX_FIRST + number])
            total = tensor_total(gathered(sq_buf.at[number - 1]))
        return weight_norm / jnp.sqrt(total) * LEARN_RATE

    def ag_rows(chunk):
        return pl.ds(AG_STARTS[chunk], AG_SIZES[chunk])

    def update(number, rates):
        start, stop = NORM_CHUNKS[number]
        for chunk in range(AG_CHUNKS):
            if not start <= AG_STARTS[chunk] < stop:
                continue

            @pl.loop(0, AG_SIZES[chunk] // 16)
            def _(tile):
                group = AG_STARTS[chunk] // 8 + 2 * tile
                rows = pl.ds(pl.multiple_of(AG_STARTS[chunk] + tile * 16, 16), 16)
                rate = jnp.concatenate([jnp.sum(jnp.where(lane == group + i, rates, 0.0), axis=1, keepdims=True) for i in range(2)], axis=0)

                @pl.loop(0, PIECES)
                def _(i):
                    cols = pl.ds(pl.multiple_of(i * PIECE, PIECE), PIECE)
                    value = master[rows, cols] - rate * relay[rows, cols]
                    master[rows, cols] = value
                    params[rows, pl.ds(pl.multiple_of(me * COLS + i * PIECE, PIECE), PIECE)] = value.astype(BF16)

            rows = ag_rows(chunk)
            own = params.at[rows, block(me)]
            remote(own, own, ag_send.at[0], ag_x.at[chunk], near_x).start()
            remote(own, own, ag_send.at[1], ag_y.at[chunk], near_y).start()
            remote(own, own, ag_send.at[2], ag_o, other).start()

    groups = [(start // 8, stop // 8) for start, stop in NORM_CHUNKS]
    zero_tile = jnp.zeros((8, 128), F32)
    first_buf[linear] = jnp.sum(lax.fori_loop(*groups[0], adam_first, zero_tile), axis=0, keepdims=True)
    tile = lax.fori_loop(groups[1][0], groups[1][0] + 1, adam_rows, zero_tile)
    exchange(first_buf, EX_FIRST)
    sq_buf[0, linear] = lax.fori_loop(groups[1][0] + 1, groups[1][1], adam_rows, tile)
    tile = lax.fori_loop(groups[2][0], groups[2][0] + 1, adam_rows, zero_tile)
    exchange(sq_buf.at[0], EX_FIRST + 1)
    update(0, step_rates(0))
    sq_buf[1, linear] = lax.fori_loop(groups[2][0] + 1, groups[2][1], adam_rows, tile)
    rates = step_rates(1)
    exchange(sq_buf.at[1], EX_FIRST + 2)
    update(1, rates)
    update(2, step_rates(2))

    def arrived(sem, source, rows):
        view = params.at[rows, block(source)]
        pltpu.make_async_copy(view, view, sem).wait()
        return view

    for chunk in range(AG_CHUNKS):
        rows = ag_rows(chunk)
        view = arrived(ag_x.at[chunk], near_x, rows)
        if chunk % 2 == 0:
            remote(view, view, ag_send.at[1], ag_d.at[chunk], near_y).start()
        remote(view, view, ag_send.at[2], ag_o, other).start()
        view = arrived(ag_y.at[chunk], near_y, rows)
        if chunk % 2 == 1:
            remote(view, view, ag_send.at[0], ag_d.at[chunk], near_x).start()
        remote(view, view, ag_send.at[2], ag_o, other).start()

    for chunk in range(AG_CHUNKS):
        view = arrived(ag_d.at[chunk], diag, ag_rows(chunk))
        remote(view, view, ag_send.at[2], ag_o, other).start()

    half_cols = params.at[:, pl.ds(0, DATA // 2 * COLS)]
    pltpu.make_async_copy(half_cols, half_cols, ag_o).wait()
    pltpu.make_async_copy(half_cols, half_cols, ag_send.at[2]).wait()
    for direction in range(2):
        for part in (pl.ds(0, ROWS), pl.ds(0, HALF)):
            view = params.at[part, pl.ds(0, COLS)]
            pltpu.make_async_copy(view, view, ag_send.at[direction]).wait()
    for half in range(2):
        view = params.at[pl.ds(0, HALF), pl.ds(0, 6 * COLS)]
        pltpu.make_async_copy(view, view, rs_send.at[half]).wait()
    exchange_wait(weight_buf, ex_send.at[EX_WEIGHT])
    exchange_wait(norm_buf, ex_send.at[EX_GRAD])
    exchange_wait(first_buf, ex_send.at[EX_FIRST])
    for number in range(2):
        exchange_wait(sq_buf.at[number], ex_send.at[EX_FIRST + 1 + number])


def write_out(*refs):
    count = len(refs) // 2
    sem = refs[-1]
    copies = []
    for source, target in zip(refs[:count], refs[count:-1]):
        for part in range(OUT_PARTS):
            rows = pl.ds(part * (ROWS // OUT_PARTS), ROWS // OUT_PARTS)
            copies.append(pltpu.make_async_copy(source.at[rows], target.at[rows], sem.at[len(copies)]))
    for copy in copies:
        copy.start()
    for copy in copies:
        copy.wait()


def solution(mesh):
    def device_step(local_grads, master, moment_one, moment_two):
        any_spec = pl.BlockSpec(memory_space=pl.ANY)
        vmem_spec = pl.BlockSpec(memory_space=pltpu.VMEM)
        state = pltpu.VMEM((ROWS, COLS), F32)
        dma = pltpu.SemaphoreType.DMA
        results = pl.pallas_call(
            kernel,
            name="lamb",
            out_shape=(pltpu.VMEM((ROWS, DATA * COLS), BF16), state, state, state),
            in_specs=[any_spec] * 4,
            out_specs=[vmem_spec] * 4,
            scratch_shapes=[
                pltpu.VMEM((ROWS, COLS), F32),
                pltpu.VMEM((ROWS, COLS), F32),
                pltpu.VMEM((DEVICES, 8, 128), F32),
                pltpu.VMEM((DEVICES, 1, 128), F32),
                pltpu.VMEM((DEVICES, 1, 128), F32),
                pltpu.VMEM((2, DEVICES, 8, 128), F32),
                dma((3,)),
                dma((2, RS_CHUNKS)),
                dma((2,)),
                dma((2, RS_CHUNKS)),
                dma((2,)),
                dma((5,)),
                dma((5,)),
                dma((AG_CHUNKS,)),
                dma((AG_CHUNKS,)),
                dma((AG_CHUNKS,)),
                dma,
                dma((3,)),
            ],
            compiler_params=pltpu.CompilerParams(collective_id=0, has_side_effects=True, vmem_limit_bytes=16 << 20),
        )(local_grads, master, moment_one, moment_two)
        written = []
        for group in (results[:1], results[1:]):
            written += pl.pallas_call(
                write_out,
                name="write_out",
                out_shape=[jax.ShapeDtypeStruct(value.shape, value.dtype) for value in group],
                in_specs=[vmem_spec] * len(group),
                out_specs=[any_spec] * len(group),
                scratch_shapes=[dma((len(group) * OUT_PARTS,))],
                compiler_params=pltpu.CompilerParams(vmem_limit_bytes=1 << 20),
            )(*group)
        return tuple(written)

    state_spec = P(None, ('model', 'data'))
    return jax.shard_map(device_step, mesh=mesh, in_specs=(P('data', None, 'model'), state_spec, state_spec, state_spec), out_specs=(P(None, 'model'), state_spec, state_spec, state_spec), check_vma=False)
```

```python
import jax
import jax.numpy as jnp
from jax import lax
from jax.experimental import pallas as pl
from jax.experimental.pallas import tpu as pltpu
from jax.sharding import PartitionSpec as P

STEP = 4
LEARN_RATE = 0.08
BETA_ONE = 0.9
BETA_TWO = 0.999
EPSILON = 1e-6
WEIGHT_DECAY = 0.01
MAX_NORM = 1.0
CORR_ONE = 1.0 - BETA_ONE ** STEP
CORR_TWO = 1.0 - BETA_TWO ** STEP

ROWS = 384
HALF = 192
COLS = 4096
DATA = 8
DEVICES = 16
PIECE = 1024
PIECES = COLS // PIECE
ADAM_PIECE = 1024

RS_SIZES = (48, 48, 48, 32, 16)
RS_CHUNKS = len(RS_SIZES)
RS_STARTS = tuple(sum(RS_SIZES[:i]) for i in range(RS_CHUNKS))
AG_SIZES = (32,) * 10 + (16,) * 4
AG_CHUNKS = len(AG_SIZES)
AG_STARTS = tuple(sum(AG_SIZES[:i]) for i in range(AG_CHUNKS))
NORM_CHUNKS = ((0, 32), (32, 288), (288, 384))
OUT_PARTS = 4

MESH = pl.DeviceIdType.MESH
F32 = jnp.float32
BF16 = jnp.bfloat16


def fold_lanes(values):
    total = values[:, 0:128]
    for group in range(1, values.shape[1] // 128):
        total = total + values[:, group * 128:(group + 1) * 128]
    return total


def tensor_total(tile):
    row = [tile[s:s + 1, :] for s in range(8)]
    first3 = row[0] + row[1] + row[2]
    first4 = first3 + row[3]
    mid3 = row[4] + row[5] + row[6]
    last4 = mid3 + row[7]
    sub = lax.broadcasted_iota(jnp.int32, (8, 128), 0)
    kind = lax.broadcasted_iota(jnp.int32, (8, 128), 1) % 3
    full = lambda value: jnp.broadcast_to(value, (8, 128))
    low = jnp.where(kind == 0, jnp.where(sub == 3, full(row[3]), full(first3)), full(first4))
    high = jnp.where(kind == 1, jnp.where(sub == 7, full(row[7]), full(mid3)), full(last4))
    return jnp.where(sub < 4, low, high)


def first_totals(row):
    lane = lax.broadcasted_iota(jnp.int32, (8, 128), 1)
    sub = lax.broadcasted_iota(jnp.int32, (8, 128), 0)
    tile = jnp.zeros((8, 128), F32)
    for group in range(NORM_CHUNKS[0][1] // 8):
        low, high = ((3, 4), (4, 7), (4, 8))[group % 3]
        part = lambda s: (s >= low).astype(jnp.int32) + (s >= high).astype(jnp.int32)
        same = (lane // 8 == group) & (part(sub) == part(lane % 8))
        total = jnp.sum(jnp.where(same, jnp.broadcast_to(row, (8, 128)), 0.0), axis=1, keepdims=True)
        tile = jnp.where(lane == group, total, tile)
    return tile


def kernel(grad_ref, master_ref, one_ref, two_ref, params, master, one, two, relay, grad, weight_buf, norm_buf, first_buf, sq_buf, part_buf,
           load_sem, rs_recv, rs_send, hop_recv, hop_send, ex_recv, ex_send, ag_x, ag_y, ag_d, ag_o, ag_send):
    model = lax.axis_index("model")
    me = lax.axis_index("data")
    linear = model * DATA + me
    core = me % 2
    x = (me // 2) % 2
    y = me // 4
    to_core = 1 - 2 * core
    near_x = me + 2 - 4 * x
    near_y = me + 4 - 8 * y
    diag = near_x + 4 - 8 * y
    other = me + to_core
    peer = lambda index: {"model": model, "data": index}
    block = lambda index: pl.ds(pl.multiple_of(index * COLS, COLS), COLS)

    loads = [pltpu.make_async_copy(source, target, load_sem.at[i])
             for i, (source, target) in enumerate(((master_ref, master), (one_ref, one), (two_ref, two)))]

    first = (near_x, near_y)
    second = (near_y, near_x)

    def rows_of(half, chunk):
        return pl.ds(half * HALF + RS_STARTS[chunk], RS_SIZES[chunk])

    barrier = pltpu.get_barrier_semaphore()

    @pl.loop(1, DEVICES)
    def _(offset):
        index = (linear + offset) % DEVICES
        pl.semaphore_signal(barrier, inc=1, device_id={"model": index // DATA, "data": index % DATA}, device_id_type=MESH)

    pl.semaphore_wait(barrier, DEVICES - 1)

    def remote(source, target, send, recv, index):
        return pltpu.make_async_remote_copy(src_ref=source, dst_ref=target, send_sem=send, recv_sem=recv,
                                            device_id=peer(index), device_id_type=MESH)

    for chunk in range(RS_CHUNKS):
        for half in range(2):
            rows = rows_of(half, chunk)
            recv = rs_recv.at[half, chunk]
            send = rs_send.at[half]
            for turn in range(2):
                shift = turn * to_core
                for part, owner in enumerate((first[half] + shift, diag + shift)):
                    remote(grad_ref.at[0, rows, block(owner)], params.at[rows, pl.ds((4 + 2 * turn + part) * COLS, COLS)], send, recv, first[half] + shift).start()
            for part, owner in enumerate((other, second[half] + to_core)):
                remote(grad_ref.at[0, rows, block(owner)], params.at[rows, pl.ds((2 + part) * COLS, COLS)], send, recv, other).start()

    def load_own(chunk):
        for half in range(2):
            rows = rows_of(half, chunk)
            for part, owner in enumerate((me, second[half])):
                pltpu.make_async_copy(grad_ref.at[0, rows, block(owner)], params.at[rows, pl.ds(part * COLS, COLS)], rs_recv.at[half, chunk]).start()

    load_own(0)

    lane = lax.broadcasted_iota(jnp.int32, (8, 128), 1)
    sub = lax.broadcasted_iota(jnp.int32, (8, 128), 0)

    def weight_rows(group, tile):
        rows = pl.ds(pl.multiple_of(group * 8, 8), 8)

        def piece(i, total):
            value = master[rows, pl.ds(pl.multiple_of(i * PIECE, PIECE), PIECE)]
            return total + fold_lanes(value * value)

        total = lax.fori_loop(0, PIECES, piece, jnp.zeros((8, 128), F32))
        return jnp.where(lane == group, jnp.sum(total, axis=1, keepdims=True), tile)


    def exchange(buf, number):
        for flips in reversed(range(1, DEVICES)):
            to_model, to_y, to_x, to_core = [at + (1 - 2 * at) * (flips >> bit & 1) for bit, at in zip((3, 2, 1, 0), (model, y, x, core))]
            pltpu.make_async_remote_copy(src_ref=buf.at[linear], dst_ref=buf.at[linear], send_sem=ex_send.at[number], recv_sem=ex_recv.at[number],
                                         device_id={"model": to_model, "data": to_y * 4 + to_x * 2 + to_core}, device_id_type=MESH).start()

    def exchange_wait(buf, sem):
        others = buf.at[pl.ds(0, DEVICES - 1)]
        pltpu.make_async_copy(others, others, sem).wait()

    def gathered(buf):
        total = buf[0]
        for index in range(1, DEVICES):
            total = total + buf[index]
        return total

    EX_WEIGHT, EX_GRAD, EX_FIRST = range(3)

    def decay(state, factor):
        @pl.loop(0, ROWS // 8 * PIECES)
        def _(step):
            rows = pl.ds(pl.multiple_of(step // PIECES * 8, 8), 8)
            cols = pl.ds(pl.multiple_of(step % PIECES * PIECE, PIECE), PIECE)
            state[rows, cols] = state[rows, cols] * factor

    def four(rows, cols_at, part):
        total = params[rows, pl.ds(pl.multiple_of(part * COLS + cols_at, PIECE), PIECE)].astype(F32)
        for source in range(1, 4):
            total = total + params[rows, pl.ds(pl.multiple_of((2 * source + part) * COLS + cols_at, PIECE), PIECE)].astype(F32)
        return total

    def hop(half, chunk):
        rows = rows_of(half, chunk)
        return remote(relay.at[rows], grad.at[rows], hop_send.at[half], hop_recv.at[half, chunk], second[half])

    for chunk in range(RS_CHUNKS):
        for half in range(2):
            rows = rows_of(half, chunk)
            whole = params.at[rows]
            pltpu.make_async_copy(whole, whole, rs_recv.at[half, chunk]).wait()

            @pl.loop(0, RS_SIZES[chunk] // 16 * PIECES)
            def _(step):
                tile_rows = pl.ds(pl.multiple_of(half * HALF + RS_STARTS[chunk] + step // PIECES * 16, 16), 16)
                cols_at = step % PIECES * PIECE
                relay[tile_rows, pl.ds(pl.multiple_of(cols_at, PIECE), PIECE)] = four(tile_rows, cols_at, 1)

            hop(half, chunk).start()
        if chunk + 1 < RS_CHUNKS:
            load_own(chunk + 1)
        if chunk < 3:
            loads[chunk].start()
        if chunk == 1:
            loads[0].wait()
            weight_buf[linear] = lax.fori_loop(0, ROWS // 8, weight_rows, jnp.zeros((8, 128), F32))
        if chunk == 2:
            exchange(weight_buf, EX_WEIGHT)
            loads[1].wait()
            decay(one, BETA_ONE)
        if chunk == 3:
            loads[2].wait()
            decay(two, BETA_TWO)

    square = jnp.zeros((8, 128), F32)
    for chunk in range(RS_CHUNKS):
        for half in range(2):
            hop(half, chunk).wait_recv()

            def finish(step, total):
                tile_rows = pl.ds(pl.multiple_of(half * HALF + RS_STARTS[chunk] + step // PIECES * 16, 16), 16)
                cols_at = step % PIECES * PIECE
                cols = pl.ds(pl.multiple_of(cols_at, PIECE), PIECE)
                value = (grad[tile_rows, cols] + four(tile_rows, cols_at, 0)) * (1.0 / DATA)
                grad[tile_rows, cols] = value
                folded = fold_lanes(value * value)
                return total + (folded[0:8] + folded[8:16])

            square = lax.fori_loop(0, RS_SIZES[chunk] // 16 * PIECES, finish, square)

    norm_buf[linear] = jnp.sum(square, axis=0, keepdims=True)
    exchange(norm_buf, EX_GRAD)
    for half in range(2):
        rows = pl.ds(half * HALF, HALF)
        pltpu.make_async_copy(relay.at[rows], relay.at[rows], hop_send.at[half]).wait()
    exchange_wait(weight_buf, ex_recv.at[EX_WEIGHT])
    weight_norm = jnp.sqrt(tensor_total(gathered(weight_buf)))
    exchange_wait(norm_buf, ex_recv.at[EX_GRAD])
    grad_norm = jnp.sqrt(jnp.sum(gathered(norm_buf), axis=1, keepdims=True))
    clip = jnp.minimum(1.0, MAX_NORM / grad_norm)

    grad_one = (1.0 - BETA_ONE) * clip
    grad_two = (1.0 - BETA_TWO) ** 0.5 * clip

    def adam(start, stop):
        @pl.loop(start, stop)
        def _(group):
            rows = pl.ds(pl.multiple_of(group * 8, 8), 8)
            total = jnp.zeros((8, 128), F32)
            for i in range(COLS // ADAM_PIECE):
                cols = pl.ds(i * ADAM_PIECE, ADAM_PIECE)
                mean = grad[rows, cols]
                new_one = one[rows, cols] + grad_one * mean
                scaled = grad_two * mean
                new_two = two[rows, cols] + scaled * scaled
                one[rows, cols] = new_one
                two[rows, cols] = new_two
                direction = new_one / (jnp.sqrt(new_two) * (CORR_ONE / CORR_TWO ** 0.5) + CORR_ONE * EPSILON) + WEIGHT_DECAY * master[rows, cols]
                relay[rows, cols] = direction
                total = total + fold_lanes(direction * direction)
            part_buf[group] = total

    def row_sums(start, stop, place):
        tile = jnp.zeros((8, 128), F32)
        for group in range(start, stop):
            tile = jnp.where(lane == place(group), jnp.sum(part_buf[group], axis=1, keepdims=True), tile)
        return tile

    def step_rates(number):
        if number == 0:
            exchange_wait(first_buf, ex_recv.at[EX_FIRST])
            total = first_totals(gathered(first_buf))
        else:
            exchange_wait(sq_buf.at[number - 1], ex_recv.at[EX_FIRST + number])
            total = tensor_total(gathered(sq_buf.at[number - 1]))
        return weight_norm / jnp.sqrt(total) * LEARN_RATE

    def ag_rows(chunk):
        return pl.ds(AG_STARTS[chunk], AG_SIZES[chunk])

    def update(number, rates):
        start, stop = NORM_CHUNKS[number]
        for chunk in range(AG_CHUNKS):
            if not start <= AG_STARTS[chunk] < stop:
                continue

            @pl.loop(0, AG_SIZES[chunk] // 16)
            def _(tile):
                group = AG_STARTS[chunk] // 8 + 2 * tile
                rows = pl.ds(pl.multiple_of(AG_STARTS[chunk] + tile * 16, 16), 16)
                rate = jnp.concatenate([jnp.sum(jnp.where(lane == group + i, rates, 0.0), axis=1, keepdims=True) for i in range(2)], axis=0)

                @pl.loop(0, PIECES)
                def _(i):
                    cols = pl.ds(pl.multiple_of(i * PIECE, PIECE), PIECE)
                    value = master[rows, cols] - rate * relay[rows, cols]
                    master[rows, cols] = value
                    params[rows, pl.ds(pl.multiple_of(me * COLS + i * PIECE, PIECE), PIECE)] = value.astype(BF16)

            rows = ag_rows(chunk)
            own = params.at[rows, block(me)]
            remote(own, own, ag_send.at[0], ag_x.at[chunk], near_x).start()
            remote(own, own, ag_send.at[1], ag_y.at[chunk], near_y).start()
            remote(own, own, ag_send.at[2], ag_o, other).start()

    groups = [(start // 8, stop // 8) for start, stop in NORM_CHUNKS]
    adam(*groups[0])
    first_buf[linear] = jnp.sum(row_sums(*groups[0], lambda group: 8 * group + sub), axis=0, keepdims=True)
    adam(groups[1][0], groups[1][0] + 1)
    exchange(first_buf, EX_FIRST)
    adam(groups[1][0] + 1, groups[1][1])
    sq_buf[0, linear] = row_sums(*groups[1], lambda group: group)
    adam(groups[2][0], groups[2][0] + 1)
    exchange(sq_buf.at[0], EX_FIRST + 1)
    update(0, step_rates(0))
    adam(groups[2][0] + 1, groups[2][1])
    sq_buf[1, linear] = row_sums(*groups[2], lambda group: group)
    rates = step_rates(1)
    exchange(sq_buf.at[1], EX_FIRST + 2)
    update(1, rates)
    update(2, step_rates(2))

    def arrived(sem, source, rows):
        view = params.at[rows, block(source)]
        pltpu.make_async_copy(view, view, sem).wait()
        return view

    for chunk in range(AG_CHUNKS):
        rows = ag_rows(chunk)
        view = arrived(ag_x.at[chunk], near_x, rows)
        if chunk % 2 == 0:
            remote(view, view, ag_send.at[1], ag_d.at[chunk], near_y).start()
        remote(view, view, ag_send.at[2], ag_o, other).start()
        view = arrived(ag_y.at[chunk], near_y, rows)
        if chunk % 2 == 1:
            remote(view, view, ag_send.at[0], ag_d.at[chunk], near_x).start()
        remote(view, view, ag_send.at[2], ag_o, other).start()

    for chunk in range(AG_CHUNKS):
        view = arrived(ag_d.at[chunk], diag, ag_rows(chunk))
        remote(view, view, ag_send.at[2], ag_o, other).start()

    half_cols = params.at[:, pl.ds(0, DATA // 2 * COLS)]
    pltpu.make_async_copy(half_cols, half_cols, ag_o).wait()
    pltpu.make_async_copy(half_cols, half_cols, ag_send.at[2]).wait()
    for direction in range(2):
        for part in (pl.ds(0, ROWS), pl.ds(0, HALF)):
            view = params.at[part, pl.ds(0, COLS)]
            pltpu.make_async_copy(view, view, ag_send.at[direction]).wait()
    for half in range(2):
        view = params.at[pl.ds(0, HALF), pl.ds(0, 6 * COLS)]
        pltpu.make_async_copy(view, view, rs_send.at[half]).wait()
    exchange_wait(weight_buf, ex_send.at[EX_WEIGHT])
    exchange_wait(norm_buf, ex_send.at[EX_GRAD])
    exchange_wait(first_buf, ex_send.at[EX_FIRST])
    for number in range(2):
        exchange_wait(sq_buf.at[number], ex_send.at[EX_FIRST + 1 + number])


def write_out(*refs):
    count = len(refs) // 2
    sem = refs[-1]
    copies = []
    for source, target in zip(refs[:count], refs[count:-1]):
        for part in range(OUT_PARTS):
            rows = pl.ds(part * (ROWS // OUT_PARTS), ROWS // OUT_PARTS)
            copies.append(pltpu.make_async_copy(source.at[rows], target.at[rows], sem.at[len(copies)]))
    for copy in copies:
        copy.start()
    for copy in copies:
        copy.wait()


def solution(mesh):
    def device_step(local_grads, master, moment_one, moment_two):
        any_spec = pl.BlockSpec(memory_space=pl.ANY)
        vmem_spec = pl.BlockSpec(memory_space=pltpu.VMEM)
        state = pltpu.VMEM((ROWS, COLS), F32)
        dma = pltpu.SemaphoreType.DMA
        results = pl.pallas_call(
            kernel,
            name="lamb",
            out_shape=(pltpu.VMEM((ROWS, DATA * COLS), BF16), state, state, state),
            in_specs=[any_spec] * 4,
            out_specs=[vmem_spec] * 4,
            scratch_shapes=[
                pltpu.VMEM((ROWS, COLS), F32),
                pltpu.VMEM((ROWS, COLS), F32),
                pltpu.VMEM((DEVICES, 8, 128), F32),
                pltpu.VMEM((DEVICES, 1, 128), F32),
                pltpu.VMEM((DEVICES, 1, 128), F32),
                pltpu.VMEM((2, DEVICES, 8, 128), F32),
                pltpu.VMEM((ROWS // 8, 8, 128), F32),
                dma((3,)),
                dma((2, RS_CHUNKS)),
                dma((2,)),
                dma((2, RS_CHUNKS)),
                dma((2,)),
                dma((5,)),
                dma((5,)),
                dma((AG_CHUNKS,)),
                dma((AG_CHUNKS,)),
                dma((AG_CHUNKS,)),
                dma,
                dma((3,)),
            ],
            compiler_params=pltpu.CompilerParams(collective_id=0, has_side_effects=True, vmem_limit_bytes=16 << 20),
        )(local_grads, master, moment_one, moment_two)
        written = []
        for group in (results[:1], results[1:]):
            written += pl.pallas_call(
                write_out,
                name="write_out",
                out_shape=[jax.ShapeDtypeStruct(value.shape, value.dtype) for value in group],
                in_specs=[vmem_spec] * len(group),
                out_specs=[any_spec] * len(group),
                scratch_shapes=[dma((len(group) * OUT_PARTS,))],
                compiler_params=pltpu.CompilerParams(vmem_limit_bytes=1 << 20),
            )(*group)
        return tuple(written)

    state_spec = P(None, ('model', 'data'))
    return jax.shard_map(device_step, mesh=mesh, in_specs=(P('data', None, 'model'), state_spec, state_spec, state_spec), out_specs=(P(None, 'model'), state_spec, state_spec, state_spec), check_vma=False)
```

```python
import functools

import jax
import jax.numpy as jnp
from jax import lax
from jax.experimental import pallas as pl
from jax.experimental.pallas import tpu as pltpu
from jax.sharding import PartitionSpec as P

STEP = 4
LEARN_RATE = 0.08
BETA_ONE = 0.9
BETA_TWO = 0.999
EPSILON = 1e-6
WEIGHT_DECAY = 0.01
MAX_NORM = 1.0
CORR_ONE = 1.0 - BETA_ONE ** STEP
CORR_TWO = 1.0 - BETA_TWO ** STEP

ROWS = 384
HALF = 192
COLS = 4096
DATA = 8
DEVICES = 16
PIECE = 1024
PIECES = COLS // PIECE
ADAM_PIECE = 1024

RS_SIZES = (48, 48, 48, 32, 16)
RS_CHUNKS = len(RS_SIZES)
RS_STARTS = tuple(sum(RS_SIZES[:i]) for i in range(RS_CHUNKS))
AG_SIZES = (16,) * 2 + (32,) * 9 + (16,) * 4
AG_FAR_BY_Y = (1, 0) + (1, 0) * 4 + (1,) + (0, 0, 1, 0)
AG_CHUNKS = len(AG_SIZES)
AG_STARTS = tuple(sum(AG_SIZES[:i]) for i in range(AG_CHUNKS))
NORM_CHUNKS = ((0, 32), (32, 288), (288, 384))

MESH = pl.DeviceIdType.MESH
F32 = jnp.float32
BF16 = jnp.bfloat16


def fold_lanes(values):
    total = values[:, 0:128]
    for group in range(1, values.shape[1] // 128):
        total = total + values[:, group * 128:(group + 1) * 128]
    return total


def tensor_total(tile):
    row = [tile[s:s + 1, :] for s in range(8)]
    first3 = row[0] + row[1] + row[2]
    first4 = first3 + row[3]
    mid3 = row[4] + row[5] + row[6]
    last4 = mid3 + row[7]
    sub = lax.broadcasted_iota(jnp.int32, (8, 128), 0)
    kind = lax.broadcasted_iota(jnp.int32, (8, 128), 1) % 3
    full = lambda value: jnp.broadcast_to(value, (8, 128))
    low = jnp.where(kind == 0, jnp.where(sub == 3, full(row[3]), full(first3)), full(first4))
    high = jnp.where(kind == 1, jnp.where(sub == 7, full(row[7]), full(mid3)), full(last4))
    return jnp.where(sub < 4, low, high)


def first_totals(row):
    lane = lax.broadcasted_iota(jnp.int32, (8, 128), 1)
    sub = lax.broadcasted_iota(jnp.int32, (8, 128), 0)
    tile = jnp.zeros((8, 128), F32)
    for group in range(NORM_CHUNKS[0][1] // 8):
        low, high = ((3, 4), (4, 7), (4, 8))[group % 3]
        part = lambda s: (s >= low).astype(jnp.int32) + (s >= high).astype(jnp.int32)
        same = (lane // 8 == group) & (part(sub) == part(lane % 8))
        total = jnp.sum(jnp.where(same, jnp.broadcast_to(row, (8, 128)), 0.0), axis=1, keepdims=True)
        tile = jnp.where(lane == group, total, tile)
    return tile


def kernel(grad_ref, master_ref, one_ref, two_ref, params, master, one, two, relay, grad, weight_buf, norm_buf, first_buf, sq_buf, part_buf,
           load_sem, rs_recv, rs_send, hop_recv, hop_send, ex_recv, ex_send, ag_x, ag_y, ag_d, ag_o, ag_send, plane_sem):
    model = lax.axis_index("model")
    me = lax.axis_index("data")
    linear = model * DATA + me
    core = me % 2
    x = (me // 2) % 2
    y = me // 4
    to_core = 1 - 2 * core
    near_x = me + 2 - 4 * x
    near_y = me + 4 - 8 * y
    diag = near_x + 4 - 8 * y
    other = me + to_core
    peer = lambda index: {"model": model, "data": index}
    block = lambda index: pl.ds(pl.multiple_of(index * COLS, COLS), COLS)

    loads = [pltpu.make_async_copy(source, target, load_sem.at[i])
             for i, (source, target) in enumerate(((master_ref, master), (one_ref, one), (two_ref, two)))]

    first = (near_x, near_y)
    second = (near_y, near_x)

    def rows_of(half, chunk):
        return pl.ds(half * HALF + RS_STARTS[chunk], RS_SIZES[chunk])

    barrier = pltpu.get_barrier_semaphore()

    mirror = {"model": 1 - model, "data": me}
    for neighbour in (peer(near_x), peer(near_x + to_core), peer(near_y), peer(near_y + to_core), mirror, peer(other)):
        pl.semaphore_signal(barrier, inc=1, device_id=neighbour, device_id_type=MESH)
    pl.semaphore_wait(barrier, 6)

    def remote(source, target, send, recv, index):
        return pltpu.make_async_remote_copy(src_ref=source, dst_ref=target, send_sem=send, recv_sem=recv,
                                            device_id=peer(index), device_id_type=MESH)

    for chunk in range(RS_CHUNKS):
        for half in range(2):
            rows = rows_of(half, chunk)
            recv = rs_recv.at[half, chunk]
            send = rs_send.at[half]
            for turn in range(2):
                shift = turn * to_core
                for part, owner in enumerate((first[half] + shift, diag + shift)):
                    remote(grad_ref.at[0, rows, block(owner)], params.at[rows, pl.ds((4 + 2 * turn + part) * COLS, COLS)], send, recv, first[half] + shift).start()
            for part, owner in enumerate((other, second[half] + to_core)):
                remote(grad_ref.at[0, rows, block(owner)], params.at[rows, pl.ds((2 + part) * COLS, COLS)], send, recv, other).start()

    def load_own(chunk):
        for half in range(2):
            rows = rows_of(half, chunk)
            for part, owner in enumerate((me, second[half])):
                pltpu.make_async_copy(grad_ref.at[0, rows, block(owner)], params.at[rows, pl.ds(part * COLS, COLS)], rs_recv.at[half, chunk]).start()

    load_own(0)

    lane = lax.broadcasted_iota(jnp.int32, (8, 128), 1)
    sub = lax.broadcasted_iota(jnp.int32, (8, 128), 0)

    def weight_rows(group, tile):
        rows = pl.ds(pl.multiple_of(group * 8, 8), 8)

        def piece(i, total):
            value = master[rows, pl.ds(pl.multiple_of(i * PIECE, PIECE), PIECE)]
            return total + fold_lanes(value * value)

        total = lax.fori_loop(0, PIECES, piece, jnp.zeros((8, 128), F32))
        return jnp.where(lane == group, jnp.sum(total, axis=1, keepdims=True), tile)


    def exchange(buf, number):
        for flips in reversed(range(1, DEVICES)):
            to_model, to_y, to_x, to_core = [at + (1 - 2 * at) * (flips >> bit & 1) for bit, at in zip((3, 2, 1, 0), (model, y, x, core))]
            pltpu.make_async_remote_copy(src_ref=buf.at[linear], dst_ref=buf.at[linear], send_sem=ex_send.at[number], recv_sem=ex_recv.at[number],
                                         device_id={"model": to_model, "data": to_y * 4 + to_x * 2 + to_core}, device_id_type=MESH).start()

    def exchange_wait(buf, sem):
        others = buf.at[pl.ds(0, DEVICES - 1)]
        pltpu.make_async_copy(others, others, sem).wait()

    def gathered(buf):
        total = buf[0]
        for index in range(1, DEVICES):
            total = total + buf[index]
        return total

    EX_WEIGHT, EX_GRAD, EX_FIRST = range(3)

    def decay(state, factor):
        @pl.loop(0, ROWS // 8 * PIECES)
        def _(step):
            rows = pl.ds(pl.multiple_of(step // PIECES * 8, 8), 8)
            cols = pl.ds(pl.multiple_of(step % PIECES * PIECE, PIECE), PIECE)
            state[rows, cols] = state[rows, cols] * factor

    def four(rows, cols_at, part):
        total = params[rows, pl.ds(pl.multiple_of(part * COLS + cols_at, PIECE), PIECE)].astype(F32)
        for source in range(1, 4):
            total = total + params[rows, pl.ds(pl.multiple_of((2 * source + part) * COLS + cols_at, PIECE), PIECE)].astype(F32)
        return total

    def hop(half, chunk):
        rows = rows_of(half, chunk)
        return remote(relay.at[rows], grad.at[rows], hop_send.at[half], hop_recv.at[half, chunk], second[half])

    for chunk in range(RS_CHUNKS):
        for half in range(2):
            rows = rows_of(half, chunk)
            whole = params.at[rows]
            pltpu.make_async_copy(whole, whole, rs_recv.at[half, chunk]).wait()

            @pl.loop(0, RS_SIZES[chunk] // 16 * PIECES)
            def _(step):
                tile_rows = pl.ds(pl.multiple_of(half * HALF + RS_STARTS[chunk] + step // PIECES * 16, 16), 16)
                cols_at = step % PIECES * PIECE
                relay[tile_rows, pl.ds(pl.multiple_of(cols_at, PIECE), PIECE)] = four(tile_rows, cols_at, 1)

            hop(half, chunk).start()
        if chunk == 0:
            pl.semaphore_signal(plane_sem, inc=1, device_id=mirror, device_id_type=MESH)
        if chunk + 1 < RS_CHUNKS:
            load_own(chunk + 1)
        if chunk < 3:
            loads[chunk].start()
        if chunk == 1:
            loads[0].wait()
            weight_buf[linear] = lax.fori_loop(0, ROWS // 8, weight_rows, jnp.zeros((8, 128), F32))
        if chunk == 2:
            pl.semaphore_wait(plane_sem, 1)
            exchange(weight_buf, EX_WEIGHT)
            loads[1].wait()
            decay(one, BETA_ONE)
        if chunk == 3:
            loads[2].wait()
            decay(two, BETA_TWO)

    square = jnp.zeros((8, 128), F32)
    for chunk in range(RS_CHUNKS):
        for half in range(2):
            hop(half, chunk).wait_recv()

            def finish(step, total):
                tile_rows = pl.ds(pl.multiple_of(half * HALF + RS_STARTS[chunk] + step // PIECES * 16, 16), 16)
                cols_at = step % PIECES * PIECE
                cols = pl.ds(pl.multiple_of(cols_at, PIECE), PIECE)
                value = (grad[tile_rows, cols] + four(tile_rows, cols_at, 0)) * (1.0 / DATA)
                grad[tile_rows, cols] = value
                folded = fold_lanes(value * value)
                return total + (folded[0:8] + folded[8:16])

            square = lax.fori_loop(0, RS_SIZES[chunk] // 16 * PIECES, finish, square)

    norm_buf[linear] = jnp.sum(square, axis=0, keepdims=True)
    exchange(norm_buf, EX_GRAD)
    for half in range(2):
        rows = pl.ds(half * HALF, HALF)
        pltpu.make_async_copy(relay.at[rows], relay.at[rows], hop_send.at[half]).wait()
    exchange_wait(weight_buf, ex_recv.at[EX_WEIGHT])
    weight_norm = jnp.sqrt(tensor_total(gathered(weight_buf)))
    exchange_wait(norm_buf, ex_recv.at[EX_GRAD])
    grad_norm = jnp.sqrt(jnp.sum(gathered(norm_buf), axis=1, keepdims=True))
    clip = jnp.minimum(1.0, MAX_NORM / grad_norm)

    grad_one = (1.0 - BETA_ONE) * clip
    grad_two = (1.0 - BETA_TWO) ** 0.5 * clip

    def adam(start, stop):
        @pl.loop(start, stop)
        def _(group):
            rows = pl.ds(pl.multiple_of(group * 8, 8), 8)
            total = jnp.zeros((8, 128), F32)
            for i in range(COLS // ADAM_PIECE):
                cols = pl.ds(i * ADAM_PIECE, ADAM_PIECE)
                mean = grad[rows, cols]
                new_one = one[rows, cols] + grad_one * mean
                scaled = grad_two * mean
                new_two = two[rows, cols] + scaled * scaled
                one[rows, cols] = new_one
                two[rows, cols] = new_two
                direction = new_one / (jnp.sqrt(new_two) * (CORR_ONE / CORR_TWO ** 0.5) + CORR_ONE * EPSILON) + WEIGHT_DECAY * master[rows, cols]
                relay[rows, cols] = direction
                total = total + fold_lanes(direction * direction)
            part_buf[group] = total

    def row_sums(start, stop, place):
        tile = jnp.zeros((8, 128), F32)
        for group in range(start, stop):
            tile = jnp.where(lane == place(group), jnp.sum(part_buf[group], axis=1, keepdims=True), tile)
        return tile

    def step_rates(number):
        if number == 0:
            exchange_wait(first_buf, ex_recv.at[EX_FIRST])
            total = first_totals(gathered(first_buf))
        else:
            exchange_wait(sq_buf.at[number - 1], ex_recv.at[EX_FIRST + number])
            total = tensor_total(gathered(sq_buf.at[number - 1]))
        return weight_norm / jnp.sqrt(total) * LEARN_RATE

    def ag_rows(chunk):
        return pl.ds(AG_STARTS[chunk], AG_SIZES[chunk])

    def update(number, rates):
        start, stop = NORM_CHUNKS[number]
        for chunk in range(AG_CHUNKS):
            if not start <= AG_STARTS[chunk] < stop:
                continue

            @pl.loop(0, AG_SIZES[chunk] // 16)
            def _(tile):
                group = AG_STARTS[chunk] // 8 + 2 * tile
                rows = pl.ds(pl.multiple_of(AG_STARTS[chunk] + tile * 16, 16), 16)
                rate = jnp.concatenate([jnp.sum(jnp.where(lane == group + i, rates, 0.0), axis=1, keepdims=True) for i in range(2)], axis=0)

                @pl.loop(0, PIECES)
                def _(i):
                    cols = pl.ds(pl.multiple_of(i * PIECE, PIECE), PIECE)
                    value = master[rows, cols] - rate * relay[rows, cols]
                    master[rows, cols] = value
                    params[rows, pl.ds(pl.multiple_of(me * COLS + i * PIECE, PIECE), PIECE)] = value.astype(BF16)

            rows = ag_rows(chunk)
            own = params.at[rows, block(me)]
            remote(own, own, ag_send.at[0], ag_x.at[chunk], near_x).start()
            remote(own, own, ag_send.at[1], ag_y.at[chunk], near_y).start()
            remote(own, own, ag_send.at[2], ag_o, other).start()

    groups = [(start // 8, stop // 8) for start, stop in NORM_CHUNKS]
    adam(*groups[0])
    first_buf[linear] = jnp.sum(row_sums(*groups[0], lambda group: 8 * group + sub), axis=0, keepdims=True)
    adam(groups[1][0], groups[1][0] + 1)
    exchange(first_buf, EX_FIRST)
    adam(groups[1][0] + 1, groups[1][1])
    sq_buf[0, linear] = row_sums(*groups[1], lambda group: group)
    adam(groups[2][0], groups[2][0] + 1)
    exchange(sq_buf.at[0], EX_FIRST + 1)
    update(0, step_rates(0))
    adam(groups[2][0] + 1, groups[2][1])
    sq_buf[1, linear] = row_sums(*groups[2], lambda group: group)
    rates = step_rates(1)
    exchange(sq_buf.at[1], EX_FIRST + 2)
    update(1, rates)
    update(2, step_rates(2))

    def arrived(sem, source, rows):
        view = params.at[rows, block(source)]
        pltpu.make_async_copy(view, view, sem).wait()
        return view

    for chunk in range(AG_CHUNKS):
        rows = ag_rows(chunk)
        view = arrived(ag_x.at[chunk], near_x, rows)
        if AG_FAR_BY_Y[chunk]:
            remote(view, view, ag_send.at[1], ag_d.at[chunk], near_y).start()
        remote(view, view, ag_send.at[2], ag_o, other).start()
        view = arrived(ag_y.at[chunk], near_y, rows)
        if not AG_FAR_BY_Y[chunk]:
            remote(view, view, ag_send.at[0], ag_d.at[chunk], near_x).start()
        remote(view, view, ag_send.at[2], ag_o, other).start()

    for chunk in range(AG_CHUNKS):
        view = arrived(ag_d.at[chunk], diag, ag_rows(chunk))
        remote(view, view, ag_send.at[2], ag_o, other).start()

    half_cols = params.at[:, pl.ds(0, DATA // 2 * COLS)]
    pltpu.make_async_copy(half_cols, half_cols, ag_o).wait()
    pltpu.make_async_copy(half_cols, half_cols, ag_send.at[2]).wait()
    for direction in range(2):
        for part in (pl.ds(0, ROWS), pl.ds(0, HALF)):
            view = params.at[part, pl.ds(0, COLS)]
            pltpu.make_async_copy(view, view, ag_send.at[direction]).wait()
    for half in range(2):
        view = params.at[pl.ds(0, HALF), pl.ds(0, 6 * COLS)]
        pltpu.make_async_copy(view, view, rs_send.at[half]).wait()
    exchange_wait(weight_buf, ex_send.at[EX_WEIGHT])
    exchange_wait(norm_buf, ex_send.at[EX_GRAD])
    exchange_wait(first_buf, ex_send.at[EX_FIRST])
    for number in range(2):
        exchange_wait(sq_buf.at[number], ex_send.at[EX_FIRST + 1 + number])


def write_out(parts, *refs):
    count = len(refs) // 2
    sem = refs[-1]
    copies = []
    for part in range(parts):
        rows = pl.ds(part * (ROWS // parts), ROWS // parts)
        for source, target in zip(refs[:count], refs[count:-1]):
            copies.append(pltpu.make_async_copy(source.at[rows], target.at[rows], sem.at[len(copies)]))
    for number, copy in enumerate(copies):
        copy.start(priority=number % 2)
    for copy in copies:
        copy.wait()


def solution(mesh):
    def device_step(local_grads, master, moment_one, moment_two):
        any_spec = pl.BlockSpec(memory_space=pl.ANY)
        vmem_spec = pl.BlockSpec(memory_space=pltpu.VMEM)
        state = pltpu.VMEM((ROWS, COLS), F32)
        dma = pltpu.SemaphoreType.DMA
        results = pl.pallas_call(
            kernel,
            name="lamb",
            out_shape=(pltpu.VMEM((ROWS, DATA * COLS), BF16), state, state, state),
            in_specs=[any_spec] * 4,
            out_specs=[vmem_spec] * 4,
            scratch_shapes=[
                pltpu.VMEM((ROWS, COLS), F32),
                pltpu.VMEM((ROWS, COLS), F32),
                pltpu.VMEM((DEVICES, 8, 128), F32),
                pltpu.VMEM((DEVICES, 1, 128), F32),
                pltpu.VMEM((DEVICES, 1, 128), F32),
                pltpu.VMEM((2, DEVICES, 8, 128), F32),
                pltpu.VMEM((ROWS // 8, 8, 128), F32),
                dma((3,)),
                dma((2, RS_CHUNKS)),
                dma((2,)),
                dma((2, RS_CHUNKS)),
                dma((2,)),
                dma((5,)),
                dma((5,)),
                dma((AG_CHUNKS,)),
                dma((AG_CHUNKS,)),
                dma((AG_CHUNKS,)),
                dma,
                dma((3,)),
                pltpu.SemaphoreType.REGULAR,
            ],
            compiler_params=pltpu.CompilerParams(collective_id=0, has_side_effects=True, vmem_limit_bytes=16 << 20),
        )(local_grads, master, moment_one, moment_two)
        written = []
        for group, parts in ((results[:1], 12), (results[1:], 4)):
            written += pl.pallas_call(
                functools.partial(write_out, parts),
                name="write_out",
                out_shape=[jax.ShapeDtypeStruct(value.shape, value.dtype) for value in group],
                in_specs=[vmem_spec] * len(group),
                out_specs=[any_spec] * len(group),
                scratch_shapes=[dma((len(group) * parts,))],
                compiler_params=pltpu.CompilerParams(vmem_limit_bytes=1 << 20),
            )(*group)
        return tuple(written)

    state_spec = P(None, ('model', 'data'))
    return jax.shard_map(device_step, mesh=mesh, in_specs=(P('data', None, 'model'), state_spec, state_spec, state_spec), out_specs=(P(None, 'model'), state_spec, state_spec, state_spec), check_vma=False)
```

```python
import jax
import jax.numpy as jnp
from jax import lax
from jax.experimental import pallas as pl
from jax.experimental.pallas import tpu as pltpu
from jax.sharding import PartitionSpec as P

STEP = 4
LEARN_RATE = 0.08
BETA_ONE = 0.9
BETA_TWO = 0.999
EPSILON = 1e-6
WEIGHT_DECAY = 0.01
MAX_NORM = 1.0
CORR_ONE = 1.0 - BETA_ONE ** STEP
CORR_TWO = 1.0 - BETA_TWO ** STEP

ROWS = 384
HALF = 192
COLS = 4096
DATA = 8
DEVICES = 16
PIECE = 1024
PIECES = COLS // PIECE
ADAM_PIECE = 1024
OUT_PARTS = 6
VMEM_LIMIT = 16 << 20

RS_SIZES = (48, 48, 48, 32, 16)
RS_CHUNKS = len(RS_SIZES)
RS_STARTS = tuple(sum(RS_SIZES[:i]) for i in range(RS_CHUNKS))
AG_SIZES = (16,) + (32,) * 10 + (16,) * 3
AG_FAR_BY_Y = (1,) + (0, 1) * 5 + (0, 1, 0)
AG_CHUNKS = len(AG_SIZES)
AG_STARTS = tuple(sum(AG_SIZES[:i]) for i in range(AG_CHUNKS))
NORM_CHUNKS = ((0, 16), (16, 208), (208, 384))

MESH = pl.DeviceIdType.MESH
F32 = jnp.float32
BF16 = jnp.bfloat16


def fold_lanes(values):
    total = values[:, 0:128]
    for group in range(1, values.shape[1] // 128):
        total = total + values[:, group * 128:(group + 1) * 128]
    return total


def tensor_total(tile):
    row = [tile[s:s + 1, :] for s in range(8)]
    first3 = row[0] + row[1] + row[2]
    first4 = first3 + row[3]
    mid3 = row[4] + row[5] + row[6]
    last4 = mid3 + row[7]
    sub = lax.broadcasted_iota(jnp.int32, (8, 128), 0)
    kind = lax.broadcasted_iota(jnp.int32, (8, 128), 1) % 3
    full = lambda value: jnp.broadcast_to(value, (8, 128))
    low = jnp.where(kind == 0, jnp.where(sub == 3, full(row[3]), full(first3)), full(first4))
    high = jnp.where(kind == 1, jnp.where(sub == 7, full(row[7]), full(mid3)), full(last4))
    return jnp.where(sub < 4, low, high)


def first_totals(row):
    lane = lax.broadcasted_iota(jnp.int32, (8, 128), 1)
    sub = lax.broadcasted_iota(jnp.int32, (8, 128), 0)
    tile = jnp.zeros((8, 128), F32)
    for group in range(NORM_CHUNKS[0][1] // 8):
        low, high = ((3, 4), (4, 7), (4, 8))[group % 3]
        part = lambda s: (s >= low).astype(jnp.int32) + (s >= high).astype(jnp.int32)
        same = (lane // 8 == group) & (part(sub) == part(lane % 8))
        total = jnp.sum(jnp.where(same, jnp.broadcast_to(row, (8, 128)), 0.0), axis=1, keepdims=True)
        tile = jnp.where(lane == group, total, tile)
    return tile


def kernel(grad_ref, master_ref, one_ref, two_ref, params, master, one, two, relay, grad, weight_buf, norm_buf, first_buf, sq_buf, part_buf,
           load_sem, rs_recv, rs_send, hop_recv, hop_send, ex_recv, ex_send, ag_x, ag_y, ag_d, ag_o, ag_send, plane_sem):
    model = lax.axis_index("model")
    me = lax.axis_index("data")
    linear = model * DATA + me
    core = me % 2
    x = (me // 2) % 2
    y = me // 4
    to_core = 1 - 2 * core
    near_x = me + 2 - 4 * x
    near_y = me + 4 - 8 * y
    diag = near_x + 4 - 8 * y
    other = me + to_core
    peer = lambda index: {"model": model, "data": index}
    block = lambda index: pl.ds(pl.multiple_of(index * COLS, COLS), COLS)

    loads = [pltpu.make_async_copy(source, target, load_sem.at[i])
             for i, (source, target) in enumerate(((master_ref, master), (one_ref, one), (two_ref, two)))]

    first = (near_x, near_y)
    second = (near_y, near_x)

    def rows_of(half, chunk):
        return pl.ds(half * HALF + RS_STARTS[chunk], RS_SIZES[chunk])

    barrier = pltpu.get_barrier_semaphore()

    mirror = {"model": 1 - model, "data": me}
    for neighbour in (peer(near_x), peer(near_x + to_core), peer(near_y), peer(near_y + to_core), mirror, peer(other)):
        pl.semaphore_signal(barrier, inc=1, device_id=neighbour, device_id_type=MESH)
    pl.semaphore_wait(barrier, 6)

    def remote(source, target, send, recv, index):
        return pltpu.make_async_remote_copy(src_ref=source, dst_ref=target, send_sem=send, recv_sem=recv,
                                            device_id=peer(index), device_id_type=MESH)

    for chunk in range(RS_CHUNKS):
        for half in range(2):
            rows = rows_of(half, chunk)
            recv = rs_recv.at[half, chunk]
            send = rs_send.at[half]
            for turn in range(2):
                shift = turn * to_core
                for part, owner in enumerate((first[half] + shift, diag + shift)):
                    remote(grad_ref.at[0, rows, block(owner)], params.at[rows, pl.ds((4 + 2 * turn + part) * COLS, COLS)], send, recv, first[half] + shift).start()
            for part, owner in enumerate((other, second[half] + to_core)):
                remote(grad_ref.at[0, rows, block(owner)], params.at[rows, pl.ds((2 + part) * COLS, COLS)], send, recv, other).start()

    def load_own(chunk):
        for half in range(2):
            rows = rows_of(half, chunk)
            for part, owner in enumerate((me, second[half])):
                pltpu.make_async_copy(grad_ref.at[0, rows, block(owner)], params.at[rows, pl.ds(part * COLS, COLS)], rs_recv.at[half, chunk]).start()

    load_own(0)

    lane = lax.broadcasted_iota(jnp.int32, (8, 128), 1)
    sub = lax.broadcasted_iota(jnp.int32, (8, 128), 0)

    def weight_rows(group, tile):
        rows = pl.ds(pl.multiple_of(group * 8, 8), 8)

        def piece(i, total):
            value = master[rows, pl.ds(pl.multiple_of(i * PIECE, PIECE), PIECE)]
            return total + fold_lanes(value * value)

        total = lax.fori_loop(0, PIECES, piece, jnp.zeros((8, 128), F32))
        return jnp.where(lane == group, jnp.sum(total, axis=1, keepdims=True), tile)


    def exchange(buf, number):
        for flips in reversed(range(1, DEVICES)):
            to_model, to_y, to_x, to_core = [at + (1 - 2 * at) * (flips >> bit & 1) for bit, at in zip((3, 2, 1, 0), (model, y, x, core))]
            pltpu.make_async_remote_copy(src_ref=buf.at[linear], dst_ref=buf.at[linear], send_sem=ex_send.at[number], recv_sem=ex_recv.at[number],
                                         device_id={"model": to_model, "data": to_y * 4 + to_x * 2 + to_core}, device_id_type=MESH).start()

    def exchange_wait(buf, sem):
        others = buf.at[pl.ds(0, DEVICES - 1)]
        pltpu.make_async_copy(others, others, sem).wait()

    def gathered(buf):
        total = buf[0]
        for index in range(1, DEVICES):
            total = total + buf[index]
        return total

    EX_WEIGHT, EX_GRAD, EX_FIRST = range(3)

    def decay(state, factor):
        @pl.loop(0, ROWS // 8 * PIECES)
        def _(step):
            rows = pl.ds(pl.multiple_of(step // PIECES * 8, 8), 8)
            cols = pl.ds(pl.multiple_of(step % PIECES * PIECE, PIECE), PIECE)
            state[rows, cols] = state[rows, cols] * factor

    def four(rows, cols_at, part):
        total = params[rows, pl.ds(pl.multiple_of(part * COLS + cols_at, PIECE), PIECE)].astype(F32)
        for source in range(1, 4):
            total = total + params[rows, pl.ds(pl.multiple_of((2 * source + part) * COLS + cols_at, PIECE), PIECE)].astype(F32)
        return total

    def hop(half, chunk):
        rows = rows_of(half, chunk)
        return remote(relay.at[rows], grad.at[rows], hop_send.at[half], hop_recv.at[half, chunk], second[half])

    for chunk in range(RS_CHUNKS):
        for half in range(2):
            rows = rows_of(half, chunk)
            whole = params.at[rows]
            pltpu.make_async_copy(whole, whole, rs_recv.at[half, chunk]).wait()

            @pl.loop(0, RS_SIZES[chunk] // 16 * PIECES)
            def _(step):
                tile_rows = pl.ds(pl.multiple_of(half * HALF + RS_STARTS[chunk] + step // PIECES * 16, 16), 16)
                cols_at = step % PIECES * PIECE
                relay[tile_rows, pl.ds(pl.multiple_of(cols_at, PIECE), PIECE)] = four(tile_rows, cols_at, 1)

            hop(half, chunk).start()
        if chunk == 0:
            pl.semaphore_signal(plane_sem, inc=1, device_id=mirror, device_id_type=MESH)
        if chunk + 1 < RS_CHUNKS:
            load_own(chunk + 1)
        if chunk < 3:
            loads[chunk].start()
        if chunk == 1:
            loads[0].wait()
            weight_buf[linear] = lax.fori_loop(0, ROWS // 8, weight_rows, jnp.zeros((8, 128), F32))
        if chunk == 2:
            pl.semaphore_wait(plane_sem, 1)
            exchange(weight_buf, EX_WEIGHT)
            loads[1].wait()
            decay(one, BETA_ONE)
        if chunk == 3:
            loads[2].wait()
            decay(two, BETA_TWO)

    square = jnp.zeros((8, 128), F32)
    for chunk in range(RS_CHUNKS):
        for half in range(2):
            hop(half, chunk).wait_recv()

            def finish(step, total):
                tile_rows = pl.ds(pl.multiple_of(half * HALF + RS_STARTS[chunk] + step // PIECES * 16, 16), 16)
                cols_at = step % PIECES * PIECE
                cols = pl.ds(pl.multiple_of(cols_at, PIECE), PIECE)
                value = (grad[tile_rows, cols] + four(tile_rows, cols_at, 0)) * (1.0 / DATA)
                grad[tile_rows, cols] = value
                folded = fold_lanes(value * value)
                return total + (folded[0:8] + folded[8:16])

            square = lax.fori_loop(0, RS_SIZES[chunk] // 16 * PIECES, finish, square)

    norm_buf[linear] = jnp.sum(square, axis=0, keepdims=True)
    exchange(norm_buf, EX_GRAD)
    for half in range(2):
        rows = pl.ds(half * HALF, HALF)
        pltpu.make_async_copy(relay.at[rows], relay.at[rows], hop_send.at[half]).wait()
    exchange_wait(weight_buf, ex_recv.at[EX_WEIGHT])
    weight_norm = jnp.sqrt(tensor_total(gathered(weight_buf)))
    exchange_wait(norm_buf, ex_recv.at[EX_GRAD])
    grad_norm = jnp.sqrt(jnp.sum(gathered(norm_buf), axis=1, keepdims=True))
    clip = jnp.minimum(1.0, MAX_NORM / grad_norm)

    grad_one = (1.0 - BETA_ONE) * clip
    grad_two = (1.0 - BETA_TWO) ** 0.5 * clip

    def adam(start, stop):
        @pl.loop(start, stop)
        def _(group):
            rows = pl.ds(pl.multiple_of(group * 8, 8), 8)
            total = jnp.zeros((8, 128), F32)
            for i in range(COLS // ADAM_PIECE):
                cols = pl.ds(i * ADAM_PIECE, ADAM_PIECE)
                mean = grad[rows, cols]
                new_one = one[rows, cols] + grad_one * mean
                scaled = grad_two * mean
                new_two = two[rows, cols] + scaled * scaled
                one[rows, cols] = new_one
                two[rows, cols] = new_two
                direction = new_one / (jnp.sqrt(new_two) * (CORR_ONE / CORR_TWO ** 0.5) + CORR_ONE * EPSILON) + WEIGHT_DECAY * master[rows, cols]
                relay[rows, cols] = direction
                total = total + fold_lanes(direction * direction)
            part_buf[group] = total

    def row_sums(start, stop, place):
        tile = jnp.zeros((8, 128), F32)
        for group in range(start, stop):
            tile = jnp.where(lane == place(group), jnp.sum(part_buf[group], axis=1, keepdims=True), tile)
        return tile

    def step_rates(number):
        if number == 0:
            exchange_wait(first_buf, ex_recv.at[EX_FIRST])
            total = first_totals(gathered(first_buf))
        else:
            exchange_wait(sq_buf.at[number - 1], ex_recv.at[EX_FIRST + number])
            total = tensor_total(gathered(sq_buf.at[number - 1]))
        return weight_norm / jnp.sqrt(total) * LEARN_RATE

    def ag_rows(chunk):
        return pl.ds(AG_STARTS[chunk], AG_SIZES[chunk])

    def update(number, rates):
        start, stop = NORM_CHUNKS[number]
        for chunk in range(AG_CHUNKS):
            if not start <= AG_STARTS[chunk] < stop:
                continue

            @pl.loop(0, AG_SIZES[chunk] // 16)
            def _(tile):
                group = AG_STARTS[chunk] // 8 + 2 * tile
                rows = pl.ds(pl.multiple_of(AG_STARTS[chunk] + tile * 16, 16), 16)
                rate = jnp.concatenate([jnp.sum(jnp.where(lane == group + i, rates, 0.0), axis=1, keepdims=True) for i in range(2)], axis=0)

                @pl.loop(0, PIECES)
                def _(i):
                    cols = pl.ds(pl.multiple_of(i * PIECE, PIECE), PIECE)
                    value = master[rows, cols] - rate * relay[rows, cols]
                    master[rows, cols] = value
                    params[rows, pl.ds(pl.multiple_of(me * COLS + i * PIECE, PIECE), PIECE)] = value.astype(BF16)

            rows = ag_rows(chunk)
            own = params.at[rows, block(me)]
            remote(own, own, ag_send.at[0], ag_x.at[chunk], near_x).start()
            remote(own, own, ag_send.at[1], ag_y.at[chunk], near_y).start()
            remote(own, own, ag_send.at[2], ag_o, other).start()

    groups = [(start // 8, stop // 8) for start, stop in NORM_CHUNKS]
    adam(*groups[0])
    first_buf[linear] = jnp.sum(row_sums(*groups[0], lambda group: 8 * group + sub), axis=0, keepdims=True)
    adam(groups[1][0], groups[1][0] + 1)
    exchange(first_buf, EX_FIRST)
    adam(groups[1][0] + 1, groups[1][1])
    sq_buf[0, linear] = row_sums(*groups[1], lambda group: group)
    adam(groups[2][0], groups[2][0] + 1)
    exchange(sq_buf.at[0], EX_FIRST + 1)
    update(0, step_rates(0))
    adam(groups[2][0] + 1, groups[2][1])
    sq_buf[1, linear] = row_sums(*groups[2], lambda group: group)
    rates = step_rates(1)
    exchange(sq_buf.at[1], EX_FIRST + 2)
    update(1, rates)
    update(2, step_rates(2))

    def arrived(sem, source, rows):
        view = params.at[rows, block(source)]
        pltpu.make_async_copy(view, view, sem).wait()
        return view

    for chunk in range(AG_CHUNKS):
        rows = ag_rows(chunk)
        view = arrived(ag_x.at[chunk], near_x, rows)
        if AG_FAR_BY_Y[chunk]:
            remote(view, view, ag_send.at[1], ag_d.at[chunk], near_y).start()
        remote(view, view, ag_send.at[2], ag_o, other).start()
        view = arrived(ag_y.at[chunk], near_y, rows)
        if not AG_FAR_BY_Y[chunk]:
            remote(view, view, ag_send.at[0], ag_d.at[chunk], near_x).start()
        remote(view, view, ag_send.at[2], ag_o, other).start()

    for chunk in range(AG_CHUNKS):
        view = arrived(ag_d.at[chunk], diag, ag_rows(chunk))
        remote(view, view, ag_send.at[2], ag_o, other).start()

    half_cols = params.at[:, pl.ds(0, DATA // 2 * COLS)]
    pltpu.make_async_copy(half_cols, half_cols, ag_o).wait()
    pltpu.make_async_copy(half_cols, half_cols, ag_send.at[2]).wait()
    for direction in range(2):
        for part in (pl.ds(0, ROWS), pl.ds(0, HALF)):
            view = params.at[part, pl.ds(0, COLS)]
            pltpu.make_async_copy(view, view, ag_send.at[direction]).wait()
    for half in range(2):
        view = params.at[pl.ds(0, HALF), pl.ds(0, 6 * COLS)]
        pltpu.make_async_copy(view, view, rs_send.at[half]).wait()
    exchange_wait(weight_buf, ex_send.at[EX_WEIGHT])
    exchange_wait(norm_buf, ex_send.at[EX_GRAD])
    exchange_wait(first_buf, ex_send.at[EX_FIRST])
    for number in range(2):
        exchange_wait(sq_buf.at[number], ex_send.at[EX_FIRST + 1 + number])


def write_out(*refs):
    count = len(refs) // 2
    sem = refs[-1]
    copies = []
    for part in range(OUT_PARTS):
        rows = pl.ds(part * (ROWS // OUT_PARTS), ROWS // OUT_PARTS)
        for source, target in zip(refs[:count], refs[count:-1]):
            copies.append(pltpu.make_async_copy(source.at[rows], target.at[rows], sem.at[len(copies)]))
    for number, copy in enumerate(copies):
        copy.start(priority=number % 2)
    for copy in copies:
        copy.wait()


def solution(mesh):
    def device_step(local_grads, master, moment_one, moment_two):
        any_spec = pl.BlockSpec(memory_space=pl.ANY)
        vmem_spec = pl.BlockSpec(memory_space=pltpu.VMEM)
        state = pltpu.VMEM((ROWS, COLS), F32)
        dma = pltpu.SemaphoreType.DMA
        results = pl.pallas_call(
            kernel,
            name="lamb",
            out_shape=(pltpu.VMEM((ROWS, DATA * COLS), BF16), state, state, state),
            in_specs=[any_spec] * 4,
            out_specs=[vmem_spec] * 4,
            scratch_shapes=[
                pltpu.VMEM((ROWS, COLS), F32),
                pltpu.VMEM((ROWS, COLS), F32),
                pltpu.VMEM((DEVICES, 8, 128), F32),
                pltpu.VMEM((DEVICES, 1, 128), F32),
                pltpu.VMEM((DEVICES, 1, 128), F32),
                pltpu.VMEM((2, DEVICES, 8, 128), F32),
                pltpu.VMEM((ROWS // 8, 8, 128), F32),
                dma((3,)),
                dma((2, RS_CHUNKS)),
                dma((2,)),
                dma((2, RS_CHUNKS)),
                dma((2,)),
                dma((5,)),
                dma((5,)),
                dma((AG_CHUNKS,)),
                dma((AG_CHUNKS,)),
                dma((AG_CHUNKS,)),
                dma,
                dma((3,)),
                pltpu.SemaphoreType.REGULAR,
            ],
            compiler_params=pltpu.CompilerParams(collective_id=0, has_side_effects=True, vmem_limit_bytes=VMEM_LIMIT),
        )(local_grads, master, moment_one, moment_two)
        results = [pltpu.with_memory_space_constraint(value, pltpu.VMEM) for value in results]
        return tuple(pl.pallas_call(
            write_out,
            name="write_out",
            out_shape=[jax.ShapeDtypeStruct(value.shape, value.dtype) for value in results],
            in_specs=[vmem_spec] * 4,
            out_specs=[any_spec] * 4,
            scratch_shapes=[dma((4 * OUT_PARTS,))],
            compiler_params=pltpu.CompilerParams(vmem_limit_bytes=VMEM_LIMIT),
        )(*results))

    state_spec = P(None, ('model', 'data'))
    return jax.shard_map(device_step, mesh=mesh, in_specs=(P('data', None, 'model'), state_spec, state_spec, state_spec), out_specs=(P(None, 'model'), state_spec, state_spec, state_spec), check_vma=False)
```

```python
import jax
import jax.numpy as jnp
from jax import lax
from jax.experimental import pallas as pl
from jax.experimental.pallas import tpu as pltpu
from jax.sharding import PartitionSpec as P

STEP = 4
LEARN_RATE = 0.08
BETA_ONE = 0.9
BETA_TWO = 0.999
EPSILON = 1e-6
WEIGHT_DECAY = 0.01
MAX_NORM = 1.0
CORR_ONE = 1.0 - BETA_ONE ** STEP
CORR_TWO = 1.0 - BETA_TWO ** STEP

ROWS = 384
HALF = 192
COLS = 4096
DATA = 8
DEVICES = 16
PIECE = 1024
PIECES = COLS // PIECE
ADAM_PIECE = 1024
LEAD = 16
EARLY = 2048
OUT_PARTS = 6
VMEM_LIMIT = 16 << 20

RS_SIZES = (48, 48, 48, 32, 16)
RS_CHUNKS = len(RS_SIZES)
RS_STARTS = tuple(sum(RS_SIZES[:i]) for i in range(RS_CHUNKS))
AG_SIZES = (16,) + (32,) * 10 + (16,) * 3
AG_FAR_BY_Y = (1,) + (0, 1) * 5 + (0, 1, 0)
AG_CHUNKS = len(AG_SIZES)
AG_STARTS = tuple(sum(AG_SIZES[:i]) for i in range(AG_CHUNKS))
NORM_CHUNKS = ((0, 16), (16, 208), (208, 384))

MESH = pl.DeviceIdType.MESH
F32 = jnp.float32
BF16 = jnp.bfloat16


def fold_lanes(values):
    total = values[:, 0:128]
    for group in range(1, values.shape[1] // 128):
        total = total + values[:, group * 128:(group + 1) * 128]
    return total


def tensor_total(tile):
    row = [tile[s:s + 1, :] for s in range(8)]
    first3 = row[0] + row[1] + row[2]
    first4 = first3 + row[3]
    mid3 = row[4] + row[5] + row[6]
    last4 = mid3 + row[7]
    sub = lax.broadcasted_iota(jnp.int32, (8, 128), 0)
    kind = lax.broadcasted_iota(jnp.int32, (8, 128), 1) % 3
    full = lambda value: jnp.broadcast_to(value, (8, 128))
    low = jnp.where(kind == 0, jnp.where(sub == 3, full(row[3]), full(first3)), full(first4))
    high = jnp.where(kind == 1, jnp.where(sub == 7, full(row[7]), full(mid3)), full(last4))
    return jnp.where(sub < 4, low, high)


def first_totals(row):
    lane = lax.broadcasted_iota(jnp.int32, (8, 128), 1)
    sub = lax.broadcasted_iota(jnp.int32, (8, 128), 0)
    tile = jnp.zeros((8, 128), F32)
    for group in range(NORM_CHUNKS[0][1] // 8):
        low, high = ((3, 4), (4, 7), (4, 8))[group % 3]
        part = lambda s: (s >= low).astype(jnp.int32) + (s >= high).astype(jnp.int32)
        same = (lane // 8 == group) & (part(sub) == part(lane % 8))
        total = jnp.sum(jnp.where(same, jnp.broadcast_to(row, (8, 128)), 0.0), axis=1, keepdims=True)
        tile = jnp.where(lane == group, total, tile)
    return tile


def kernel(grad_ref, master_ref, one_ref, two_ref, params, master, one, two, relay, grad, weight_buf, norm_buf, first_buf, sq_buf, part_buf, lead, early,
           load_sem, rs_recv, rs_send, hop_recv, hop_send, ex_recv, ex_send, ag_x, ag_y, ag_d, ag_o, ag_send, plane_sem,
           lead_sem, early_recv, early_send):
    model = lax.axis_index("model")
    me = lax.axis_index("data")
    linear = model * DATA + me
    core = me % 2
    x = (me // 2) % 2
    y = me // 4
    to_core = 1 - 2 * core
    near_x = me + 2 - 4 * x
    near_y = me + 4 - 8 * y
    diag = near_x + 4 - 8 * y
    other = me + to_core
    peer = lambda index: {"model": model, "data": index}
    block = lambda index: pl.ds(pl.multiple_of(index * COLS, COLS), COLS)

    loads = [pltpu.make_async_copy(source, target, load_sem.at[i])
             for i, (source, target) in enumerate(((master_ref, master), (one_ref, one), (two_ref, two)))]

    first = (near_x, near_y)
    second = (near_y, near_x)

    def rows_of(half, chunk):
        return pl.ds(half * HALF + RS_STARTS[chunk], RS_SIZES[chunk])

    leads = [pltpu.make_async_copy(grad_ref.at[0, pl.ds(half * HALF, LEAD), block(first[half])], lead.at[half], lead_sem.at[half]) for half in range(2)]
    for copy in leads:
        copy.start()

    barrier = pltpu.get_barrier_semaphore()

    mirror = {"model": 1 - model, "data": me}
    for neighbour in (peer(near_x), peer(near_x + to_core), peer(near_y), peer(near_y + to_core), mirror, peer(other)):
        pl.semaphore_signal(barrier, inc=1, device_id=neighbour, device_id_type=MESH)
    pl.semaphore_wait(barrier, 6)

    def remote(source, target, send, recv, index):
        return pltpu.make_async_remote_copy(src_ref=source, dst_ref=target, send_sem=send, recv_sem=recv,
                                            device_id=peer(index), device_id_type=MESH)

    for chunk in range(RS_CHUNKS):
        for half in range(2):
            rows = rows_of(half, chunk)
            recv = rs_recv.at[half, chunk]
            send = rs_send.at[half]
            for turn in range(2):
                shift = turn * to_core
                for part, owner in enumerate((first[half] + shift, diag + shift)):
                    place = pl.ds((4 + 2 * turn + part) * COLS, COLS)
                    sent = rows
                    if (chunk, turn, part) == (0, 0, 0):
                        leads[half].wait()
                        remote(lead.at[half], params.at[pl.ds(half * HALF, LEAD), place], send, recv, first[half]).start()
                        sent = pl.ds(half * HALF + LEAD, RS_SIZES[0] - LEAD)
                    remote(grad_ref.at[0, sent, block(owner)], params.at[sent, place], send, recv, first[half] + shift).start()
            for part, owner in enumerate((other, second[half] + to_core)):
                remote(grad_ref.at[0, rows, block(owner)], params.at[rows, pl.ds((2 + part) * COLS, COLS)], send, recv, other).start()

    def load_own(chunk):
        for half in range(2):
            rows = rows_of(half, chunk)
            for part, owner in enumerate((me, second[half])):
                pltpu.make_async_copy(grad_ref.at[0, rows, block(owner)], params.at[rows, pl.ds(part * COLS, COLS)], rs_recv.at[half, chunk]).start()

    load_own(0)

    lane = lax.broadcasted_iota(jnp.int32, (8, 128), 1)
    sub = lax.broadcasted_iota(jnp.int32, (8, 128), 0)

    def weight_rows(group, tile):
        rows = pl.ds(pl.multiple_of(group * 8, 8), 8)

        def piece(i, total):
            value = master[rows, pl.ds(pl.multiple_of(i * PIECE, PIECE), PIECE)]
            return total + fold_lanes(value * value)

        total = lax.fori_loop(0, PIECES, piece, jnp.zeros((8, 128), F32))
        return jnp.where(lane == group, jnp.sum(total, axis=1, keepdims=True), tile)


    def exchange(buf, number):
        for flips in reversed(range(1, DEVICES)):
            to_model, to_y, to_x, to_core = [at + (1 - 2 * at) * (flips >> bit & 1) for bit, at in zip((3, 2, 1, 0), (model, y, x, core))]
            pltpu.make_async_remote_copy(src_ref=buf.at[linear], dst_ref=buf.at[linear], send_sem=ex_send.at[number], recv_sem=ex_recv.at[number],
                                         device_id={"model": to_model, "data": to_y * 4 + to_x * 2 + to_core}, device_id_type=MESH).start()

    def exchange_wait(buf, sem):
        others = buf.at[pl.ds(0, DEVICES - 1)]
        pltpu.make_async_copy(others, others, sem).wait()

    def gathered(buf):
        total = buf[0]
        for index in range(1, DEVICES):
            total = total + buf[index]
        return total

    EX_WEIGHT, EX_GRAD, EX_FIRST = range(3)

    def decay(state, factor):
        @pl.loop(0, ROWS // 8 * PIECES)
        def _(step):
            rows = pl.ds(pl.multiple_of(step // PIECES * 8, 8), 8)
            cols = pl.ds(pl.multiple_of(step % PIECES * PIECE, PIECE), PIECE)
            state[rows, cols] = state[rows, cols] * factor

    def four(rows, cols_at, part):
        total = params[rows, pl.ds(pl.multiple_of(part * COLS + cols_at, PIECE), PIECE)].astype(F32)
        for source in range(1, 4):
            total = total + params[rows, pl.ds(pl.multiple_of((2 * source + part) * COLS + cols_at, PIECE), PIECE)].astype(F32)
        return total

    def hop(half, chunk):
        rows = rows_of(half, chunk)
        return remote(relay.at[rows], grad.at[rows], hop_send.at[half], hop_recv.at[half, chunk], second[half])

    for chunk in range(RS_CHUNKS):
        for half in range(2):
            rows = rows_of(half, chunk)
            whole = params.at[rows]
            pltpu.make_async_copy(whole, whole, rs_recv.at[half, chunk]).wait()

            @pl.loop(0, RS_SIZES[chunk] // 16 * PIECES)
            def _(step):
                tile_rows = pl.ds(pl.multiple_of(half * HALF + RS_STARTS[chunk] + step // PIECES * 16, 16), 16)
                cols_at = step % PIECES * PIECE
                relay[tile_rows, pl.ds(pl.multiple_of(cols_at, PIECE), PIECE)] = four(tile_rows, cols_at, 1)

            hop(half, chunk).start()
        if chunk == 0:
            pl.semaphore_signal(plane_sem, inc=1, device_id=mirror, device_id_type=MESH)
        if chunk + 1 < RS_CHUNKS:
            load_own(chunk + 1)
        if chunk < 3:
            loads[chunk].start()
        if chunk == 1:
            loads[0].wait()
            weight_buf[linear] = lax.fori_loop(0, ROWS // 8, weight_rows, jnp.zeros((8, 128), F32))
        if chunk == 2:
            pl.semaphore_wait(plane_sem, 1)
            exchange(weight_buf, EX_WEIGHT)
            loads[1].wait()
            decay(one, BETA_ONE)
        if chunk == 3:
            loads[2].wait()
            decay(two, BETA_TWO)

    square = jnp.zeros((8, 128), F32)
    for chunk in range(RS_CHUNKS):
        for half in range(2):
            hop(half, chunk).wait_recv()

            def finish(step, total):
                tile_rows = pl.ds(pl.multiple_of(half * HALF + RS_STARTS[chunk] + step // PIECES * 16, 16), 16)
                cols_at = step % PIECES * PIECE
                cols = pl.ds(pl.multiple_of(cols_at, PIECE), PIECE)
                value = (grad[tile_rows, cols] + four(tile_rows, cols_at, 0)) * (1.0 / DATA)
                grad[tile_rows, cols] = value
                folded = fold_lanes(value * value)
                return total + (folded[0:8] + folded[8:16])

            square = lax.fori_loop(0, RS_SIZES[chunk] // 16 * PIECES, finish, square)

    norm_buf[linear] = jnp.sum(square, axis=0, keepdims=True)
    def send_early(kind, source):
        for side, near in enumerate((near_x, near_y)):
            remote(source.at[pl.ds(0, 16), pl.ds(0, EARLY)], early.at[kind, side], early_send.at[kind, side], early_recv.at[kind, side], near).start()

    def early_wait(sem, kind):
        for side in range(2):
            view = early.at[kind, side]
            pltpu.make_async_copy(view, view, sem.at[kind, side]).wait()

    exchange(norm_buf, EX_GRAD)
    send_early(0, master)
    for half in range(2):
        rows = pl.ds(half * HALF, HALF)
        pltpu.make_async_copy(relay.at[rows], relay.at[rows], hop_send.at[half]).wait()
    exchange_wait(weight_buf, ex_recv.at[EX_WEIGHT])
    weight_norm = jnp.sqrt(tensor_total(gathered(weight_buf)))
    exchange_wait(norm_buf, ex_recv.at[EX_GRAD])
    grad_norm = jnp.sqrt(jnp.sum(gathered(norm_buf), axis=1, keepdims=True))
    clip = jnp.minimum(1.0, MAX_NORM / grad_norm)

    grad_one = (1.0 - BETA_ONE) * clip
    grad_two = (1.0 - BETA_TWO) ** 0.5 * clip

    def adam(start, stop):
        @pl.loop(start, stop)
        def _(group):
            rows = pl.ds(pl.multiple_of(group * 8, 8), 8)
            total = jnp.zeros((8, 128), F32)
            for i in range(COLS // ADAM_PIECE):
                cols = pl.ds(i * ADAM_PIECE, ADAM_PIECE)
                mean = grad[rows, cols]
                new_one = one[rows, cols] + grad_one * mean
                scaled = grad_two * mean
                new_two = two[rows, cols] + scaled * scaled
                one[rows, cols] = new_one
                two[rows, cols] = new_two
                direction = new_one / (jnp.sqrt(new_two) * (CORR_ONE / CORR_TWO ** 0.5) + CORR_ONE * EPSILON) + WEIGHT_DECAY * master[rows, cols]
                relay[rows, cols] = direction
                total = total + fold_lanes(direction * direction)
            part_buf[group] = total

    def row_sums(start, stop, place):
        tile = jnp.zeros((8, 128), F32)
        for group in range(start, stop):
            tile = jnp.where(lane == place(group), jnp.sum(part_buf[group], axis=1, keepdims=True), tile)
        return tile

    def step_rates(number):
        if number == 0:
            exchange_wait(first_buf, ex_recv.at[EX_FIRST])
            total = first_totals(gathered(first_buf))
        else:
            exchange_wait(sq_buf.at[number - 1], ex_recv.at[EX_FIRST + number])
            total = tensor_total(gathered(sq_buf.at[number - 1]))
        return weight_norm / jnp.sqrt(total) * LEARN_RATE

    def ag_rows(chunk):
        return pl.ds(AG_STARTS[chunk], AG_SIZES[chunk])

    def rate_column(rates, group):
        return jnp.concatenate([jnp.sum(jnp.where(lane == group + i, rates, 0.0), axis=1, keepdims=True) for i in range(2)], axis=0)

    def late_part(chunk, source):
        return params.at[ag_rows(chunk), pl.ds(pl.multiple_of(source * COLS + EARLY, EARLY), COLS - EARLY)]

    def update(number, rates):
        start, stop = NORM_CHUNKS[number]
        for chunk in range(AG_CHUNKS):
            if not start <= AG_STARTS[chunk] < stop:
                continue

            @pl.loop(0, AG_SIZES[chunk] // 16)
            def _(tile):
                group = AG_STARTS[chunk] // 8 + 2 * tile
                rows = pl.ds(pl.multiple_of(AG_STARTS[chunk] + tile * 16, 16), 16)
                rate = rate_column(rates, group)

                @pl.loop(0, PIECES)
                def _(i):
                    cols = pl.ds(pl.multiple_of(i * PIECE, PIECE), PIECE)
                    value = master[rows, cols] - rate * relay[rows, cols]
                    master[rows, cols] = value
                    params[rows, pl.ds(pl.multiple_of(me * COLS + i * PIECE, PIECE), PIECE)] = value.astype(BF16)

            rows = ag_rows(chunk)
            own = params.at[rows, block(me)]
            near = late_part(chunk, me) if chunk == 0 else own
            remote(near, near, ag_send.at[0], ag_x.at[chunk], near_x).start()
            remote(near, near, ag_send.at[1], ag_y.at[chunk], near_y).start()
            remote(own, own, ag_send.at[2], ag_o, other).start()

    groups = [(start // 8, stop // 8) for start, stop in NORM_CHUNKS]
    adam(*groups[0])
    first_buf[linear] = jnp.sum(row_sums(*groups[0], lambda group: 8 * group + sub), axis=0, keepdims=True)
    adam(groups[1][0], groups[1][0] + 1)
    exchange(first_buf, EX_FIRST)
    send_early(1, relay)
    adam(groups[1][0] + 1, groups[1][1])
    sq_buf[0, linear] = row_sums(*groups[1], lambda group: group)
    adam(groups[2][0], groups[2][0] + 1)
    exchange(sq_buf.at[0], EX_FIRST + 1)
    first_rates = step_rates(0)
    early_wait(early_send, 0)
    update(0, first_rates)
    adam(groups[2][0] + 1, groups[2][1])
    sq_buf[1, linear] = row_sums(*groups[2], lambda group: group)
    rates = step_rates(1)
    exchange(sq_buf.at[1], EX_FIRST + 2)
    update(1, rates)
    rate = rate_column(first_rates, 0)
    for kind in range(2):
        early_wait(early_recv, kind)
    for side, near in enumerate((near_x, near_y)):
        @pl.loop(0, EARLY // PIECE)
        def _(i):
            cols = pl.ds(pl.multiple_of(i * PIECE, PIECE), PIECE)
            value = early[0, side, :, cols] - rate * early[1, side, :, cols]
            params[pl.ds(0, 16), pl.ds(pl.multiple_of(near * COLS + i * PIECE, PIECE), PIECE)] = value.astype(BF16)

    update(2, step_rates(2))

    def arrived(sem, source, chunk, early_part=False):
        view = late_part(chunk, source) if early_part else params.at[ag_rows(chunk), block(source)]
        pltpu.make_async_copy(view, view, sem).wait()
        return params.at[ag_rows(chunk), block(source)]

    for chunk in range(AG_CHUNKS):
        view = arrived(ag_x.at[chunk], near_x, chunk, chunk == 0)
        if AG_FAR_BY_Y[chunk]:
            remote(view, view, ag_send.at[1], ag_d.at[chunk], near_y).start()
        remote(view, view, ag_send.at[2], ag_o, other).start()
        view = arrived(ag_y.at[chunk], near_y, chunk, chunk == 0)
        if not AG_FAR_BY_Y[chunk]:
            remote(view, view, ag_send.at[0], ag_d.at[chunk], near_x).start()
        remote(view, view, ag_send.at[2], ag_o, other).start()

    for chunk in range(AG_CHUNKS):
        view = arrived(ag_d.at[chunk], diag, chunk)
        remote(view, view, ag_send.at[2], ag_o, other).start()

    half_cols = params.at[:, pl.ds(0, DATA // 2 * COLS)]
    pltpu.make_async_copy(half_cols, half_cols, ag_o).wait()
    pltpu.make_async_copy(half_cols, half_cols, ag_send.at[2]).wait()
    for direction in range(2):
        for rows, cols in ((ROWS - 16, COLS), (16, COLS - EARLY), (HALF, COLS)):
            view = params.at[pl.ds(0, rows), pl.ds(0, cols)]
            pltpu.make_async_copy(view, view, ag_send.at[direction]).wait()
    early_wait(early_send, 1)
    for half in range(2):
        view = params.at[pl.ds(0, HALF), pl.ds(0, 6 * COLS)]
        pltpu.make_async_copy(view, view, rs_send.at[half]).wait()
    exchange_wait(weight_buf, ex_send.at[EX_WEIGHT])
    exchange_wait(norm_buf, ex_send.at[EX_GRAD])
    exchange_wait(first_buf, ex_send.at[EX_FIRST])
    for number in range(2):
        exchange_wait(sq_buf.at[number], ex_send.at[EX_FIRST + 1 + number])


def write_out(*refs):
    count = len(refs) // 2
    sem = refs[-1]
    copies = []
    for part in range(OUT_PARTS):
        rows = pl.ds(part * (ROWS // OUT_PARTS), ROWS // OUT_PARTS)
        for source, target in zip(refs[:count], refs[count:-1]):
            copies.append(pltpu.make_async_copy(source.at[rows], target.at[rows], sem.at[len(copies)]))
    for number, copy in enumerate(copies):
        copy.start(priority=number % 2)
    for copy in copies:
        copy.wait()


def solution(mesh):
    def device_step(local_grads, master, moment_one, moment_two):
        any_spec = pl.BlockSpec(memory_space=pl.ANY)
        vmem_spec = pl.BlockSpec(memory_space=pltpu.VMEM)
        state = pltpu.VMEM((ROWS, COLS), F32)
        dma = pltpu.SemaphoreType.DMA
        results = pl.pallas_call(
            kernel,
            name="lamb",
            out_shape=(pltpu.VMEM((ROWS, DATA * COLS), BF16), state, state, state),
            in_specs=[any_spec] * 4,
            out_specs=[vmem_spec] * 4,
            scratch_shapes=[
                pltpu.VMEM((ROWS, COLS), F32),
                pltpu.VMEM((ROWS, COLS), F32),
                pltpu.VMEM((DEVICES, 8, 128), F32),
                pltpu.VMEM((DEVICES, 1, 128), F32),
                pltpu.VMEM((DEVICES, 1, 128), F32),
                pltpu.VMEM((2, DEVICES, 8, 128), F32),
                pltpu.VMEM((ROWS // 8, 8, 128), F32),
                pltpu.VMEM((2, LEAD, COLS), BF16),
                pltpu.VMEM((2, 2, 16, EARLY), F32),
                dma((3,)),
                dma((2, RS_CHUNKS)),
                dma((2,)),
                dma((2, RS_CHUNKS)),
                dma((2,)),
                dma((5,)),
                dma((5,)),
                dma((AG_CHUNKS,)),
                dma((AG_CHUNKS,)),
                dma((AG_CHUNKS,)),
                dma,
                dma((3,)),
                pltpu.SemaphoreType.REGULAR,
                dma((2,)),
                dma((2, 2)),
                dma((2, 2)),
            ],
            compiler_params=pltpu.CompilerParams(collective_id=0, has_side_effects=True, vmem_limit_bytes=VMEM_LIMIT),
        )(local_grads, master, moment_one, moment_two)
        results = [pltpu.with_memory_space_constraint(value, pltpu.VMEM) for value in results]
        return tuple(pl.pallas_call(
            write_out,
            name="write_out",
            out_shape=[jax.ShapeDtypeStruct(value.shape, value.dtype) for value in results],
            in_specs=[vmem_spec] * 4,
            out_specs=[any_spec] * 4,
            scratch_shapes=[dma((4 * OUT_PARTS,))],
            compiler_params=pltpu.CompilerParams(vmem_limit_bytes=VMEM_LIMIT),
        )(*results))

    state_spec = P(None, ('model', 'data'))
    return jax.shard_map(device_step, mesh=mesh, in_specs=(P('data', None, 'model'), state_spec, state_spec, state_spec), out_specs=(P(None, 'model'), state_spec, state_spec, state_spec), check_vma=False)
```

```python
import jax
import jax.numpy as jnp
from jax import lax
from jax.experimental import pallas as pl
from jax.experimental.pallas import tpu as pltpu
from jax.sharding import PartitionSpec as P

STEP = 4
LEARN_RATE = 0.08
BETA_ONE = 0.9
BETA_TWO = 0.999
EPSILON = 1e-6
WEIGHT_DECAY = 0.01
MAX_NORM = 1.0
CORR_ONE = 1.0 - BETA_ONE ** STEP
CORR_TWO = 1.0 - BETA_TWO ** STEP

ROWS = 384
HALF = 192
COLS = 4096
DATA = 8
DEVICES = 16
PIECE = 1024
PIECES = COLS // PIECE
ADAM_PIECE = 1024
LEAD = 16
OUT_PARTS = 6
VMEM_LIMIT = 16 << 20

RS_SIZES = (48, 48, 48, 32, 16)
RS_CHUNKS = len(RS_SIZES)
RS_STARTS = tuple(sum(RS_SIZES[:i]) for i in range(RS_CHUNKS))
AG_SIZES = (16,) + (32,) * 10 + (16,) * 3
AG_FAR_BY_Y = (1,) + (0, 1) * 5 + (0, 1, 0)
AG_CHUNKS = len(AG_SIZES)
AG_STARTS = tuple(sum(AG_SIZES[:i]) for i in range(AG_CHUNKS))
NORM_CHUNKS = ((0, 16), (16, 208), (208, 384))

MESH = pl.DeviceIdType.MESH
F32 = jnp.float32
BF16 = jnp.bfloat16


def fold_lanes(values):
    total = values[:, 0:128]
    for group in range(1, values.shape[1] // 128):
        total = total + values[:, group * 128:(group + 1) * 128]
    return total


def tensor_total(tile):
    row = [tile[s:s + 1, :] for s in range(8)]
    first3 = row[0] + row[1] + row[2]
    first4 = first3 + row[3]
    mid3 = row[4] + row[5] + row[6]
    last4 = mid3 + row[7]
    sub = lax.broadcasted_iota(jnp.int32, (8, 128), 0)
    kind = lax.broadcasted_iota(jnp.int32, (8, 128), 1) % 3
    full = lambda value: jnp.broadcast_to(value, (8, 128))
    low = jnp.where(kind == 0, jnp.where(sub == 3, full(row[3]), full(first3)), full(first4))
    high = jnp.where(kind == 1, jnp.where(sub == 7, full(row[7]), full(mid3)), full(last4))
    return jnp.where(sub < 4, low, high)


def first_totals(row):
    lane = lax.broadcasted_iota(jnp.int32, (8, 128), 1)
    sub = lax.broadcasted_iota(jnp.int32, (8, 128), 0)
    tile = jnp.zeros((8, 128), F32)
    for group in range(NORM_CHUNKS[0][1] // 8):
        low, high = ((3, 4), (4, 7), (4, 8))[group % 3]
        part = lambda s: (s >= low).astype(jnp.int32) + (s >= high).astype(jnp.int32)
        same = (lane // 8 == group) & (part(sub) == part(lane % 8))
        total = jnp.sum(jnp.where(same, jnp.broadcast_to(row, (8, 128)), 0.0), axis=1, keepdims=True)
        tile = jnp.where(lane == group, total, tile)
    return tile


def kernel(grad_ref, master_ref, one_ref, two_ref, params, master, one, two, relay, grad, weight_buf, norm_buf, first_buf, sq_buf, part_buf, lead,
           load_sem, rs_recv, rs_send, hop_recv, hop_send, ex_recv, ex_send, ag_x, ag_y, ag_d, ag_o, ag_send, plane_sem, lead_sem):
    model = lax.axis_index("model")
    me = lax.axis_index("data")
    linear = model * DATA + me
    core = me % 2
    x = (me // 2) % 2
    y = me // 4
    to_core = 1 - 2 * core
    near_x = me + 2 - 4 * x
    near_y = me + 4 - 8 * y
    diag = near_x + 4 - 8 * y
    other = me + to_core
    peer = lambda index: {"model": model, "data": index}
    block = lambda index: pl.ds(pl.multiple_of(index * COLS, COLS), COLS)

    loads = [pltpu.make_async_copy(source, target, load_sem.at[i])
             for i, (source, target) in enumerate(((master_ref, master), (one_ref, one), (two_ref, two)))]

    first = (near_x, near_y)
    second = (near_y, near_x)

    def rows_of(half, chunk):
        return pl.ds(half * HALF + RS_STARTS[chunk], RS_SIZES[chunk])

    leads = [pltpu.make_async_copy(grad_ref.at[0, pl.ds(half * HALF, LEAD), block(first[half])], lead.at[half], lead_sem.at[half]) for half in range(2)]
    for copy in leads:
        copy.start()

    barrier = pltpu.get_barrier_semaphore()

    mirror = {"model": 1 - model, "data": me}
    for neighbour in (peer(near_x), peer(near_x + to_core), peer(near_y), peer(near_y + to_core), mirror, peer(other)):
        pl.semaphore_signal(barrier, inc=1, device_id=neighbour, device_id_type=MESH)
    pl.semaphore_wait(barrier, 6)

    def remote(source, target, send, recv, index):
        return pltpu.make_async_remote_copy(src_ref=source, dst_ref=target, send_sem=send, recv_sem=recv,
                                            device_id=peer(index), device_id_type=MESH)

    for chunk in range(RS_CHUNKS):
        for half in range(2):
            rows = rows_of(half, chunk)
            recv = rs_recv.at[half, chunk]
            send = rs_send.at[half]
            for turn in range(2):
                shift = turn * to_core
                for part, owner in enumerate((first[half] + shift, diag + shift)):
                    place = pl.ds((4 + 2 * turn + part) * COLS, COLS)
                    sent = rows
                    if (chunk, turn, part) == (0, 0, 0):
                        leads[half].wait()
                        remote(lead.at[half], params.at[pl.ds(half * HALF, LEAD), place], send, recv, first[half]).start()
                        sent = pl.ds(half * HALF + LEAD, RS_SIZES[0] - LEAD)
                    remote(grad_ref.at[0, sent, block(owner)], params.at[sent, place], send, recv, first[half] + shift).start()
            for part, owner in enumerate((other, second[half] + to_core)):
                remote(grad_ref.at[0, rows, block(owner)], params.at[rows, pl.ds((2 + part) * COLS, COLS)], send, recv, other).start()

    def load_own(chunk):
        for half in range(2):
            rows = rows_of(half, chunk)
            for part, owner in enumerate((me, second[half])):
                pltpu.make_async_copy(grad_ref.at[0, rows, block(owner)], params.at[rows, pl.ds(part * COLS, COLS)], rs_recv.at[half, chunk]).start()

    load_own(0)

    lane = lax.broadcasted_iota(jnp.int32, (8, 128), 1)
    sub = lax.broadcasted_iota(jnp.int32, (8, 128), 0)

    def weight_rows(group, tile):
        rows = pl.ds(pl.multiple_of(group * 8, 8), 8)

        def piece(i, total):
            value = master[rows, pl.ds(pl.multiple_of(i * PIECE, PIECE), PIECE)]
            return total + fold_lanes(value * value)

        total = lax.fori_loop(0, PIECES, piece, jnp.zeros((8, 128), F32))
        return jnp.where(lane == group, jnp.sum(total, axis=1, keepdims=True), tile)


    def exchange(buf, number):
        for flips in reversed(range(1, DEVICES)):
            to_model, to_y, to_x, to_core = [at + (1 - 2 * at) * (flips >> bit & 1) for bit, at in zip((3, 2, 1, 0), (model, y, x, core))]
            pltpu.make_async_remote_copy(src_ref=buf.at[linear], dst_ref=buf.at[linear], send_sem=ex_send.at[number], recv_sem=ex_recv.at[number],
                                         device_id={"model": to_model, "data": to_y * 4 + to_x * 2 + to_core}, device_id_type=MESH).start()

    def exchange_wait(buf, sem):
        others = buf.at[pl.ds(0, DEVICES - 1)]
        pltpu.make_async_copy(others, others, sem).wait()

    def gathered(buf):
        total = buf[0]
        for index in range(1, DEVICES):
            total = total + buf[index]
        return total

    EX_WEIGHT, EX_GRAD, EX_FIRST = range(3)

    def decay(state, factor):
        @pl.loop(0, ROWS // 8 * PIECES)
        def _(step):
            rows = pl.ds(pl.multiple_of(step // PIECES * 8, 8), 8)
            cols = pl.ds(pl.multiple_of(step % PIECES * PIECE, PIECE), PIECE)
            state[rows, cols] = state[rows, cols] * factor

    def four(rows, cols_at, part):
        total = params[rows, pl.ds(pl.multiple_of(part * COLS + cols_at, PIECE), PIECE)].astype(F32)
        for source in range(1, 4):
            total = total + params[rows, pl.ds(pl.multiple_of((2 * source + part) * COLS + cols_at, PIECE), PIECE)].astype(F32)
        return total

    def hop(half, chunk):
        rows = rows_of(half, chunk)
        return remote(relay.at[rows], grad.at[rows], hop_send.at[half], hop_recv.at[half, chunk], second[half])

    for chunk in range(RS_CHUNKS):
        for half in range(2):
            rows = rows_of(half, chunk)
            whole = params.at[rows]
            pltpu.make_async_copy(whole, whole, rs_recv.at[half, chunk]).wait()

            @pl.loop(0, RS_SIZES[chunk] // 16 * PIECES)
            def _(step):
                tile_rows = pl.ds(pl.multiple_of(half * HALF + RS_STARTS[chunk] + step // PIECES * 16, 16), 16)
                cols_at = step % PIECES * PIECE
                relay[tile_rows, pl.ds(pl.multiple_of(cols_at, PIECE), PIECE)] = four(tile_rows, cols_at, 1)

            hop(half, chunk).start()
        if chunk == 0:
            pl.semaphore_signal(plane_sem, inc=1, device_id=mirror, device_id_type=MESH)
        if chunk + 1 < RS_CHUNKS:
            load_own(chunk + 1)
        if chunk < 3:
            loads[chunk].start()
        if chunk == 1:
            loads[0].wait()
            weight_buf[linear] = lax.fori_loop(0, ROWS // 8, weight_rows, jnp.zeros((8, 128), F32))
        if chunk == 2:
            pl.semaphore_wait(plane_sem, 1)
            exchange(weight_buf, EX_WEIGHT)
            loads[1].wait()
            decay(one, BETA_ONE)
        if chunk == 3:
            loads[2].wait()
            decay(two, BETA_TWO)

    square = jnp.zeros((8, 128), F32)
    for chunk in range(RS_CHUNKS):
        for half in range(2):
            hop(half, chunk).wait_recv()

            def finish(step, total):
                tile_rows = pl.ds(pl.multiple_of(half * HALF + RS_STARTS[chunk] + step // PIECES * 16, 16), 16)
                cols_at = step % PIECES * PIECE
                cols = pl.ds(pl.multiple_of(cols_at, PIECE), PIECE)
                value = (grad[tile_rows, cols] + four(tile_rows, cols_at, 0)) * (1.0 / DATA)
                grad[tile_rows, cols] = value
                folded = fold_lanes(value * value)
                return total + (folded[0:8] + folded[8:16])

            square = lax.fori_loop(0, RS_SIZES[chunk] // 16 * PIECES, finish, square)

    norm_buf[linear] = jnp.sum(square, axis=0, keepdims=True)
    exchange(norm_buf, EX_GRAD)
    for half in range(2):
        rows = pl.ds(half * HALF, HALF)
        pltpu.make_async_copy(relay.at[rows], relay.at[rows], hop_send.at[half]).wait()
    exchange_wait(weight_buf, ex_recv.at[EX_WEIGHT])
    weight_norm = jnp.sqrt(tensor_total(gathered(weight_buf)))
    exchange_wait(norm_buf, ex_recv.at[EX_GRAD])
    grad_norm = jnp.sqrt(jnp.sum(gathered(norm_buf), axis=1, keepdims=True))
    clip = jnp.minimum(1.0, MAX_NORM / grad_norm)

    grad_one = (1.0 - BETA_ONE) * clip
    grad_two = (1.0 - BETA_TWO) ** 0.5 * clip

    def adam(start, stop):
        @pl.loop(start, stop)
        def _(group):
            rows = pl.ds(pl.multiple_of(group * 8, 8), 8)
            total = jnp.zeros((8, 128), F32)
            for i in range(COLS // ADAM_PIECE):
                cols = pl.ds(i * ADAM_PIECE, ADAM_PIECE)
                mean = grad[rows, cols]
                new_one = one[rows, cols] + grad_one * mean
                scaled = grad_two * mean
                new_two = two[rows, cols] + scaled * scaled
                one[rows, cols] = new_one
                two[rows, cols] = new_two
                direction = new_one / (jnp.sqrt(new_two) * (CORR_ONE / CORR_TWO ** 0.5) + CORR_ONE * EPSILON) + WEIGHT_DECAY * master[rows, cols]
                relay[rows, cols] = direction
                total = total + fold_lanes(direction * direction)
            part_buf[group] = total

    def row_sums(start, stop, place):
        tile = jnp.zeros((8, 128), F32)
        for group in range(start, stop):
            tile = jnp.where(lane == place(group), jnp.sum(part_buf[group], axis=1, keepdims=True), tile)
        return tile

    def step_rates(number):
        if number == 0:
            exchange_wait(first_buf, ex_recv.at[EX_FIRST])
            total = first_totals(gathered(first_buf))
        else:
            exchange_wait(sq_buf.at[number - 1], ex_recv.at[EX_FIRST + number])
            total = tensor_total(gathered(sq_buf.at[number - 1]))
        return weight_norm / jnp.sqrt(total) * LEARN_RATE

    def ag_rows(chunk):
        return pl.ds(AG_STARTS[chunk], AG_SIZES[chunk])

    def update(number, rates):
        start, stop = NORM_CHUNKS[number]
        for chunk in range(AG_CHUNKS):
            if not start <= AG_STARTS[chunk] < stop:
                continue

            @pl.loop(0, AG_SIZES[chunk] // 16)
            def _(tile):
                group = AG_STARTS[chunk] // 8 + 2 * tile
                rows = pl.ds(pl.multiple_of(AG_STARTS[chunk] + tile * 16, 16), 16)
                rate = jnp.concatenate([jnp.sum(jnp.where(lane == group + i, rates, 0.0), axis=1, keepdims=True) for i in range(2)], axis=0)

                @pl.loop(0, PIECES)
                def _(i):
                    cols = pl.ds(pl.multiple_of(i * PIECE, PIECE), PIECE)
                    value = master[rows, cols] - rate * relay[rows, cols]
                    master[rows, cols] = value
                    params[rows, pl.ds(pl.multiple_of(me * COLS + i * PIECE, PIECE), PIECE)] = value.astype(BF16)

            rows = ag_rows(chunk)
            own = params.at[rows, block(me)]
            remote(own, own, ag_send.at[0], ag_x.at[chunk], near_x).start()
            remote(own, own, ag_send.at[1], ag_y.at[chunk], near_y).start()
            remote(own, own, ag_send.at[2], ag_o, other).start()

    groups = [(start // 8, stop // 8) for start, stop in NORM_CHUNKS]
    adam(*groups[0])
    first_buf[linear] = jnp.sum(row_sums(*groups[0], lambda group: 8 * group + sub), axis=0, keepdims=True)
    adam(groups[1][0], groups[1][0] + 1)
    exchange(first_buf, EX_FIRST)
    adam(groups[1][0] + 1, groups[1][1])
    sq_buf[0, linear] = row_sums(*groups[1], lambda group: group)
    adam(groups[2][0], groups[2][0] + 1)
    exchange(sq_buf.at[0], EX_FIRST + 1)
    update(0, step_rates(0))
    adam(groups[2][0] + 1, groups[2][1])
    sq_buf[1, linear] = row_sums(*groups[2], lambda group: group)
    rates = step_rates(1)
    exchange(sq_buf.at[1], EX_FIRST + 2)
    update(1, rates)
    update(2, step_rates(2))

    def arrived(sem, source, rows):
        view = params.at[rows, block(source)]
        pltpu.make_async_copy(view, view, sem).wait()
        return view

    for chunk in range(AG_CHUNKS):
        rows = ag_rows(chunk)
        view = arrived(ag_x.at[chunk], near_x, rows)
        if AG_FAR_BY_Y[chunk]:
            remote(view, view, ag_send.at[1], ag_d.at[chunk], near_y).start()
        remote(view, view, ag_send.at[2], ag_o, other).start()
        view = arrived(ag_y.at[chunk], near_y, rows)
        if not AG_FAR_BY_Y[chunk]:
            remote(view, view, ag_send.at[0], ag_d.at[chunk], near_x).start()
        remote(view, view, ag_send.at[2], ag_o, other).start()

    for chunk in range(AG_CHUNKS):
        view = arrived(ag_d.at[chunk], diag, ag_rows(chunk))
        remote(view, view, ag_send.at[2], ag_o, other).start()

    half_cols = params.at[:, pl.ds(0, DATA // 2 * COLS)]
    pltpu.make_async_copy(half_cols, half_cols, ag_o).wait()
    pltpu.make_async_copy(half_cols, half_cols, ag_send.at[2]).wait()
    for direction in range(2):
        for part in (pl.ds(0, ROWS), pl.ds(0, HALF)):
            view = params.at[part, pl.ds(0, COLS)]
            pltpu.make_async_copy(view, view, ag_send.at[direction]).wait()
    for half in range(2):
        view = params.at[pl.ds(0, HALF), pl.ds(0, 6 * COLS)]
        pltpu.make_async_copy(view, view, rs_send.at[half]).wait()
    exchange_wait(weight_buf, ex_send.at[EX_WEIGHT])
    exchange_wait(norm_buf, ex_send.at[EX_GRAD])
    exchange_wait(first_buf, ex_send.at[EX_FIRST])
    for number in range(2):
        exchange_wait(sq_buf.at[number], ex_send.at[EX_FIRST + 1 + number])


def write_out(*refs):
    count = len(refs) // 2
    sem = refs[-1]
    copies = []
    for part in range(OUT_PARTS):
        rows = pl.ds(part * (ROWS // OUT_PARTS), ROWS // OUT_PARTS)
        for source, target in zip(refs[:count], refs[count:-1]):
            copies.append(pltpu.make_async_copy(source.at[rows], target.at[rows], sem.at[len(copies)]))
    for number, copy in enumerate(copies):
        copy.start(priority=number % 2)
    for copy in copies:
        copy.wait()


def solution(mesh):
    def device_step(local_grads, master, moment_one, moment_two):
        any_spec = pl.BlockSpec(memory_space=pl.ANY)
        vmem_spec = pl.BlockSpec(memory_space=pltpu.VMEM)
        state = pltpu.VMEM((ROWS, COLS), F32)
        dma = pltpu.SemaphoreType.DMA
        results = pl.pallas_call(
            kernel,
            name="lamb",
            out_shape=(pltpu.VMEM((ROWS, DATA * COLS), BF16), state, state, state),
            in_specs=[any_spec] * 4,
            out_specs=[vmem_spec] * 4,
            scratch_shapes=[
                pltpu.VMEM((ROWS, COLS), F32),
                pltpu.VMEM((ROWS, COLS), F32),
                pltpu.VMEM((DEVICES, 8, 128), F32),
                pltpu.VMEM((DEVICES, 1, 128), F32),
                pltpu.VMEM((DEVICES, 1, 128), F32),
                pltpu.VMEM((2, DEVICES, 8, 128), F32),
                pltpu.VMEM((ROWS // 8, 8, 128), F32),
                pltpu.VMEM((2, LEAD, COLS), BF16),
                dma((3,)),
                dma((2, RS_CHUNKS)),
                dma((2,)),
                dma((2, RS_CHUNKS)),
                dma((2,)),
                dma((5,)),
                dma((5,)),
                dma((AG_CHUNKS,)),
                dma((AG_CHUNKS,)),
                dma((AG_CHUNKS,)),
                dma,
                dma((3,)),
                pltpu.SemaphoreType.REGULAR,
                dma((2,)),
            ],
            compiler_params=pltpu.CompilerParams(collective_id=0, has_side_effects=True, vmem_limit_bytes=VMEM_LIMIT),
        )(local_grads, master, moment_one, moment_two)
        results = [pltpu.with_memory_space_constraint(value, pltpu.VMEM) for value in results]
        return tuple(pl.pallas_call(
            write_out,
            name="write_out",
            out_shape=[jax.ShapeDtypeStruct(value.shape, value.dtype) for value in results],
            in_specs=[vmem_spec] * 4,
            out_specs=[any_spec] * 4,
            scratch_shapes=[dma((4 * OUT_PARTS,))],
            compiler_params=pltpu.CompilerParams(vmem_limit_bytes=VMEM_LIMIT),
        )(*results))

    state_spec = P(None, ('model', 'data'))
    return jax.shard_map(device_step, mesh=mesh, in_specs=(P('data', None, 'model'), state_spec, state_spec, state_spec), out_specs=(P(None, 'model'), state_spec, state_spec, state_spec), check_vma=False)
```

```python
import jax
import jax.numpy as jnp
from jax import lax
from jax.experimental import pallas as pl
from jax.experimental.pallas import tpu as pltpu
from jax.sharding import PartitionSpec as P

STEP = 4
LEARN_RATE = 0.08
BETA_ONE = 0.9
BETA_TWO = 0.999
EPSILON = 1e-6
WEIGHT_DECAY = 0.01
MAX_NORM = 1.0
CORR_ONE = 1.0 - BETA_ONE ** STEP
CORR_TWO = 1.0 - BETA_TWO ** STEP

ROWS = 384
HALF = 192
COLS = 4096
DATA = 8
DEVICES = 16
PIECE = 1024
PIECES = COLS // PIECE
ADAM_PIECE = 1024
OUT_PARTS = 6
VMEM_LIMIT = 16 << 20

RS_SIZES = (48, 48, 48, 32, 16)
RS_CHUNKS = len(RS_SIZES)
RS_STARTS = tuple(sum(RS_SIZES[:i]) for i in range(RS_CHUNKS))
AG_SIZES = (16,) + (32,) * 10 + (16,) * 3
AG_FAR_BY_Y = (1,) + (0, 1) * 5 + (0, 1, 0)
AG_CHUNKS = len(AG_SIZES)
AG_STARTS = tuple(sum(AG_SIZES[:i]) for i in range(AG_CHUNKS))
NORM_CHUNKS = ((0, 16), (16, 208), (208, 384))

MESH = pl.DeviceIdType.MESH
F32 = jnp.float32
BF16 = jnp.bfloat16


def fold_lanes(values):
    total = values[:, 0:128]
    for group in range(1, values.shape[1] // 128):
        total = total + values[:, group * 128:(group + 1) * 128]
    return total


def tensor_total(tile):
    row = [tile[s:s + 1, :] for s in range(8)]
    first3 = row[0] + row[1] + row[2]
    first4 = first3 + row[3]
    mid3 = row[4] + row[5] + row[6]
    last4 = mid3 + row[7]
    sub = lax.broadcasted_iota(jnp.int32, (8, 128), 0)
    kind = lax.broadcasted_iota(jnp.int32, (8, 128), 1) % 3
    full = lambda value: jnp.broadcast_to(value, (8, 128))
    low = jnp.where(kind == 0, jnp.where(sub == 3, full(row[3]), full(first3)), full(first4))
    high = jnp.where(kind == 1, jnp.where(sub == 7, full(row[7]), full(mid3)), full(last4))
    return jnp.where(sub < 4, low, high)


def first_totals(row):
    lane = lax.broadcasted_iota(jnp.int32, (8, 128), 1)
    sub = lax.broadcasted_iota(jnp.int32, (8, 128), 0)
    tile = jnp.zeros((8, 128), F32)
    for group in range(NORM_CHUNKS[0][1] // 8):
        low, high = ((3, 4), (4, 7), (4, 8))[group % 3]
        part = lambda s: (s >= low).astype(jnp.int32) + (s >= high).astype(jnp.int32)
        same = (lane // 8 == group) & (part(sub) == part(lane % 8))
        total = jnp.sum(jnp.where(same, jnp.broadcast_to(row, (8, 128)), 0.0), axis=1, keepdims=True)
        tile = jnp.where(lane == group, total, tile)
    return tile


def kernel(grad_ref, master_ref, one_ref, two_ref, params, master, one, two, relay, grad, weight_buf, norm_buf, first_buf, sq_buf, part_buf,
           load_sem, rs_recv, rs_send, hop_recv, hop_send, ex_recv, ex_send, ag_x, ag_y, ag_d, ag_o, ag_send, plane_sem):
    model = lax.axis_index("model")
    me = lax.axis_index("data")
    linear = model * DATA + me
    core = me % 2
    x = (me // 2) % 2
    y = me // 4
    to_core = 1 - 2 * core
    near_x = me + 2 - 4 * x
    near_y = me + 4 - 8 * y
    diag = near_x + 4 - 8 * y
    other = me + to_core
    peer = lambda index: {"model": model, "data": index}
    block = lambda index: pl.ds(pl.multiple_of(index * COLS, COLS), COLS)

    loads = [pltpu.make_async_copy(source, target, load_sem.at[i])
             for i, (source, target) in enumerate(((master_ref, master), (one_ref, one), (two_ref, two)))]

    first = (near_x, near_y)
    second = (near_y, near_x)

    def rows_of(half, chunk):
        return pl.ds(half * HALF + RS_STARTS[chunk], RS_SIZES[chunk])

    barrier = pltpu.get_barrier_semaphore()

    mirror = {"model": 1 - model, "data": me}
    for neighbour in (peer(near_x), peer(near_x + to_core), peer(near_y), peer(near_y + to_core), mirror, peer(other)):
        pl.semaphore_signal(barrier, inc=1, device_id=neighbour, device_id_type=MESH)
    pl.semaphore_wait(barrier, 6)

    def remote(source, target, send, recv, index):
        return pltpu.make_async_remote_copy(src_ref=source, dst_ref=target, send_sem=send, recv_sem=recv,
                                            device_id=peer(index), device_id_type=MESH)

    for chunk in range(RS_CHUNKS):
        for half in range(2):
            rows = rows_of(half, chunk)
            recv = rs_recv.at[half, chunk]
            send = rs_send.at[half]
            for turn in range(2):
                shift = turn * to_core
                for part, owner in enumerate((first[half] + shift, diag + shift)):
                    remote(grad_ref.at[0, rows, block(owner)], params.at[rows, pl.ds((4 + 2 * turn + part) * COLS, COLS)], send, recv, first[half] + shift).start()

    def load_own(chunk):
        for half in range(2):
            rows = rows_of(half, chunk)
            for part, owner in enumerate((me, second[half])):
                pltpu.make_async_copy(grad_ref.at[0, rows, block(owner)], params.at[rows, pl.ds(part * COLS, COLS)], rs_recv.at[half, chunk]).start()
            for part, owner in enumerate((other, second[half] + to_core)):
                remote(grad_ref.at[0, rows, block(owner)], params.at[rows, pl.ds((2 + part) * COLS, COLS)], rs_send.at[half], rs_recv.at[half, chunk], other).start()

    load_own(0)

    lane = lax.broadcasted_iota(jnp.int32, (8, 128), 1)
    sub = lax.broadcasted_iota(jnp.int32, (8, 128), 0)

    def weight_rows(group, tile):
        rows = pl.ds(pl.multiple_of(group * 8, 8), 8)

        def piece(i, total):
            value = master[rows, pl.ds(pl.multiple_of(i * PIECE, PIECE), PIECE)]
            return total + fold_lanes(value * value)

        total = lax.fori_loop(0, PIECES, piece, jnp.zeros((8, 128), F32))
        return jnp.where(lane == group, jnp.sum(total, axis=1, keepdims=True), tile)


    def exchange(buf, number):
        for flips in reversed(range(1, DEVICES)):
            to_model, to_y, to_x, to_core = [at + (1 - 2 * at) * (flips >> bit & 1) for bit, at in zip((3, 2, 1, 0), (model, y, x, core))]
            pltpu.make_async_remote_copy(src_ref=buf.at[linear], dst_ref=buf.at[linear], send_sem=ex_send.at[number], recv_sem=ex_recv.at[number],
                                         device_id={"model": to_model, "data": to_y * 4 + to_x * 2 + to_core}, device_id_type=MESH).start()

    def exchange_wait(buf, sem):
        others = buf.at[pl.ds(0, DEVICES - 1)]
        pltpu.make_async_copy(others, others, sem).wait()

    def gathered(buf):
        total = buf[0]
        for index in range(1, DEVICES):
            total = total + buf[index]
        return total

    EX_WEIGHT, EX_GRAD, EX_FIRST = range(3)

    def decay(state, factor):
        @pl.loop(0, ROWS // 8 * PIECES)
        def _(step):
            rows = pl.ds(pl.multiple_of(step // PIECES * 8, 8), 8)
            cols = pl.ds(pl.multiple_of(step % PIECES * PIECE, PIECE), PIECE)
            state[rows, cols] = state[rows, cols] * factor

    def four(rows, cols_at, part):
        total = params[rows, pl.ds(pl.multiple_of(part * COLS + cols_at, PIECE), PIECE)].astype(F32)
        for source in range(1, 4):
            total = total + params[rows, pl.ds(pl.multiple_of((2 * source + part) * COLS + cols_at, PIECE), PIECE)].astype(F32)
        return total

    def hop(half, chunk):
        rows = rows_of(half, chunk)
        return remote(relay.at[rows], grad.at[rows], hop_send.at[half], hop_recv.at[half, chunk], second[half])

    for chunk in range(RS_CHUNKS):
        for half in range(2):
            rows = rows_of(half, chunk)
            whole = params.at[rows]
            pltpu.make_async_copy(whole, whole, rs_recv.at[half, chunk]).wait()

            @pl.loop(0, RS_SIZES[chunk] // 16 * PIECES)
            def _(step):
                tile_rows = pl.ds(pl.multiple_of(half * HALF + RS_STARTS[chunk] + step // PIECES * 16, 16), 16)
                cols_at = step % PIECES * PIECE
                relay[tile_rows, pl.ds(pl.multiple_of(cols_at, PIECE), PIECE)] = four(tile_rows, cols_at, 1)

            hop(half, chunk).start()
        if chunk == 0:
            pl.semaphore_signal(plane_sem, inc=1, device_id=mirror, device_id_type=MESH)
        if chunk + 1 < RS_CHUNKS:
            load_own(chunk + 1)
        if chunk < 3:
            loads[chunk].start()
        if chunk == 1:
            loads[0].wait()
            weight_buf[linear] = lax.fori_loop(0, ROWS // 8, weight_rows, jnp.zeros((8, 128), F32))
        if chunk == 2:
            pl.semaphore_wait(plane_sem, 1)
            exchange(weight_buf, EX_WEIGHT)
            loads[1].wait()
            decay(one, BETA_ONE)
        if chunk == 3:
            loads[2].wait()
            decay(two, BETA_TWO)

    square = jnp.zeros((8, 128), F32)
    for chunk in range(RS_CHUNKS):
        for half in range(2):
            hop(half, chunk).wait_recv()

            def finish(step, total):
                tile_rows = pl.ds(pl.multiple_of(half * HALF + RS_STARTS[chunk] + step // PIECES * 16, 16), 16)
                cols_at = step % PIECES * PIECE
                cols = pl.ds(pl.multiple_of(cols_at, PIECE), PIECE)
                value = (grad[tile_rows, cols] + four(tile_rows, cols_at, 0)) * (1.0 / DATA)
                grad[tile_rows, cols] = value
                folded = fold_lanes(value * value)
                return total + (folded[0:8] + folded[8:16])

            square = lax.fori_loop(0, RS_SIZES[chunk] // 16 * PIECES, finish, square)

    norm_buf[linear] = jnp.sum(square, axis=0, keepdims=True)
    exchange(norm_buf, EX_GRAD)
    for half in range(2):
        rows = pl.ds(half * HALF, HALF)
        pltpu.make_async_copy(relay.at[rows], relay.at[rows], hop_send.at[half]).wait()
    exchange_wait(weight_buf, ex_recv.at[EX_WEIGHT])
    weight_norm = jnp.sqrt(tensor_total(gathered(weight_buf)))
    exchange_wait(norm_buf, ex_recv.at[EX_GRAD])
    grad_norm = jnp.sqrt(jnp.sum(gathered(norm_buf), axis=1, keepdims=True))
    clip = jnp.minimum(1.0, MAX_NORM / grad_norm)

    grad_one = (1.0 - BETA_ONE) * clip
    grad_two = (1.0 - BETA_TWO) ** 0.5 * clip

    def adam(start, stop):
        @pl.loop(start, stop)
        def _(group):
            rows = pl.ds(pl.multiple_of(group * 8, 8), 8)
            total = jnp.zeros((8, 128), F32)
            for i in range(COLS // ADAM_PIECE):
                cols = pl.ds(i * ADAM_PIECE, ADAM_PIECE)
                mean = grad[rows, cols]
                new_one = one[rows, cols] + grad_one * mean
                scaled = grad_two * mean
                new_two = two[rows, cols] + scaled * scaled
                one[rows, cols] = new_one
                two[rows, cols] = new_two
                direction = new_one / (jnp.sqrt(new_two) * (CORR_ONE / CORR_TWO ** 0.5) + CORR_ONE * EPSILON) + WEIGHT_DECAY * master[rows, cols]
                relay[rows, cols] = direction
                total = total + fold_lanes(direction * direction)
            part_buf[group] = total

    def row_sums(start, stop, place):
        tile = jnp.zeros((8, 128), F32)
        for group in range(start, stop):
            tile = jnp.where(lane == place(group), jnp.sum(part_buf[group], axis=1, keepdims=True), tile)
        return tile

    def step_rates(number):
        if number == 0:
            exchange_wait(first_buf, ex_recv.at[EX_FIRST])
            total = first_totals(gathered(first_buf))
        else:
            exchange_wait(sq_buf.at[number - 1], ex_recv.at[EX_FIRST + number])
            total = tensor_total(gathered(sq_buf.at[number - 1]))
        return weight_norm / jnp.sqrt(total) * LEARN_RATE

    def ag_rows(chunk):
        return pl.ds(AG_STARTS[chunk], AG_SIZES[chunk])

    def update(number, rates):
        start, stop = NORM_CHUNKS[number]
        for chunk in range(AG_CHUNKS):
            if not start <= AG_STARTS[chunk] < stop:
                continue

            @pl.loop(0, AG_SIZES[chunk] // 16)
            def _(tile):
                group = AG_STARTS[chunk] // 8 + 2 * tile
                rows = pl.ds(pl.multiple_of(AG_STARTS[chunk] + tile * 16, 16), 16)
                rate = jnp.concatenate([jnp.sum(jnp.where(lane == group + i, rates, 0.0), axis=1, keepdims=True) for i in range(2)], axis=0)

                @pl.loop(0, PIECES)
                def _(i):
                    cols = pl.ds(pl.multiple_of(i * PIECE, PIECE), PIECE)
                    value = master[rows, cols] - rate * relay[rows, cols]
                    master[rows, cols] = value
                    params[rows, pl.ds(pl.multiple_of(me * COLS + i * PIECE, PIECE), PIECE)] = value.astype(BF16)

            rows = ag_rows(chunk)
            own = params.at[rows, block(me)]
            remote(own, own, ag_send.at[0], ag_x.at[chunk], near_x).start()
            remote(own, own, ag_send.at[1], ag_y.at[chunk], near_y).start()
            remote(own, own, ag_send.at[2], ag_o, other).start()

    groups = [(start // 8, stop // 8) for start, stop in NORM_CHUNKS]
    adam(*groups[0])
    first_buf[linear] = jnp.sum(row_sums(*groups[0], lambda group: 8 * group + sub), axis=0, keepdims=True)
    adam(groups[1][0], groups[1][0] + 1)
    exchange(first_buf, EX_FIRST)
    adam(groups[1][0] + 1, groups[1][1])
    sq_buf[0, linear] = row_sums(*groups[1], lambda group: group)
    adam(groups[2][0], groups[2][0] + 1)
    exchange(sq_buf.at[0], EX_FIRST + 1)
    update(0, step_rates(0))
    adam(groups[2][0] + 1, groups[2][1])
    sq_buf[1, linear] = row_sums(*groups[2], lambda group: group)
    rates = step_rates(1)
    exchange(sq_buf.at[1], EX_FIRST + 2)
    update(1, rates)
    update(2, step_rates(2))

    def arrived(sem, source, rows):
        view = params.at[rows, block(source)]
        pltpu.make_async_copy(view, view, sem).wait()
        return view

    for chunk in range(AG_CHUNKS):
        rows = ag_rows(chunk)
        view = arrived(ag_x.at[chunk], near_x, rows)
        if AG_FAR_BY_Y[chunk]:
            remote(view, view, ag_send.at[1], ag_d.at[chunk], near_y).start()
        remote(view, view, ag_send.at[2], ag_o, other).start()
        view = arrived(ag_y.at[chunk], near_y, rows)
        if not AG_FAR_BY_Y[chunk]:
            remote(view, view, ag_send.at[0], ag_d.at[chunk], near_x).start()
        remote(view, view, ag_send.at[2], ag_o, other).start()

    for chunk in range(AG_CHUNKS):
        view = arrived(ag_d.at[chunk], diag, ag_rows(chunk))
        remote(view, view, ag_send.at[2], ag_o, other).start()

    half_cols = params.at[:, pl.ds(0, DATA // 2 * COLS)]
    pltpu.make_async_copy(half_cols, half_cols, ag_o).wait()
    pltpu.make_async_copy(half_cols, half_cols, ag_send.at[2]).wait()
    for direction in range(2):
        for part in (pl.ds(0, ROWS), pl.ds(0, HALF)):
            view = params.at[part, pl.ds(0, COLS)]
            pltpu.make_async_copy(view, view, ag_send.at[direction]).wait()
    for half in range(2):
        view = params.at[pl.ds(0, HALF), pl.ds(0, 6 * COLS)]
        pltpu.make_async_copy(view, view, rs_send.at[half]).wait()
    exchange_wait(weight_buf, ex_send.at[EX_WEIGHT])
    exchange_wait(norm_buf, ex_send.at[EX_GRAD])
    exchange_wait(first_buf, ex_send.at[EX_FIRST])
    for number in range(2):
        exchange_wait(sq_buf.at[number], ex_send.at[EX_FIRST + 1 + number])


def write_out(*refs):
    count = len(refs) // 2
    sem = refs[-1]
    copies = []
    for part in range(OUT_PARTS):
        rows = pl.ds(part * (ROWS // OUT_PARTS), ROWS // OUT_PARTS)
        for source, target in zip(refs[:count], refs[count:-1]):
            copies.append(pltpu.make_async_copy(source.at[rows], target.at[rows], sem.at[len(copies)]))
    for number, copy in enumerate(copies):
        copy.start(priority=number % 2)
    for copy in copies:
        copy.wait()


def solution(mesh):
    def device_step(local_grads, master, moment_one, moment_two):
        any_spec = pl.BlockSpec(memory_space=pl.ANY)
        vmem_spec = pl.BlockSpec(memory_space=pltpu.VMEM)
        state = pltpu.VMEM((ROWS, COLS), F32)
        dma = pltpu.SemaphoreType.DMA
        results = pl.pallas_call(
            kernel,
            name="lamb",
            out_shape=(pltpu.VMEM((ROWS, DATA * COLS), BF16), state, state, state),
            in_specs=[any_spec] * 4,
            out_specs=[vmem_spec] * 4,
            scratch_shapes=[
                pltpu.VMEM((ROWS, COLS), F32),
                pltpu.VMEM((ROWS, COLS), F32),
                pltpu.VMEM((DEVICES, 8, 128), F32),
                pltpu.VMEM((DEVICES, 1, 128), F32),
                pltpu.VMEM((DEVICES, 1, 128), F32),
                pltpu.VMEM((2, DEVICES, 8, 128), F32),
                pltpu.VMEM((ROWS // 8, 8, 128), F32),
                dma((3,)),
                dma((2, RS_CHUNKS)),
                dma((2,)),
                dma((2, RS_CHUNKS)),
                dma((2,)),
                dma((5,)),
                dma((5,)),
                dma((AG_CHUNKS,)),
                dma((AG_CHUNKS,)),
                dma((AG_CHUNKS,)),
                dma,
                dma((3,)),
                pltpu.SemaphoreType.REGULAR,
            ],
            compiler_params=pltpu.CompilerParams(collective_id=0, has_side_effects=True, vmem_limit_bytes=VMEM_LIMIT),
        )(local_grads, master, moment_one, moment_two)
        results = [pltpu.with_memory_space_constraint(value, pltpu.VMEM) for value in results]
        return tuple(pl.pallas_call(
            write_out,
            name="write_out",
            out_shape=[jax.ShapeDtypeStruct(value.shape, value.dtype) for value in results],
            in_specs=[vmem_spec] * 4,
            out_specs=[any_spec] * 4,
            scratch_shapes=[dma((4 * OUT_PARTS,))],
            compiler_params=pltpu.CompilerParams(vmem_limit_bytes=VMEM_LIMIT),
        )(*results))

    state_spec = P(None, ('model', 'data'))
    return jax.shard_map(device_step, mesh=mesh, in_specs=(P('data', None, 'model'), state_spec, state_spec, state_spec), out_specs=(P(None, 'model'), state_spec, state_spec, state_spec), check_vma=False)
```

```python
import jax
import jax.numpy as jnp
from jax import lax
from jax.experimental import pallas as pl
from jax.experimental.pallas import tpu as pltpu
from jax.sharding import PartitionSpec as P

STEP = 4
LEARN_RATE = 0.08
BETA_ONE = 0.9
BETA_TWO = 0.999
EPSILON = 1e-6
WEIGHT_DECAY = 0.01
MAX_NORM = 1.0
CORR_ONE = 1.0 - BETA_ONE ** STEP
CORR_TWO = 1.0 - BETA_TWO ** STEP

ROWS = 384
HALF = 192
GROUPS = ROWS // 8
COLS = 4096
DATA = 8
DEVICES = 16
PIECE = 1024
PIECES = COLS // PIECE
ADAM_PIECE = 1024
OUT_PARTS = 6
VMEM_LIMIT = 16 << 20

RS_SIZES = (48, 48, 48, 32, 16)
RS_CHUNKS = len(RS_SIZES)
RS_STARTS = tuple(sum(RS_SIZES[:i]) for i in range(RS_CHUNKS))
AG_SIZES = (16,) + (32,) * 10 + (16,) * 3
AG_FAR_BY_Y = (1,) + (0, 1) * 5 + (0, 1, 0)
AG_CHUNKS = len(AG_SIZES)
AG_STARTS = tuple(sum(AG_SIZES[:i]) for i in range(AG_CHUNKS))
NORM_CHUNKS = ((0, 16), (16, 208), (208, 384))

MESH = pl.DeviceIdType.MESH
F32 = jnp.float32
BF16 = jnp.bfloat16


def fold_lanes(values):
    total = values[:, 0:128]
    for group in range(1, values.shape[1] // 128):
        total = total + values[:, group * 128:(group + 1) * 128]
    return total


def packed_totals(rows, start, stop):
    lane = lax.broadcasted_iota(jnp.int32, (8, 128), 1)
    sub = lax.broadcasted_iota(jnp.int32, (8, 128), 0)
    value = jnp.where(sub < 4, jnp.broadcast_to(rows[0:1], (8, 128)), jnp.broadcast_to(rows[1:2], (8, 128)))
    tile = jnp.zeros((8, 128), F32)
    for group in range(start, stop):
        low, high = ((3, 4), (4, 7), (4, 8))[group % 3]
        part = lambda s: (s >= low).astype(jnp.int32) + (s >= high).astype(jnp.int32)
        same = (lane % 32 == group - start) & (part(sub) == part(sub // 4 * 4 + lane // 32))
        tile = jnp.where(lane == group, jnp.sum(jnp.where(same, value, 0.0), axis=1, keepdims=True), tile)
    return tile


def packed(tile):
    return jnp.concatenate([jnp.sum(tile[0:4], axis=0, keepdims=True), jnp.sum(tile[4:8], axis=0, keepdims=True)], axis=0)


def first_totals(row):
    lane = lax.broadcasted_iota(jnp.int32, (8, 128), 1)
    sub = lax.broadcasted_iota(jnp.int32, (8, 128), 0)
    tile = jnp.zeros((8, 128), F32)
    for group in range(NORM_CHUNKS[0][1] // 8):
        low, high = ((3, 4), (4, 7), (4, 8))[group % 3]
        part = lambda s: (s >= low).astype(jnp.int32) + (s >= high).astype(jnp.int32)
        same = (lane // 8 == group) & (part(sub) == part(lane % 8))
        total = jnp.sum(jnp.where(same, jnp.broadcast_to(row, (8, 128)), 0.0), axis=1, keepdims=True)
        tile = jnp.where(lane == group, total, tile)
    return tile


def kernel(grad_ref, master_ref, one_ref, two_ref, params, master, one, two, relay, grad, weight_buf, norm_buf, first_buf, sq_buf, part_buf,
           load_sem, rs_recv, rs_send, hop_recv, hop_send, ex_recv, ex_send, ag_x, ag_y, ag_d, ag_o, ag_send, plane_sem):
    model = lax.axis_index("model")
    me = lax.axis_index("data")
    linear = model * DATA + me
    core = me % 2
    x = (me // 2) % 2
    y = me // 4
    to_core = 1 - 2 * core
    near_x = me + 2 - 4 * x
    near_y = me + 4 - 8 * y
    diag = near_x + 4 - 8 * y
    other = me + to_core
    peer = lambda index: {"model": model, "data": index}
    block = lambda index: pl.ds(pl.multiple_of(index * COLS, COLS), COLS)

    loads = [pltpu.make_async_copy(source, target, load_sem.at[i])
             for i, (source, target) in enumerate(((master_ref, master), (one_ref, one), (two_ref, two)))]

    first = (near_x, near_y)
    second = (near_y, near_x)

    def rows_of(half, chunk):
        return pl.ds(half * HALF + RS_STARTS[chunk], RS_SIZES[chunk])

    barrier = pltpu.get_barrier_semaphore()

    mirror = {"model": 1 - model, "data": me}
    for neighbour in (peer(near_x), peer(near_x + to_core), peer(near_y), peer(near_y + to_core), mirror, peer(other)):
        pl.semaphore_signal(barrier, inc=1, device_id=neighbour, device_id_type=MESH)
    pl.semaphore_wait(barrier, 6)

    def remote(source, target, send, recv, index):
        return pltpu.make_async_remote_copy(src_ref=source, dst_ref=target, send_sem=send, recv_sem=recv,
                                            device_id=peer(index), device_id_type=MESH)

    for chunk in range(RS_CHUNKS):
        for half in range(2):
            rows = rows_of(half, chunk)
            recv = rs_recv.at[half, chunk]
            send = rs_send.at[half]
            for turn in range(2):
                shift = turn * to_core
                for part, owner in enumerate((first[half] + shift, diag + shift)):
                    remote(grad_ref.at[0, rows, block(owner)], params.at[rows, pl.ds((4 + 2 * turn + part) * COLS, COLS)], send, recv, first[half] + shift).start()
            for part, owner in enumerate((other, second[half] + to_core)):
                remote(grad_ref.at[0, rows, block(owner)], params.at[rows, pl.ds((2 + part) * COLS, COLS)], send, recv, other).start()

    def load_own(chunk):
        for half in range(2):
            rows = rows_of(half, chunk)
            for part, owner in enumerate((me, second[half])):
                pltpu.make_async_copy(grad_ref.at[0, rows, block(owner)], params.at[rows, pl.ds(part * COLS, COLS)], rs_recv.at[half, chunk]).start()

    load_own(0)

    lane = lax.broadcasted_iota(jnp.int32, (8, 128), 1)
    sub = lax.broadcasted_iota(jnp.int32, (8, 128), 0)

    def weight_rows(group, tile):
        rows = pl.ds(pl.multiple_of(group * 8, 8), 8)

        def piece(i, total):
            value = master[rows, pl.ds(pl.multiple_of(i * PIECE, PIECE), PIECE)]
            return total + fold_lanes(value * value)

        total = lax.fori_loop(0, PIECES, piece, jnp.zeros((8, 128), F32))
        return jnp.where(lane == 32 * (sub % 4) + group % (GROUPS // 2), jnp.sum(total, axis=1, keepdims=True), tile)


    def exchange(buf, number):
        for flips in reversed(range(1, DEVICES)):
            to_model, to_y, to_x, to_core = [at + (1 - 2 * at) * (flips >> bit & 1) for bit, at in zip((3, 2, 1, 0), (model, y, x, core))]
            pltpu.make_async_remote_copy(src_ref=buf.at[linear], dst_ref=buf.at[linear], send_sem=ex_send.at[number], recv_sem=ex_recv.at[number],
                                         device_id={"model": to_model, "data": to_y * 4 + to_x * 2 + to_core}, device_id_type=MESH).start()

    def exchange_wait(buf, sem):
        others = buf.at[pl.ds(0, DEVICES - 1)]
        pltpu.make_async_copy(others, others, sem).wait()

    def gathered(buf):
        total = buf[0]
        for index in range(1, DEVICES):
            total = total + buf[index]
        return total

    EX_WEIGHT, EX_GRAD, EX_FIRST = range(3)

    def decay(state, factor):
        @pl.loop(0, ROWS // 8 * PIECES)
        def _(step):
            rows = pl.ds(pl.multiple_of(step // PIECES * 8, 8), 8)
            cols = pl.ds(pl.multiple_of(step % PIECES * PIECE, PIECE), PIECE)
            state[rows, cols] = state[rows, cols] * factor

    def four(rows, cols_at, part):
        total = params[rows, pl.ds(pl.multiple_of(part * COLS + cols_at, PIECE), PIECE)].astype(F32)
        for source in range(1, 4):
            total = total + params[rows, pl.ds(pl.multiple_of((2 * source + part) * COLS + cols_at, PIECE), PIECE)].astype(F32)
        return total

    def hop(half, chunk):
        rows = rows_of(half, chunk)
        return remote(relay.at[rows], grad.at[rows], hop_send.at[half], hop_recv.at[half, chunk], second[half])

    for chunk in range(RS_CHUNKS):
        for half in range(2):
            rows = rows_of(half, chunk)
            whole = params.at[rows]
            pltpu.make_async_copy(whole, whole, rs_recv.at[half, chunk]).wait()

            @pl.loop(0, RS_SIZES[chunk] // 16 * PIECES)
            def _(step):
                tile_rows = pl.ds(pl.multiple_of(half * HALF + RS_STARTS[chunk] + step // PIECES * 16, 16), 16)
                cols_at = step % PIECES * PIECE
                relay[tile_rows, pl.ds(pl.multiple_of(cols_at, PIECE), PIECE)] = four(tile_rows, cols_at, 1)

            hop(half, chunk).start()
        if chunk == 0:
            pl.semaphore_signal(plane_sem, inc=1, device_id=mirror, device_id_type=MESH)
        if chunk + 1 < RS_CHUNKS:
            load_own(chunk + 1)
        if chunk < 3:
            loads[chunk].start()
        if chunk == 1:
            loads[0].wait()
            for part in range(2):
                span = (part * (GROUPS // 2), (part + 1) * (GROUPS // 2))
                weight_buf[linear, 2 * part:2 * part + 2, :] = packed(lax.fori_loop(*span, weight_rows, jnp.zeros((8, 128), F32)))
        if chunk == 2:
            pl.semaphore_wait(plane_sem, 1)
            exchange(weight_buf, EX_WEIGHT)
            loads[1].wait()
            decay(one, BETA_ONE)
        if chunk == 3:
            loads[2].wait()
            decay(two, BETA_TWO)

    square = jnp.zeros((8, 128), F32)
    for chunk in range(RS_CHUNKS):
        for half in range(2):
            hop(half, chunk).wait_recv()

            def finish(step, total):
                tile_rows = pl.ds(pl.multiple_of(half * HALF + RS_STARTS[chunk] + step // PIECES * 16, 16), 16)
                cols_at = step % PIECES * PIECE
                cols = pl.ds(pl.multiple_of(cols_at, PIECE), PIECE)
                value = (grad[tile_rows, cols] + four(tile_rows, cols_at, 0)) * (1.0 / DATA)
                grad[tile_rows, cols] = value
                folded = fold_lanes(value * value)
                return total + (folded[0:8] + folded[8:16])

            square = lax.fori_loop(0, RS_SIZES[chunk] // 16 * PIECES, finish, square)

    norm_buf[linear] = jnp.sum(square, axis=0, keepdims=True)
    exchange(norm_buf, EX_GRAD)
    for half in range(2):
        rows = pl.ds(half * HALF, HALF)
        pltpu.make_async_copy(relay.at[rows], relay.at[rows], hop_send.at[half]).wait()
    exchange_wait(weight_buf, ex_recv.at[EX_WEIGHT])
    weights = gathered(weight_buf)
    weight_norm = jnp.sqrt(packed_totals(weights[0:2], 0, GROUPS // 2) + packed_totals(weights[2:4], GROUPS // 2, GROUPS))
    exchange_wait(norm_buf, ex_recv.at[EX_GRAD])
    grad_norm = jnp.sqrt(jnp.sum(gathered(norm_buf), axis=1, keepdims=True))
    clip = jnp.minimum(1.0, MAX_NORM / grad_norm)

    grad_one = (1.0 - BETA_ONE) * clip
    grad_two = (1.0 - BETA_TWO) ** 0.5 * clip

    def adam(start, stop):
        @pl.loop(start, stop)
        def _(group):
            rows = pl.ds(pl.multiple_of(group * 8, 8), 8)
            total = jnp.zeros((8, 128), F32)
            for i in range(COLS // ADAM_PIECE):
                cols = pl.ds(i * ADAM_PIECE, ADAM_PIECE)
                mean = grad[rows, cols]
                new_one = one[rows, cols] + grad_one * mean
                scaled = grad_two * mean
                new_two = two[rows, cols] + scaled * scaled
                one[rows, cols] = new_one
                two[rows, cols] = new_two
                direction = new_one / (jnp.sqrt(new_two) * (CORR_ONE / CORR_TWO ** 0.5) + CORR_ONE * EPSILON) + WEIGHT_DECAY * master[rows, cols]
                relay[rows, cols] = direction
                total = total + fold_lanes(direction * direction)
            part_buf[group] = total

    def row_sums(start, stop, place):
        tile = jnp.zeros((8, 128), F32)
        for group in range(start, stop):
            tile = jnp.where(lane == place(group), jnp.sum(part_buf[group], axis=1, keepdims=True), tile)
        return tile

    groups = [(start // 8, stop // 8) for start, stop in NORM_CHUNKS]

    def step_rates(number):
        if number == 0:
            exchange_wait(first_buf, ex_recv.at[EX_FIRST])
            total = first_totals(gathered(first_buf))
        else:
            exchange_wait(sq_buf.at[number - 1], ex_recv.at[EX_FIRST + number])
            total = packed_totals(gathered(sq_buf.at[number - 1]), *groups[number])
        return weight_norm / jnp.sqrt(total) * LEARN_RATE

    def ag_rows(chunk):
        return pl.ds(AG_STARTS[chunk], AG_SIZES[chunk])

    def update(number, rates):
        start, stop = NORM_CHUNKS[number]
        for chunk in range(AG_CHUNKS):
            if not start <= AG_STARTS[chunk] < stop:
                continue

            @pl.loop(0, AG_SIZES[chunk] // 16)
            def _(tile):
                group = AG_STARTS[chunk] // 8 + 2 * tile
                rows = pl.ds(pl.multiple_of(AG_STARTS[chunk] + tile * 16, 16), 16)
                rate = jnp.concatenate([jnp.sum(jnp.where(lane == group + i, rates, 0.0), axis=1, keepdims=True) for i in range(2)], axis=0)

                @pl.loop(0, PIECES)
                def _(i):
                    cols = pl.ds(pl.multiple_of(i * PIECE, PIECE), PIECE)
                    value = master[rows, cols] - rate * relay[rows, cols]
                    master[rows, cols] = value
                    params[rows, pl.ds(pl.multiple_of(me * COLS + i * PIECE, PIECE), PIECE)] = value.astype(BF16)

            rows = ag_rows(chunk)
            own = params.at[rows, block(me)]
            remote(own, own, ag_send.at[0], ag_x.at[chunk], near_x).start()
            remote(own, own, ag_send.at[1], ag_y.at[chunk], near_y).start()
            remote(own, own, ag_send.at[2], ag_o, other).start()

    adam(*groups[0])
    first_buf[linear] = jnp.sum(row_sums(*groups[0], lambda group: 8 * group + sub), axis=0, keepdims=True)
    adam(groups[1][0], groups[1][0] + 1)
    exchange(first_buf, EX_FIRST)
    adam(groups[1][0] + 1, groups[1][1])
    sq_buf[0, linear] = packed(row_sums(*groups[1], lambda group: 32 * (sub % 4) + group - groups[1][0]))
    adam(groups[2][0], groups[2][0] + 1)
    exchange(sq_buf.at[0], EX_FIRST + 1)
    update(0, step_rates(0))
    adam(groups[2][0] + 1, groups[2][1])
    sq_buf[1, linear] = packed(row_sums(*groups[2], lambda group: 32 * (sub % 4) + group - groups[2][0]))
    rates = step_rates(1)
    exchange(sq_buf.at[1], EX_FIRST + 2)
    update(1, rates)
    update(2, step_rates(2))

    def arrived(sem, source, rows):
        view = params.at[rows, block(source)]
        pltpu.make_async_copy(view, view, sem).wait()
        return view

    for chunk in range(AG_CHUNKS):
        rows = ag_rows(chunk)
        view = arrived(ag_x.at[chunk], near_x, rows)
        if AG_FAR_BY_Y[chunk]:
            remote(view, view, ag_send.at[1], ag_d.at[chunk], near_y).start()
        remote(view, view, ag_send.at[2], ag_o, other).start()
        view = arrived(ag_y.at[chunk], near_y, rows)
        if not AG_FAR_BY_Y[chunk]:
            remote(view, view, ag_send.at[0], ag_d.at[chunk], near_x).start()
        remote(view, view, ag_send.at[2], ag_o, other).start()

    for chunk in range(AG_CHUNKS):
        view = arrived(ag_d.at[chunk], diag, ag_rows(chunk))
        remote(view, view, ag_send.at[2], ag_o, other).start()

    half_cols = params.at[:, pl.ds(0, DATA // 2 * COLS)]
    pltpu.make_async_copy(half_cols, half_cols, ag_o).wait()
    pltpu.make_async_copy(half_cols, half_cols, ag_send.at[2]).wait()
    for direction in range(2):
        for part in (pl.ds(0, ROWS), pl.ds(0, HALF)):
            view = params.at[part, pl.ds(0, COLS)]
            pltpu.make_async_copy(view, view, ag_send.at[direction]).wait()
    for half in range(2):
        view = params.at[pl.ds(0, HALF), pl.ds(0, 6 * COLS)]
        pltpu.make_async_copy(view, view, rs_send.at[half]).wait()
    exchange_wait(weight_buf, ex_send.at[EX_WEIGHT])
    exchange_wait(norm_buf, ex_send.at[EX_GRAD])
    exchange_wait(first_buf, ex_send.at[EX_FIRST])
    for number in range(2):
        exchange_wait(sq_buf.at[number], ex_send.at[EX_FIRST + 1 + number])


def write_out(*refs):
    count = len(refs) // 2
    sem = refs[-1]
    copies = []
    for part in range(OUT_PARTS):
        rows = pl.ds(part * (ROWS // OUT_PARTS), ROWS // OUT_PARTS)
        for source, target in zip(refs[:count], refs[count:-1]):
            copies.append(pltpu.make_async_copy(source.at[rows], target.at[rows], sem.at[len(copies)]))
    for number, copy in enumerate(copies):
        copy.start(priority=number % 2)
    for copy in copies:
        copy.wait()


def solution(mesh):
    def device_step(local_grads, master, moment_one, moment_two):
        any_spec = pl.BlockSpec(memory_space=pl.ANY)
        vmem_spec = pl.BlockSpec(memory_space=pltpu.VMEM)
        state = pltpu.VMEM((ROWS, COLS), F32)
        dma = pltpu.SemaphoreType.DMA
        results = pl.pallas_call(
            kernel,
            name="lamb",
            out_shape=(pltpu.VMEM((ROWS, DATA * COLS), BF16), state, state, state),
            in_specs=[any_spec] * 4,
            out_specs=[vmem_spec] * 4,
            scratch_shapes=[
                pltpu.VMEM((ROWS, COLS), F32),
                pltpu.VMEM((ROWS, COLS), F32),
                pltpu.VMEM((DEVICES, 4, 128), F32),
                pltpu.VMEM((DEVICES, 1, 128), F32),
                pltpu.VMEM((DEVICES, 1, 128), F32),
                pltpu.VMEM((2, DEVICES, 2, 128), F32),
                pltpu.VMEM((ROWS // 8, 8, 128), F32),
                dma((3,)),
                dma((2, RS_CHUNKS)),
                dma((2,)),
                dma((2, RS_CHUNKS)),
                dma((2,)),
                dma((5,)),
                dma((5,)),
                dma((AG_CHUNKS,)),
                dma((AG_CHUNKS,)),
                dma((AG_CHUNKS,)),
                dma,
                dma((3,)),
                pltpu.SemaphoreType.REGULAR,
            ],
            compiler_params=pltpu.CompilerParams(collective_id=0, has_side_effects=True, vmem_limit_bytes=VMEM_LIMIT),
        )(local_grads, master, moment_one, moment_two)
        results = [pltpu.with_memory_space_constraint(value, pltpu.VMEM) for value in results]
        return tuple(pl.pallas_call(
            write_out,
            name="write_out",
            out_shape=[jax.ShapeDtypeStruct(value.shape, value.dtype) for value in results],
            in_specs=[vmem_spec] * 4,
            out_specs=[any_spec] * 4,
            scratch_shapes=[dma((4 * OUT_PARTS,))],
            compiler_params=pltpu.CompilerParams(vmem_limit_bytes=VMEM_LIMIT),
        )(*results))

    state_spec = P(None, ('model', 'data'))
    return jax.shard_map(device_step, mesh=mesh, in_specs=(P('data', None, 'model'), state_spec, state_spec, state_spec), out_specs=(P(None, 'model'), state_spec, state_spec, state_spec), check_vma=False)
```

```python
import jax
import jax.numpy as jnp
from jax import lax
from jax.experimental import pallas as pl
from jax.experimental.pallas import tpu as pltpu
from jax.sharding import PartitionSpec as P

STEP = 4
LEARN_RATE = 0.08
BETA_ONE = 0.9
BETA_TWO = 0.999
EPSILON = 1e-6
WEIGHT_DECAY = 0.01
MAX_NORM = 1.0
CORR_ONE = 1.0 - BETA_ONE ** STEP
CORR_TWO = 1.0 - BETA_TWO ** STEP

ROWS = 384
HALF = 192
GROUPS = ROWS // 8
COLS = 4096
DATA = 8
DEVICES = 16
PIECE = 1024
PIECES = COLS // PIECE
ADAM_PIECE = 1024
OUT_PARTS = 6
VMEM_LIMIT = 16 << 20

RS_SIZES = (48, 48, 48, 32, 16)
RS_CHUNKS = len(RS_SIZES)
RS_STARTS = tuple(sum(RS_SIZES[:i]) for i in range(RS_CHUNKS))
AG_SIZES = (16,) + (32,) * 10 + (16,) * 3
AG_FAR_BY_Y = (1,) + (0, 1) * 5 + (0, 1, 0)
AG_CHUNKS = len(AG_SIZES)
AG_STARTS = tuple(sum(AG_SIZES[:i]) for i in range(AG_CHUNKS))
NORM_CHUNKS = ((0, 16), (16, 208), (208, 384))

MESH = pl.DeviceIdType.MESH
F32 = jnp.float32
BF16 = jnp.bfloat16


def fold_lanes(values):
    total = values[:, 0:128]
    for group in range(1, values.shape[1] // 128):
        total = total + values[:, group * 128:(group + 1) * 128]
    return total


def packed_totals(rows, start, stop):
    lane = lax.broadcasted_iota(jnp.int32, (8, 128), 1)
    sub = lax.broadcasted_iota(jnp.int32, (8, 128), 0)
    value = jnp.where(sub < 4, jnp.broadcast_to(rows[0:1], (8, 128)), jnp.broadcast_to(rows[1:2], (8, 128)))
    tile = jnp.zeros((8, 128), F32)
    for group in range(start, stop):
        low, high = ((3, 4), (4, 7), (4, 8))[group % 3]
        part = lambda s: (s >= low).astype(jnp.int32) + (s >= high).astype(jnp.int32)
        same = (lane % 32 == group - start) & (part(sub) == part(sub // 4 * 4 + lane // 32))
        tile = jnp.where(lane == group, jnp.sum(jnp.where(same, value, 0.0), axis=1, keepdims=True), tile)
    return tile


def packed(tile):
    return jnp.concatenate([jnp.sum(tile[0:4], axis=0, keepdims=True), jnp.sum(tile[4:8], axis=0, keepdims=True)], axis=0)


def first_totals(row):
    lane = lax.broadcasted_iota(jnp.int32, (8, 128), 1)
    sub = lax.broadcasted_iota(jnp.int32, (8, 128), 0)
    tile = jnp.zeros((8, 128), F32)
    for group in range(NORM_CHUNKS[0][1] // 8):
        low, high = ((3, 4), (4, 7), (4, 8))[group % 3]
        part = lambda s: (s >= low).astype(jnp.int32) + (s >= high).astype(jnp.int32)
        same = (lane // 8 == group) & (part(sub) == part(lane % 8))
        total = jnp.sum(jnp.where(same, jnp.broadcast_to(row, (8, 128)), 0.0), axis=1, keepdims=True)
        tile = jnp.where(lane == group, total, tile)
    return tile


def kernel(grad_ref, master_ref, one_ref, two_ref, params, master, one, two, relay, grad, weight_buf, norm_buf, first_buf, sq_buf, part_buf,
           load_sem, rs_recv, rs_send, hop_recv, hop_send, ex_recv, ex_send, ag_x, ag_y, ag_d, ag_o, ag_send, plane_sem):
    model = lax.axis_index("model")
    me = lax.axis_index("data")
    linear = model * DATA + me
    core = me % 2
    x = (me // 2) % 2
    y = me // 4
    to_core = 1 - 2 * core
    near_x = me + 2 - 4 * x
    near_y = me + 4 - 8 * y
    diag = near_x + 4 - 8 * y
    other = me + to_core
    peer = lambda index: {"model": model, "data": index}
    block = lambda index: pl.ds(pl.multiple_of(index * COLS, COLS), COLS)

    loads = [pltpu.make_async_copy(source, target, load_sem.at[i])
             for i, (source, target) in enumerate(((master_ref, master), (one_ref, one), (two_ref, two)))]

    first = (near_x, near_y)
    second = (near_y, near_x)

    def rows_of(half, chunk):
        return pl.ds(half * HALF + RS_STARTS[chunk], RS_SIZES[chunk])

    barrier = pltpu.get_barrier_semaphore()

    mirror = {"model": 1 - model, "data": me}
    for neighbour in (peer(near_x), peer(near_x + to_core), peer(near_y), peer(near_y + to_core), mirror, peer(other)):
        pl.semaphore_signal(barrier, inc=1, device_id=neighbour, device_id_type=MESH)
    pl.semaphore_wait(barrier, 6)

    def remote(source, target, send, recv, index):
        return pltpu.make_async_remote_copy(src_ref=source, dst_ref=target, send_sem=send, recv_sem=recv,
                                            device_id=peer(index), device_id_type=MESH)

    for chunk in range(RS_CHUNKS):
        for half in range(2):
            rows = rows_of(half, chunk)
            recv = rs_recv.at[half, chunk]
            send = rs_send.at[half]
            for turn in range(2):
                shift = turn * to_core
                for part, owner in enumerate((first[half] + shift, diag + shift)):
                    remote(grad_ref.at[0, rows, block(owner)], params.at[rows, pl.ds((4 + 2 * turn + part) * COLS, COLS)], send, recv, first[half] + shift).start()
            for part, owner in enumerate((other, second[half] + to_core)):
                remote(grad_ref.at[0, rows, block(owner)], params.at[rows, pl.ds((2 + part) * COLS, COLS)], send, recv, other).start()

    def load_own(chunk):
        for half in range(2):
            rows = rows_of(half, chunk)
            for part, owner in enumerate((me, second[half])):
                pltpu.make_async_copy(grad_ref.at[0, rows, block(owner)], params.at[rows, pl.ds(part * COLS, COLS)], rs_recv.at[half, chunk]).start()

    load_own(0)

    lane = lax.broadcasted_iota(jnp.int32, (8, 128), 1)
    sub = lax.broadcasted_iota(jnp.int32, (8, 128), 0)

    def weight_rows(group, tile):
        rows = pl.ds(pl.multiple_of(group * 8, 8), 8)

        def piece(i, total):
            value = master[rows, pl.ds(pl.multiple_of(i * PIECE, PIECE), PIECE)]
            return total + fold_lanes(value * value)

        total = lax.fori_loop(0, PIECES, piece, jnp.zeros((8, 128), F32))
        return jnp.where(lane == 32 * (sub % 4) + group % (GROUPS // 2), jnp.sum(total, axis=1, keepdims=True), tile)


    def exchange(buf, number):
        for flips in reversed(range(1, DEVICES)):
            to_model, to_y, to_x, to_core = [at + (1 - 2 * at) * (flips >> bit & 1) for bit, at in zip((3, 2, 1, 0), (model, y, x, core))]
            pltpu.make_async_remote_copy(src_ref=buf.at[linear], dst_ref=buf.at[linear], send_sem=ex_send.at[number], recv_sem=ex_recv.at[number],
                                         device_id={"model": to_model, "data": to_y * 4 + to_x * 2 + to_core}, device_id_type=MESH).start()

    def exchange_wait(buf, sem):
        others = buf.at[pl.ds(0, DEVICES - 1)]
        pltpu.make_async_copy(others, others, sem).wait()

    def gathered(buf):
        total = buf[0]
        for index in range(1, DEVICES):
            total = total + buf[index]
        return total

    EX_WEIGHT, EX_GRAD, EX_FIRST = range(3)

    def decay(state, factor):
        @pl.loop(0, ROWS // 8 * PIECES)
        def _(step):
            rows = pl.ds(pl.multiple_of(step // PIECES * 8, 8), 8)
            cols = pl.ds(pl.multiple_of(step % PIECES * PIECE, PIECE), PIECE)
            state[rows, cols] = state[rows, cols] * factor

    def four(rows, cols_at, part):
        total = params[rows, pl.ds(pl.multiple_of(part * COLS + cols_at, PIECE), PIECE)].astype(F32)
        for source in range(1, 4):
            total = total + params[rows, pl.ds(pl.multiple_of((2 * source + part) * COLS + cols_at, PIECE), PIECE)].astype(F32)
        return total

    def hop(half, chunk):
        rows = rows_of(half, chunk)
        return remote(relay.at[rows], grad.at[rows], hop_send.at[half], hop_recv.at[half, chunk], second[half])

    for chunk in range(RS_CHUNKS):
        for half in range(2):
            rows = rows_of(half, chunk)
            whole = params.at[rows]
            pltpu.make_async_copy(whole, whole, rs_recv.at[half, chunk]).wait()

            @pl.loop(0, RS_SIZES[chunk] // 16 * PIECES)
            def _(step):
                tile_rows = pl.ds(pl.multiple_of(half * HALF + RS_STARTS[chunk] + step // PIECES * 16, 16), 16)
                cols_at = step % PIECES * PIECE
                relay[tile_rows, pl.ds(pl.multiple_of(cols_at, PIECE), PIECE)] = four(tile_rows, cols_at, 1)

            hop(half, chunk).start()
        if chunk == 0:
            pl.semaphore_signal(plane_sem, inc=1, device_id=mirror, device_id_type=MESH)
        if chunk + 1 < RS_CHUNKS:
            load_own(chunk + 1)
        if chunk < 3:
            loads[chunk].start()
        if chunk == 1:
            loads[0].wait()
            for part in range(2):
                span = (part * (GROUPS // 2), (part + 1) * (GROUPS // 2))
                weight_buf[linear, 2 * part:2 * part + 2, :] = packed(lax.fori_loop(*span, weight_rows, jnp.zeros((8, 128), F32)))
        if chunk == 2:
            pl.semaphore_wait(plane_sem, 1)
            loads[1].wait()
            decay(one, BETA_ONE)
        if chunk == 3:
            loads[2].wait()
            decay(two, BETA_TWO)

    square = jnp.zeros((8, 128), F32)
    for chunk in range(RS_CHUNKS):
        for half in range(2):
            hop(half, chunk).wait_recv()

            def finish(step, total):
                tile_rows = pl.ds(pl.multiple_of(half * HALF + RS_STARTS[chunk] + step // PIECES * 16, 16), 16)
                cols_at = step % PIECES * PIECE
                cols = pl.ds(pl.multiple_of(cols_at, PIECE), PIECE)
                value = (grad[tile_rows, cols] + four(tile_rows, cols_at, 0)) * (1.0 / DATA)
                grad[tile_rows, cols] = value
                folded = fold_lanes(value * value)
                return total + (folded[0:8] + folded[8:16])

            square = lax.fori_loop(0, RS_SIZES[chunk] // 16 * PIECES, finish, square)

    norm_buf[linear] = jnp.sum(square, axis=0, keepdims=True)
    exchange(norm_buf, EX_GRAD)
    exchange(weight_buf, EX_WEIGHT)
    for half in range(2):
        rows = pl.ds(half * HALF, HALF)
        pltpu.make_async_copy(relay.at[rows], relay.at[rows], hop_send.at[half]).wait()
    exchange_wait(norm_buf, ex_recv.at[EX_GRAD])
    grad_norm = jnp.sqrt(jnp.sum(gathered(norm_buf), axis=1, keepdims=True))
    clip = jnp.minimum(1.0, MAX_NORM / grad_norm)

    grad_one = (1.0 - BETA_ONE) * clip
    grad_two = (1.0 - BETA_TWO) ** 0.5 * clip

    def adam(start, stop):
        @pl.loop(start, stop)
        def _(group):
            rows = pl.ds(pl.multiple_of(group * 8, 8), 8)
            total = jnp.zeros((8, 128), F32)
            for i in range(COLS // ADAM_PIECE):
                cols = pl.ds(i * ADAM_PIECE, ADAM_PIECE)
                mean = grad[rows, cols]
                new_one = one[rows, cols] + grad_one * mean
                scaled = grad_two * mean
                new_two = two[rows, cols] + scaled * scaled
                one[rows, cols] = new_one
                two[rows, cols] = new_two
                direction = new_one / (jnp.sqrt(new_two) * (CORR_ONE / CORR_TWO ** 0.5) + CORR_ONE * EPSILON) + WEIGHT_DECAY * master[rows, cols]
                relay[rows, cols] = direction
                total = total + fold_lanes(direction * direction)
            part_buf[group] = total

    def row_sums(start, stop, place):
        tile = jnp.zeros((8, 128), F32)
        for group in range(start, stop):
            tile = jnp.where(lane == place(group), jnp.sum(part_buf[group], axis=1, keepdims=True), tile)
        return tile

    groups = [(start // 8, stop // 8) for start, stop in NORM_CHUNKS]

    def step_rates(weight_norm, number):
        if number == 0:
            exchange_wait(first_buf, ex_recv.at[EX_FIRST])
            total = first_totals(gathered(first_buf))
        else:
            exchange_wait(sq_buf.at[number - 1], ex_recv.at[EX_FIRST + number])
            total = packed_totals(gathered(sq_buf.at[number - 1]), *groups[number])
        return weight_norm / jnp.sqrt(total) * LEARN_RATE

    def ag_rows(chunk):
        return pl.ds(AG_STARTS[chunk], AG_SIZES[chunk])

    def update(number, rates):
        start, stop = NORM_CHUNKS[number]
        for chunk in range(AG_CHUNKS):
            if not start <= AG_STARTS[chunk] < stop:
                continue

            @pl.loop(0, AG_SIZES[chunk] // 16)
            def _(tile):
                group = AG_STARTS[chunk] // 8 + 2 * tile
                rows = pl.ds(pl.multiple_of(AG_STARTS[chunk] + tile * 16, 16), 16)
                rate = jnp.concatenate([jnp.sum(jnp.where(lane == group + i, rates, 0.0), axis=1, keepdims=True) for i in range(2)], axis=0)

                @pl.loop(0, PIECES)
                def _(i):
                    cols = pl.ds(pl.multiple_of(i * PIECE, PIECE), PIECE)
                    value = master[rows, cols] - rate * relay[rows, cols]
                    master[rows, cols] = value
                    params[rows, pl.ds(pl.multiple_of(me * COLS + i * PIECE, PIECE), PIECE)] = value.astype(BF16)

            rows = ag_rows(chunk)
            own = params.at[rows, block(me)]
            remote(own, own, ag_send.at[0], ag_x.at[chunk], near_x).start()
            remote(own, own, ag_send.at[1], ag_y.at[chunk], near_y).start()
            remote(own, own, ag_send.at[2], ag_o, other).start()

    adam(*groups[0])
    first_buf[linear] = jnp.sum(row_sums(*groups[0], lambda group: 8 * group + sub), axis=0, keepdims=True)
    adam(groups[1][0], groups[1][0] + 1)
    exchange(first_buf, EX_FIRST)
    adam(groups[1][0] + 1, groups[1][1])
    sq_buf[0, linear] = packed(row_sums(*groups[1], lambda group: 32 * (sub % 4) + group - groups[1][0]))
    adam(groups[2][0], groups[2][0] + 1)
    exchange(sq_buf.at[0], EX_FIRST + 1)
    exchange_wait(weight_buf, ex_recv.at[EX_WEIGHT])
    weights = gathered(weight_buf)
    weight_norm = jnp.sqrt(packed_totals(weights[0:2], 0, GROUPS // 2) + packed_totals(weights[2:4], GROUPS // 2, GROUPS))
    update(0, step_rates(weight_norm, 0))
    adam(groups[2][0] + 1, groups[2][1])
    sq_buf[1, linear] = packed(row_sums(*groups[2], lambda group: 32 * (sub % 4) + group - groups[2][0]))
    rates = step_rates(weight_norm, 1)
    exchange(sq_buf.at[1], EX_FIRST + 2)
    update(1, rates)
    update(2, step_rates(weight_norm, 2))

    def arrived(sem, source, rows):
        view = params.at[rows, block(source)]
        pltpu.make_async_copy(view, view, sem).wait()
        return view

    for chunk in range(AG_CHUNKS):
        rows = ag_rows(chunk)
        view = arrived(ag_x.at[chunk], near_x, rows)
        if AG_FAR_BY_Y[chunk]:
            remote(view, view, ag_send.at[1], ag_d.at[chunk], near_y).start()
        remote(view, view, ag_send.at[2], ag_o, other).start()
        view = arrived(ag_y.at[chunk], near_y, rows)
        if not AG_FAR_BY_Y[chunk]:
            remote(view, view, ag_send.at[0], ag_d.at[chunk], near_x).start()
        remote(view, view, ag_send.at[2], ag_o, other).start()

    for chunk in range(AG_CHUNKS):
        view = arrived(ag_d.at[chunk], diag, ag_rows(chunk))
        remote(view, view, ag_send.at[2], ag_o, other).start()

    half_cols = params.at[:, pl.ds(0, DATA // 2 * COLS)]
    pltpu.make_async_copy(half_cols, half_cols, ag_o).wait()
    pltpu.make_async_copy(half_cols, half_cols, ag_send.at[2]).wait()
    for direction in range(2):
        for part in (pl.ds(0, ROWS), pl.ds(0, HALF)):
            view = params.at[part, pl.ds(0, COLS)]
            pltpu.make_async_copy(view, view, ag_send.at[direction]).wait()
    for half in range(2):
        view = params.at[pl.ds(0, HALF), pl.ds(0, 6 * COLS)]
        pltpu.make_async_copy(view, view, rs_send.at[half]).wait()
    exchange_wait(weight_buf, ex_send.at[EX_WEIGHT])
    exchange_wait(norm_buf, ex_send.at[EX_GRAD])
    exchange_wait(first_buf, ex_send.at[EX_FIRST])
    for number in range(2):
        exchange_wait(sq_buf.at[number], ex_send.at[EX_FIRST + 1 + number])


def write_out(*refs):
    count = len(refs) // 2
    sem = refs[-1]
    copies = []
    for part in range(OUT_PARTS):
        rows = pl.ds(part * (ROWS // OUT_PARTS), ROWS // OUT_PARTS)
        for source, target in zip(refs[:count], refs[count:-1]):
            copies.append(pltpu.make_async_copy(source.at[rows], target.at[rows], sem.at[len(copies)]))
    for number, copy in enumerate(copies):
        copy.start(priority=number % 2)
    for copy in copies:
        copy.wait()


def solution(mesh):
    def device_step(local_grads, master, moment_one, moment_two):
        any_spec = pl.BlockSpec(memory_space=pl.ANY)
        vmem_spec = pl.BlockSpec(memory_space=pltpu.VMEM)
        state = pltpu.VMEM((ROWS, COLS), F32)
        dma = pltpu.SemaphoreType.DMA
        results = pl.pallas_call(
            kernel,
            name="lamb",
            out_shape=(pltpu.VMEM((ROWS, DATA * COLS), BF16), state, state, state),
            in_specs=[any_spec] * 4,
            out_specs=[vmem_spec] * 4,
            scratch_shapes=[
                pltpu.VMEM((ROWS, COLS), F32),
                pltpu.VMEM((ROWS, COLS), F32),
                pltpu.VMEM((DEVICES, 4, 128), F32),
                pltpu.VMEM((DEVICES, 1, 128), F32),
                pltpu.VMEM((DEVICES, 1, 128), F32),
                pltpu.VMEM((2, DEVICES, 2, 128), F32),
                pltpu.VMEM((ROWS // 8, 8, 128), F32),
                dma((3,)),
                dma((2, RS_CHUNKS)),
                dma((2,)),
                dma((2, RS_CHUNKS)),
                dma((2,)),
                dma((5,)),
                dma((5,)),
                dma((AG_CHUNKS,)),
                dma((AG_CHUNKS,)),
                dma((AG_CHUNKS,)),
                dma,
                dma((3,)),
                pltpu.SemaphoreType.REGULAR,
            ],
            compiler_params=pltpu.CompilerParams(collective_id=0, has_side_effects=True, vmem_limit_bytes=VMEM_LIMIT),
        )(local_grads, master, moment_one, moment_two)
        results = [pltpu.with_memory_space_constraint(value, pltpu.VMEM) for value in results]
        return tuple(pl.pallas_call(
            write_out,
            name="write_out",
            out_shape=[jax.ShapeDtypeStruct(value.shape, value.dtype) for value in results],
            in_specs=[vmem_spec] * 4,
            out_specs=[any_spec] * 4,
            scratch_shapes=[dma((4 * OUT_PARTS,))],
            compiler_params=pltpu.CompilerParams(vmem_limit_bytes=VMEM_LIMIT),
        )(*results))

    state_spec = P(None, ('model', 'data'))
    return jax.shard_map(device_step, mesh=mesh, in_specs=(P('data', None, 'model'), state_spec, state_spec, state_spec), out_specs=(P(None, 'model'), state_spec, state_spec, state_spec), check_vma=False)
```

```python
import jax
import jax.numpy as jnp
from jax import lax
from jax.experimental import pallas as pl
from jax.experimental.pallas import tpu as pltpu
from jax.sharding import PartitionSpec as P

STEP = 4
LEARN_RATE = 0.08
BETA_ONE = 0.9
BETA_TWO = 0.999
EPSILON = 1e-6
WEIGHT_DECAY = 0.01
MAX_NORM = 1.0
CORR_ONE = 1.0 - BETA_ONE ** STEP
CORR_TWO = 1.0 - BETA_TWO ** STEP

ROWS = 384
HALF = 192
GROUPS = ROWS // 8
COLS = 4096
DATA = 8
DEVICES = 16
PIECE = 1024
PIECES = COLS // PIECE
ADAM_PIECE = 1024
TAIL = 1024
OUT_PARTS = 6
VMEM_LIMIT = 16 << 20

RS_SIZES = (48, 48, 48, 32, 16)
RS_CHUNKS = len(RS_SIZES)
RS_STARTS = tuple(sum(RS_SIZES[:i]) for i in range(RS_CHUNKS))
AG_SIZES = (16,) + (32,) * 10 + (16,) * 3
AG_FAR_BY_Y = (1,) + (0, 1) * 5 + (0, 1, 0)
AG_CHUNKS = len(AG_SIZES)
AG_STARTS = tuple(sum(AG_SIZES[:i]) for i in range(AG_CHUNKS))
NORM_CHUNKS = ((0, 16), (16, 208), (208, 384))

MESH = pl.DeviceIdType.MESH
F32 = jnp.float32
BF16 = jnp.bfloat16


def fold_lanes(values):
    total = values[:, 0:128]
    for group in range(1, values.shape[1] // 128):
        total = total + values[:, group * 128:(group + 1) * 128]
    return total


def packed_totals(rows, start, stop):
    lane = lax.broadcasted_iota(jnp.int32, (8, 128), 1)
    sub = lax.broadcasted_iota(jnp.int32, (8, 128), 0)
    value = jnp.where(sub < 4, jnp.broadcast_to(rows[0:1], (8, 128)), jnp.broadcast_to(rows[1:2], (8, 128)))
    tile = jnp.zeros((8, 128), F32)
    for group in range(start, stop):
        low, high = ((3, 4), (4, 7), (4, 8))[group % 3]
        part = lambda s: (s >= low).astype(jnp.int32) + (s >= high).astype(jnp.int32)
        same = (lane % 32 == group - start) & (part(sub) == part(sub // 4 * 4 + lane // 32))
        tile = jnp.where(lane == group, jnp.sum(jnp.where(same, value, 0.0), axis=1, keepdims=True), tile)
    return tile


def packed(tile):
    return jnp.concatenate([jnp.sum(tile[0:4], axis=0, keepdims=True), jnp.sum(tile[4:8], axis=0, keepdims=True)], axis=0)


def first_totals(row):
    lane = lax.broadcasted_iota(jnp.int32, (8, 128), 1)
    sub = lax.broadcasted_iota(jnp.int32, (8, 128), 0)
    tile = jnp.zeros((8, 128), F32)
    for group in range(NORM_CHUNKS[0][1] // 8):
        low, high = ((3, 4), (4, 7), (4, 8))[group % 3]
        part = lambda s: (s >= low).astype(jnp.int32) + (s >= high).astype(jnp.int32)
        same = (lane // 8 == group) & (part(sub) == part(lane % 8))
        total = jnp.sum(jnp.where(same, jnp.broadcast_to(row, (8, 128)), 0.0), axis=1, keepdims=True)
        tile = jnp.where(lane == group, total, tile)
    return tile


def kernel(grad_ref, master_ref, one_ref, two_ref, params, master, one, two, relay, grad, weight_buf, norm_buf, first_buf, sq_buf, part_buf,
           load_sem, rs_recv, rs_send, hop_recv, hop_send, ex_recv, ex_send, ag_x, ag_y, ag_d, ag_o, ag_send, plane_sem, tail_recv, tail_send, last_recv, last_send):
    model = lax.axis_index("model")
    me = lax.axis_index("data")
    linear = model * DATA + me
    core = me % 2
    x = (me // 2) % 2
    y = me // 4
    to_core = 1 - 2 * core
    near_x = me + 2 - 4 * x
    near_y = me + 4 - 8 * y
    diag = near_x + 4 - 8 * y
    other = me + to_core
    peer = lambda index: {"model": model, "data": index}
    block = lambda index: pl.ds(pl.multiple_of(index * COLS, COLS), COLS)

    loads = [pltpu.make_async_copy(source, target, load_sem.at[i])
             for i, (source, target) in enumerate(((master_ref, master), (one_ref, one), (two_ref, two)))]

    first = (near_x, near_y)
    second = (near_y, near_x)

    def rows_of(half, chunk):
        return pl.ds(half * HALF + RS_STARTS[chunk], RS_SIZES[chunk])

    barrier = pltpu.get_barrier_semaphore()

    mirror = {"model": 1 - model, "data": me}
    for neighbour in (peer(near_x), peer(near_x + to_core), peer(near_y), peer(near_y + to_core), mirror, peer(other)):
        pl.semaphore_signal(barrier, inc=1, device_id=neighbour, device_id_type=MESH)
    pl.semaphore_wait(barrier, 6)

    def remote(source, target, send, recv, index):
        return pltpu.make_async_remote_copy(src_ref=source, dst_ref=target, send_sem=send, recv_sem=recv,
                                            device_id=peer(index), device_id_type=MESH)

    for chunk in range(RS_CHUNKS):
        for half in range(2):
            rows = rows_of(half, chunk)
            recv = rs_recv.at[half, chunk]
            send = rs_send.at[half]
            for turn in range(2):
                shift = turn * to_core
                for part, owner in enumerate((first[half] + shift, diag + shift)):
                    remote(grad_ref.at[0, rows, block(owner)], params.at[rows, pl.ds((4 + 2 * turn + part) * COLS, COLS)], send, recv, first[half] + shift).start()
            for part, owner in enumerate((other, second[half] + to_core)):
                remote(grad_ref.at[0, rows, block(owner)], params.at[rows, pl.ds((2 + part) * COLS, COLS)], send, recv, other).start()

    def load_own(chunk):
        for half in range(2):
            rows = rows_of(half, chunk)
            for part, owner in enumerate((me, second[half])):
                pltpu.make_async_copy(grad_ref.at[0, rows, block(owner)], params.at[rows, pl.ds(part * COLS, COLS)], rs_recv.at[half, chunk]).start()

    load_own(0)

    lane = lax.broadcasted_iota(jnp.int32, (8, 128), 1)
    sub = lax.broadcasted_iota(jnp.int32, (8, 128), 0)

    def weight_rows(group, tile):
        rows = pl.ds(pl.multiple_of(group * 8, 8), 8)

        def piece(i, total):
            value = master[rows, pl.ds(pl.multiple_of(i * PIECE, PIECE), PIECE)]
            return total + fold_lanes(value * value)

        total = lax.fori_loop(0, PIECES, piece, jnp.zeros((8, 128), F32))
        return jnp.where(lane == 32 * (sub % 4) + group % (GROUPS // 2), jnp.sum(total, axis=1, keepdims=True), tile)


    def exchange(buf, number):
        for flips in reversed(range(1, DEVICES)):
            to_model, to_y, to_x, to_core = [at + (1 - 2 * at) * (flips >> bit & 1) for bit, at in zip((3, 2, 1, 0), (model, y, x, core))]
            pltpu.make_async_remote_copy(src_ref=buf.at[linear], dst_ref=buf.at[linear], send_sem=ex_send.at[number], recv_sem=ex_recv.at[number],
                                         device_id={"model": to_model, "data": to_y * 4 + to_x * 2 + to_core}, device_id_type=MESH).start()

    def exchange_wait(buf, sem):
        others = buf.at[pl.ds(0, DEVICES - 1)]
        pltpu.make_async_copy(others, others, sem).wait()

    def gathered(buf):
        total = buf[0]
        for index in range(1, DEVICES):
            total = total + buf[index]
        return total

    EX_WEIGHT, EX_GRAD, EX_FIRST = range(3)

    def decay(state, factor):
        @pl.loop(0, ROWS // 8 * PIECES)
        def _(step):
            rows = pl.ds(pl.multiple_of(step // PIECES * 8, 8), 8)
            cols = pl.ds(pl.multiple_of(step % PIECES * PIECE, PIECE), PIECE)
            state[rows, cols] = state[rows, cols] * factor

    def four(rows, cols_at, part):
        total = params[rows, pl.ds(pl.multiple_of(part * COLS + cols_at, PIECE), PIECE)].astype(F32)
        for source in range(1, 4):
            total = total + params[rows, pl.ds(pl.multiple_of((2 * source + part) * COLS + cols_at, PIECE), PIECE)].astype(F32)
        return total

    def hop(half, chunk):
        rows = rows_of(half, chunk)
        return remote(relay.at[rows], grad.at[rows], hop_send.at[half], hop_recv.at[half, chunk], second[half])

    for chunk in range(RS_CHUNKS):
        for half in range(2):
            rows = rows_of(half, chunk)
            whole = params.at[rows]
            pltpu.make_async_copy(whole, whole, rs_recv.at[half, chunk]).wait()

            @pl.loop(0, RS_SIZES[chunk] // 16 * PIECES)
            def _(step):
                tile_rows = pl.ds(pl.multiple_of(half * HALF + RS_STARTS[chunk] + step // PIECES * 16, 16), 16)
                cols_at = step % PIECES * PIECE
                relay[tile_rows, pl.ds(pl.multiple_of(cols_at, PIECE), PIECE)] = four(tile_rows, cols_at, 1)

            hop(half, chunk).start()
        if chunk == 0:
            pl.semaphore_signal(plane_sem, inc=1, device_id=mirror, device_id_type=MESH)
        if chunk + 1 < RS_CHUNKS:
            load_own(chunk + 1)
        if chunk < 3:
            loads[chunk].start()
        if chunk == 1:
            loads[0].wait()
            for part in range(2):
                span = (part * (GROUPS // 2), (part + 1) * (GROUPS // 2))
                weight_buf[linear, 2 * part:2 * part + 2, :] = packed(lax.fori_loop(*span, weight_rows, jnp.zeros((8, 128), F32)))
        if chunk == 2:
            pl.semaphore_wait(plane_sem, 1)
            loads[1].wait()
            decay(one, BETA_ONE)
        if chunk == 3:
            loads[2].wait()
            decay(two, BETA_TWO)

    square = jnp.zeros((8, 128), F32)
    for chunk in range(RS_CHUNKS):
        for half in range(2):
            hop(half, chunk).wait_recv()

            def finish(step, total):
                tile_rows = pl.ds(pl.multiple_of(half * HALF + RS_STARTS[chunk] + step // PIECES * 16, 16), 16)
                cols_at = step % PIECES * PIECE
                cols = pl.ds(pl.multiple_of(cols_at, PIECE), PIECE)
                value = (grad[tile_rows, cols] + four(tile_rows, cols_at, 0)) * (1.0 / DATA)
                grad[tile_rows, cols] = value
                folded = fold_lanes(value * value)
                return total + (folded[0:8] + folded[8:16])

            square = lax.fori_loop(0, RS_SIZES[chunk] // 16 * PIECES, finish, square)

    norm_buf[linear] = jnp.sum(square, axis=0, keepdims=True)
    exchange(norm_buf, EX_GRAD)
    exchange(weight_buf, EX_WEIGHT)
    for half in range(2):
        rows = pl.ds(half * HALF, HALF)
        pltpu.make_async_copy(relay.at[rows], relay.at[rows], hop_send.at[half]).wait()
    exchange_wait(norm_buf, ex_recv.at[EX_GRAD])
    grad_norm = jnp.sqrt(jnp.sum(gathered(norm_buf), axis=1, keepdims=True))
    clip = jnp.minimum(1.0, MAX_NORM / grad_norm)

    grad_one = (1.0 - BETA_ONE) * clip
    grad_two = (1.0 - BETA_TWO) ** 0.5 * clip

    def adam(start, stop):
        @pl.loop(start, stop)
        def _(group):
            rows = pl.ds(pl.multiple_of(group * 8, 8), 8)
            total = jnp.zeros((8, 128), F32)
            for i in range(COLS // ADAM_PIECE):
                cols = pl.ds(i * ADAM_PIECE, ADAM_PIECE)
                mean = grad[rows, cols]
                new_one = one[rows, cols] + grad_one * mean
                scaled = grad_two * mean
                new_two = two[rows, cols] + scaled * scaled
                one[rows, cols] = new_one
                two[rows, cols] = new_two
                direction = new_one / (jnp.sqrt(new_two) * (CORR_ONE / CORR_TWO ** 0.5) + CORR_ONE * EPSILON) + WEIGHT_DECAY * master[rows, cols]
                relay[rows, cols] = direction
                total = total + fold_lanes(direction * direction)
            part_buf[group] = total

    def row_sums(start, stop, place):
        tile = jnp.zeros((8, 128), F32)
        for group in range(start, stop):
            tile = jnp.where(lane == place(group), jnp.sum(part_buf[group], axis=1, keepdims=True), tile)
        return tile

    groups = [(start // 8, stop // 8) for start, stop in NORM_CHUNKS]

    def step_rates(weight_norm, number):
        if number == 0:
            exchange_wait(first_buf, ex_recv.at[EX_FIRST])
            total = first_totals(gathered(first_buf))
        else:
            exchange_wait(sq_buf.at[number - 1], ex_recv.at[EX_FIRST + number])
            total = packed_totals(gathered(sq_buf.at[number - 1]), *groups[number])
        return weight_norm / jnp.sqrt(total) * LEARN_RATE

    def ag_rows(chunk):
        return pl.ds(AG_STARTS[chunk], AG_SIZES[chunk])

    def update(number, rates):
        start, stop = NORM_CHUNKS[number]
        for chunk in range(AG_CHUNKS):
            if not start <= AG_STARTS[chunk] < stop:
                continue

            @pl.loop(0, AG_SIZES[chunk] // 16)
            def _(tile):
                group = AG_STARTS[chunk] // 8 + 2 * tile
                rows = pl.ds(pl.multiple_of(AG_STARTS[chunk] + tile * 16, 16), 16)
                rate = jnp.concatenate([jnp.sum(jnp.where(lane == group + i, rates, 0.0), axis=1, keepdims=True) for i in range(2)], axis=0)

                @pl.loop(0, PIECES)
                def _(i):
                    cols = pl.ds(pl.multiple_of(i * PIECE, PIECE), PIECE)
                    value = master[rows, cols] - rate * relay[rows, cols]
                    master[rows, cols] = value
                    params[rows, pl.ds(pl.multiple_of(me * COLS + i * PIECE, PIECE), PIECE)] = value.astype(BF16)

            rows = ag_rows(chunk)
            own = params.at[rows, block(me)]
            remote(own, own, ag_send.at[0], ag_x.at[chunk], near_x).start()
            remote(own, own, ag_send.at[1], ag_y.at[chunk], near_y).start()
            remote(own, own, ag_send.at[2], ag_o, other).start()

    adam(*groups[0])
    first_buf[linear] = jnp.sum(row_sums(*groups[0], lambda group: 8 * group + sub), axis=0, keepdims=True)
    adam(groups[1][0], groups[1][0] + 1)
    exchange(first_buf, EX_FIRST)
    adam(groups[1][0] + 1, groups[1][1])
    sq_buf[0, linear] = packed(row_sums(*groups[1], lambda group: 32 * (sub % 4) + group - groups[1][0]))
    adam(groups[2][0], groups[2][0] + 1)
    exchange(sq_buf.at[0], EX_FIRST + 1)
    exchange_wait(weight_buf, ex_recv.at[EX_WEIGHT])
    weights = gathered(weight_buf)
    weight_norm = jnp.sqrt(packed_totals(weights[0:2], 0, GROUPS // 2) + packed_totals(weights[2:4], GROUPS // 2, GROUPS))
    update(0, step_rates(weight_norm, 0))
    adam(groups[2][0] + 1, groups[2][1])
    sq_buf[1, linear] = packed(row_sums(*groups[2], lambda group: 32 * (sub % 4) + group - groups[2][0]))
    rates = step_rates(weight_norm, 1)
    exchange(sq_buf.at[1], EX_FIRST + 2)
    update(1, rates)
    update(2, step_rates(weight_norm, 2))

    def arrived(sem, source, rows):
        view = params.at[rows, block(source)]
        pltpu.make_async_copy(view, view, sem).wait()
        return view

    def body_of(chunk, source):
        return params.at[ag_rows(chunk), pl.ds(pl.multiple_of(source * COLS, COLS), COLS - TAIL)]

    def pass_far(chunk, source, direction, target):
        last = chunk - (AG_CHUNKS - 2)
        if last < 0:
            whole = params.at[ag_rows(chunk), block(source)]
            remote(whole, whole, ag_send.at[direction], ag_d.at[chunk], target).start()
            return
        body = body_of(chunk, source)
        remote(body, body, ag_send.at[direction], ag_d.at[chunk], target).start()
        tail = params.at[ag_rows(chunk), pl.ds(pl.multiple_of(source * COLS + COLS - TAIL, TAIL), TAIL)]
        remote(tail, tail, ag_send.at[direction], tail_recv.at[0, last], target).start()
        remote(tail, tail, tail_send.at[last], tail_recv.at[1, last], target + to_core).start()

    for chunk in range(AG_CHUNKS):
        rows = ag_rows(chunk)
        view = arrived(ag_x.at[chunk], near_x, rows)
        if AG_FAR_BY_Y[chunk]:
            pass_far(chunk, near_x, 1, near_y)
        remote(view, view, ag_send.at[2], ag_o, other).start()
        view = arrived(ag_y.at[chunk], near_y, rows)
        if not AG_FAR_BY_Y[chunk]:
            pass_far(chunk, near_y, 0, near_x)
        remote(view, view, ag_send.at[2], ag_o, other).start()

    for chunk in range(AG_CHUNKS):
        last = chunk - (AG_CHUNKS - 2)
        if last < 0:
            view = arrived(ag_d.at[chunk], diag, ag_rows(chunk))
            remote(view, view, ag_send.at[2], ag_o, other).start()
        else:
            view = body_of(chunk, diag)
            pltpu.make_async_copy(view, view, ag_d.at[chunk]).wait()
            remote(view, view, last_send.at[last], last_recv.at[last], other).start()

    half_cols = params.at[pl.ds(0, ROWS - 8), pl.ds(0, DATA // 2 * COLS)]
    for last in range(2):
        tail = params.at[pl.ds(0, 16), pl.ds(0, TAIL)]
        for sem in (tail_recv.at[0, last], tail_recv.at[1, last], tail_send.at[last]):
            pltpu.make_async_copy(tail, tail, sem).wait()
        body = params.at[pl.ds(0, 16), pl.ds(0, COLS - TAIL)]
        for sem in (last_recv.at[last], last_send.at[last]):
            pltpu.make_async_copy(body, body, sem).wait()
    pltpu.make_async_copy(half_cols, half_cols, ag_o).wait()
    pltpu.make_async_copy(half_cols, half_cols, ag_send.at[2]).wait()
    for direction in range(2):
        for part in (pl.ds(0, ROWS), pl.ds(0, HALF)):
            view = params.at[part, pl.ds(0, COLS)]
            pltpu.make_async_copy(view, view, ag_send.at[direction]).wait()
    for half in range(2):
        view = params.at[pl.ds(0, HALF), pl.ds(0, 6 * COLS)]
        pltpu.make_async_copy(view, view, rs_send.at[half]).wait()
    exchange_wait(weight_buf, ex_send.at[EX_WEIGHT])
    exchange_wait(norm_buf, ex_send.at[EX_GRAD])
    exchange_wait(first_buf, ex_send.at[EX_FIRST])
    for number in range(2):
        exchange_wait(sq_buf.at[number], ex_send.at[EX_FIRST + 1 + number])


def write_out(*refs):
    count = len(refs) // 2
    sem = refs[-1]
    copies = []
    for part in range(OUT_PARTS):
        rows = pl.ds(part * (ROWS // OUT_PARTS), ROWS // OUT_PARTS)
        for source, target in zip(refs[:count], refs[count:-1]):
            copies.append(pltpu.make_async_copy(source.at[rows], target.at[rows], sem.at[len(copies)]))
    for number, copy in enumerate(copies):
        copy.start(priority=number % 2)
    for copy in copies:
        copy.wait()


def solution(mesh):
    def device_step(local_grads, master, moment_one, moment_two):
        any_spec = pl.BlockSpec(memory_space=pl.ANY)
        vmem_spec = pl.BlockSpec(memory_space=pltpu.VMEM)
        state = pltpu.VMEM((ROWS, COLS), F32)
        dma = pltpu.SemaphoreType.DMA
        results = pl.pallas_call(
            kernel,
            name="lamb",
            out_shape=(pltpu.VMEM((ROWS, DATA * COLS), BF16), state, state, state),
            in_specs=[any_spec] * 4,
            out_specs=[vmem_spec] * 4,
            scratch_shapes=[
                pltpu.VMEM((ROWS, COLS), F32),
                pltpu.VMEM((ROWS, COLS), F32),
                pltpu.VMEM((DEVICES, 4, 128), F32),
                pltpu.VMEM((DEVICES, 1, 128), F32),
                pltpu.VMEM((DEVICES, 1, 128), F32),
                pltpu.VMEM((2, DEVICES, 2, 128), F32),
                pltpu.VMEM((ROWS // 8, 8, 128), F32),
                dma((3,)),
                dma((2, RS_CHUNKS)),
                dma((2,)),
                dma((2, RS_CHUNKS)),
                dma((2,)),
                dma((5,)),
                dma((5,)),
                dma((AG_CHUNKS,)),
                dma((AG_CHUNKS,)),
                dma((AG_CHUNKS,)),
                dma,
                dma((3,)),
                pltpu.SemaphoreType.REGULAR,
                dma((2, 2)),
                dma((2,)),
                dma((2,)),
                dma((2,)),
            ],
            compiler_params=pltpu.CompilerParams(collective_id=0, has_side_effects=True, vmem_limit_bytes=VMEM_LIMIT),
        )(local_grads, master, moment_one, moment_two)
        results = [pltpu.with_memory_space_constraint(value, pltpu.VMEM) for value in results]
        return tuple(pl.pallas_call(
            write_out,
            name="write_out",
            out_shape=[jax.ShapeDtypeStruct(value.shape, value.dtype) for value in results],
            in_specs=[vmem_spec] * 4,
            out_specs=[any_spec] * 4,
            scratch_shapes=[dma((4 * OUT_PARTS,))],
            compiler_params=pltpu.CompilerParams(vmem_limit_bytes=VMEM_LIMIT),
        )(*results))

    state_spec = P(None, ('model', 'data'))
    return jax.shard_map(device_step, mesh=mesh, in_specs=(P('data', None, 'model'), state_spec, state_spec, state_spec), out_specs=(P(None, 'model'), state_spec, state_spec, state_spec), check_vma=False)
```

```python
import jax
import jax.numpy as jnp
from jax import lax
from jax.experimental import pallas as pl
from jax.experimental.pallas import tpu as pltpu
from jax.sharding import PartitionSpec as P

STEP = 4
LEARN_RATE = 0.08
BETA_ONE = 0.9
BETA_TWO = 0.999
EPSILON = 1e-6
WEIGHT_DECAY = 0.01
MAX_NORM = 1.0
CORR_ONE = 1.0 - BETA_ONE ** STEP
CORR_TWO = 1.0 - BETA_TWO ** STEP

ROWS = 384
HALF = 192
GROUPS = ROWS // 8
COLS = 4096
DATA = 8
DEVICES = 16
PIECE = 1024
PIECES = COLS // PIECE
ADAM_PIECE = 1024
OUT_PARTS = 12
VMEM_LIMIT = 16 << 20

RS_SIZES = (48, 48, 48, 32, 16)
RS_CHUNKS = len(RS_SIZES)
RS_STARTS = tuple(sum(RS_SIZES[:i]) for i in range(RS_CHUNKS))
AG_SIZES = (16,) + (32,) * 10 + (16,) * 3
AG_FAR_BY_Y = (1,) + (0, 1) * 5 + (0, 1, 0)
AG_CHUNKS = len(AG_SIZES)
AG_STARTS = tuple(sum(AG_SIZES[:i]) for i in range(AG_CHUNKS))
NORM_CHUNKS = ((0, 16), (16, 208), (208, 384))

MESH = pl.DeviceIdType.MESH
F32 = jnp.float32
BF16 = jnp.bfloat16


def fold_lanes(values):
    total = values[:, 0:128]
    for group in range(1, values.shape[1] // 128):
        total = total + values[:, group * 128:(group + 1) * 128]
    return total


def packed_totals(rows, start, stop):
    lane = lax.broadcasted_iota(jnp.int32, (8, 128), 1)
    sub = lax.broadcasted_iota(jnp.int32, (8, 128), 0)
    value = jnp.where(sub < 4, jnp.broadcast_to(rows[0:1], (8, 128)), jnp.broadcast_to(rows[1:2], (8, 128)))
    tile = jnp.zeros((8, 128), F32)
    for group in range(start, stop):
        low, high = ((3, 4), (4, 7), (4, 8))[group % 3]
        part = lambda s: (s >= low).astype(jnp.int32) + (s >= high).astype(jnp.int32)
        same = (lane % 32 == group - start) & (part(sub) == part(sub // 4 * 4 + lane // 32))
        tile = jnp.where(lane == group, jnp.sum(jnp.where(same, value, 0.0), axis=1, keepdims=True), tile)
    return tile


def packed(tile):
    return jnp.concatenate([jnp.sum(tile[0:4], axis=0, keepdims=True), jnp.sum(tile[4:8], axis=0, keepdims=True)], axis=0)


def first_totals(row):
    lane = lax.broadcasted_iota(jnp.int32, (8, 128), 1)
    sub = lax.broadcasted_iota(jnp.int32, (8, 128), 0)
    tile = jnp.zeros((8, 128), F32)
    for group in range(NORM_CHUNKS[0][1] // 8):
        low, high = ((3, 4), (4, 7), (4, 8))[group % 3]
        part = lambda s: (s >= low).astype(jnp.int32) + (s >= high).astype(jnp.int32)
        same = (lane // 8 == group) & (part(sub) == part(lane % 8))
        total = jnp.sum(jnp.where(same, jnp.broadcast_to(row, (8, 128)), 0.0), axis=1, keepdims=True)
        tile = jnp.where(lane == group, total, tile)
    return tile


def kernel(grad_ref, master_ref, one_ref, two_ref, params, master, one, two, relay, grad, weight_buf, norm_buf, first_buf, sq_buf, part_buf,
           load_sem, rs_recv, rs_send, hop_recv, hop_send, ex_recv, ex_send, ag_x, ag_y, ag_d, ag_o, ag_send, plane_sem):
    model = lax.axis_index("model")
    me = lax.axis_index("data")
    linear = model * DATA + me
    core = me % 2
    x = (me // 2) % 2
    y = me // 4
    to_core = 1 - 2 * core
    near_x = me + 2 - 4 * x
    near_y = me + 4 - 8 * y
    diag = near_x + 4 - 8 * y
    other = me + to_core
    peer = lambda index: {"model": model, "data": index}
    block = lambda index: pl.ds(pl.multiple_of(index * COLS, COLS), COLS)

    loads = [pltpu.make_async_copy(source, target, load_sem.at[i])
             for i, (source, target) in enumerate(((master_ref, master), (one_ref, one), (two_ref, two)))]

    first = (near_x, near_y)
    second = (near_y, near_x)

    def rows_of(half, chunk):
        return pl.ds(half * HALF + RS_STARTS[chunk], RS_SIZES[chunk])

    barrier = pltpu.get_barrier_semaphore()

    mirror = {"model": 1 - model, "data": me}
    for neighbour in (peer(near_x), peer(near_x + to_core), peer(near_y), peer(near_y + to_core), mirror, peer(other)):
        pl.semaphore_signal(barrier, inc=1, device_id=neighbour, device_id_type=MESH)
    pl.semaphore_wait(barrier, 6)

    def remote(source, target, send, recv, index):
        return pltpu.make_async_remote_copy(src_ref=source, dst_ref=target, send_sem=send, recv_sem=recv,
                                            device_id=peer(index), device_id_type=MESH)

    for chunk in range(RS_CHUNKS):
        for half in range(2):
            rows = rows_of(half, chunk)
            recv = rs_recv.at[half, chunk]
            send = rs_send.at[half]
            for turn in range(2):
                shift = turn * to_core
                for part, owner in enumerate((first[half] + shift, diag + shift)):
                    remote(grad_ref.at[0, rows, block(owner)], params.at[rows, pl.ds((4 + 2 * turn + part) * COLS, COLS)], send, recv, first[half] + shift).start()
            for part, owner in enumerate((other, second[half] + to_core)):
                remote(grad_ref.at[0, rows, block(owner)], params.at[rows, pl.ds((2 + part) * COLS, COLS)], send, recv, other).start()

    def load_own(chunk):
        for half in range(2):
            rows = rows_of(half, chunk)
            for part, owner in enumerate((me, second[half])):
                pltpu.make_async_copy(grad_ref.at[0, rows, block(owner)], params.at[rows, pl.ds(part * COLS, COLS)], rs_recv.at[half, chunk]).start()

    load_own(0)

    lane = lax.broadcasted_iota(jnp.int32, (8, 128), 1)
    sub = lax.broadcasted_iota(jnp.int32, (8, 128), 0)

    def weight_rows(group, tile):
        rows = pl.ds(pl.multiple_of(group * 8, 8), 8)

        def piece(i, total):
            value = master[rows, pl.ds(pl.multiple_of(i * PIECE, PIECE), PIECE)]
            return total + fold_lanes(value * value)

        total = lax.fori_loop(0, PIECES, piece, jnp.zeros((8, 128), F32))
        return jnp.where(lane == 32 * (sub % 4) + group % (GROUPS // 2), jnp.sum(total, axis=1, keepdims=True), tile)


    def exchange(buf, number):
        for flips in reversed(range(1, DEVICES)):
            to_model, to_y, to_x, to_core = [at + (1 - 2 * at) * (flips >> bit & 1) for bit, at in zip((3, 2, 1, 0), (model, y, x, core))]
            pltpu.make_async_remote_copy(src_ref=buf.at[linear], dst_ref=buf.at[linear], send_sem=ex_send.at[number], recv_sem=ex_recv.at[number],
                                         device_id={"model": to_model, "data": to_y * 4 + to_x * 2 + to_core}, device_id_type=MESH).start()

    def exchange_wait(buf, sem):
        others = buf.at[pl.ds(0, DEVICES - 1)]
        pltpu.make_async_copy(others, others, sem).wait()

    def gathered(buf):
        total = buf[0]
        for index in range(1, DEVICES):
            total = total + buf[index]
        return total

    EX_WEIGHT, EX_GRAD, EX_FIRST = range(3)

    def decay(state, factor):
        @pl.loop(0, ROWS // 8 * PIECES)
        def _(step):
            rows = pl.ds(pl.multiple_of(step // PIECES * 8, 8), 8)
            cols = pl.ds(pl.multiple_of(step % PIECES * PIECE, PIECE), PIECE)
            state[rows, cols] = state[rows, cols] * factor

    def four(rows, cols_at, part):
        total = params[rows, pl.ds(pl.multiple_of(part * COLS + cols_at, PIECE), PIECE)].astype(F32)
        for source in range(1, 4):
            total = total + params[rows, pl.ds(pl.multiple_of((2 * source + part) * COLS + cols_at, PIECE), PIECE)].astype(F32)
        return total

    def hop(half, chunk):
        rows = rows_of(half, chunk)
        return remote(relay.at[rows], grad.at[rows], hop_send.at[half], hop_recv.at[half, chunk], second[half])

    for chunk in range(RS_CHUNKS):
        for half in range(2):
            rows = rows_of(half, chunk)
            whole = params.at[rows]
            pltpu.make_async_copy(whole, whole, rs_recv.at[half, chunk]).wait()

            @pl.loop(0, RS_SIZES[chunk] // 16 * PIECES)
            def _(step):
                tile_rows = pl.ds(pl.multiple_of(half * HALF + RS_STARTS[chunk] + step // PIECES * 16, 16), 16)
                cols_at = step % PIECES * PIECE
                relay[tile_rows, pl.ds(pl.multiple_of(cols_at, PIECE), PIECE)] = four(tile_rows, cols_at, 1)

            hop(half, chunk).start()
        if chunk == 0:
            pl.semaphore_signal(plane_sem, inc=1, device_id=mirror, device_id_type=MESH)
        if chunk + 1 < RS_CHUNKS:
            load_own(chunk + 1)
        if chunk < 3:
            loads[chunk].start()
        if chunk == 1:
            loads[0].wait()
            for part in range(2):
                span = (part * (GROUPS // 2), (part + 1) * (GROUPS // 2))
                weight_buf[linear, 2 * part:2 * part + 2, :] = packed(lax.fori_loop(*span, weight_rows, jnp.zeros((8, 128), F32)))
        if chunk == 2:
            pl.semaphore_wait(plane_sem, 1)
            loads[1].wait()
            decay(one, BETA_ONE)
        if chunk == 3:
            loads[2].wait()
            decay(two, BETA_TWO)

    square = jnp.zeros((8, 128), F32)
    for chunk in range(RS_CHUNKS):
        for half in range(2):
            hop(half, chunk).wait_recv()

            def finish(step, total):
                tile_rows = pl.ds(pl.multiple_of(half * HALF + RS_STARTS[chunk] + step // PIECES * 16, 16), 16)
                cols_at = step % PIECES * PIECE
                cols = pl.ds(pl.multiple_of(cols_at, PIECE), PIECE)
                value = (grad[tile_rows, cols] + four(tile_rows, cols_at, 0)) * (1.0 / DATA)
                grad[tile_rows, cols] = value
                folded = fold_lanes(value * value)
                return total + (folded[0:8] + folded[8:16])

            square = lax.fori_loop(0, RS_SIZES[chunk] // 16 * PIECES, finish, square)

    norm_buf[linear] = jnp.sum(square, axis=0, keepdims=True)
    exchange(norm_buf, EX_GRAD)
    exchange(weight_buf, EX_WEIGHT)
    for half in range(2):
        rows = pl.ds(half * HALF, HALF)
        pltpu.make_async_copy(relay.at[rows], relay.at[rows], hop_send.at[half]).wait()
    exchange_wait(norm_buf, ex_recv.at[EX_GRAD])
    grad_norm = jnp.sqrt(jnp.sum(gathered(norm_buf), axis=1, keepdims=True))
    clip = jnp.minimum(1.0, MAX_NORM / grad_norm)

    grad_one = (1.0 - BETA_ONE) * clip
    grad_two = (1.0 - BETA_TWO) ** 0.5 * clip

    def adam(start, stop):
        @pl.loop(start, stop)
        def _(group):
            rows = pl.ds(pl.multiple_of(group * 8, 8), 8)
            total = jnp.zeros((8, 128), F32)
            for i in range(COLS // ADAM_PIECE):
                cols = pl.ds(i * ADAM_PIECE, ADAM_PIECE)
                mean = grad[rows, cols]
                new_one = one[rows, cols] + grad_one * mean
                scaled = grad_two * mean
                new_two = two[rows, cols] + scaled * scaled
                one[rows, cols] = new_one
                two[rows, cols] = new_two
                direction = new_one / (jnp.sqrt(new_two) * (CORR_ONE / CORR_TWO ** 0.5) + CORR_ONE * EPSILON) + WEIGHT_DECAY * master[rows, cols]
                relay[rows, cols] = direction
                total = total + fold_lanes(direction * direction)
            part_buf[group] = total

    def row_sums(start, stop, place):
        tile = jnp.zeros((8, 128), F32)
        for group in range(start, stop):
            tile = jnp.where(lane == place(group), jnp.sum(part_buf[group], axis=1, keepdims=True), tile)
        return tile

    groups = [(start // 8, stop // 8) for start, stop in NORM_CHUNKS]

    def step_rates(weight_norm, number):
        if number == 0:
            exchange_wait(first_buf, ex_recv.at[EX_FIRST])
            total = first_totals(gathered(first_buf))
        else:
            exchange_wait(sq_buf.at[number - 1], ex_recv.at[EX_FIRST + number])
            total = packed_totals(gathered(sq_buf.at[number - 1]), *groups[number])
        return weight_norm / jnp.sqrt(total) * LEARN_RATE

    def ag_rows(chunk):
        return pl.ds(AG_STARTS[chunk], AG_SIZES[chunk])

    def update(number, rates):
        start, stop = NORM_CHUNKS[number]
        for chunk in range(AG_CHUNKS):
            if not start <= AG_STARTS[chunk] < stop:
                continue

            @pl.loop(0, AG_SIZES[chunk] // 16)
            def _(tile):
                group = AG_STARTS[chunk] // 8 + 2 * tile
                rows = pl.ds(pl.multiple_of(AG_STARTS[chunk] + tile * 16, 16), 16)
                rate = jnp.concatenate([jnp.sum(jnp.where(lane == group + i, rates, 0.0), axis=1, keepdims=True) for i in range(2)], axis=0)

                @pl.loop(0, PIECES)
                def _(i):
                    cols = pl.ds(pl.multiple_of(i * PIECE, PIECE), PIECE)
                    value = master[rows, cols] - rate * relay[rows, cols]
                    master[rows, cols] = value
                    params[rows, pl.ds(pl.multiple_of(me * COLS + i * PIECE, PIECE), PIECE)] = value.astype(BF16)

            rows = ag_rows(chunk)
            own = params.at[rows, block(me)]
            remote(own, own, ag_send.at[0], ag_x.at[chunk], near_x).start()
            remote(own, own, ag_send.at[1], ag_y.at[chunk], near_y).start()
            remote(own, own, ag_send.at[2], ag_o, other).start()

    adam(*groups[0])
    first_buf[linear] = jnp.sum(row_sums(*groups[0], lambda group: 8 * group + sub), axis=0, keepdims=True)
    adam(groups[1][0], groups[1][0] + 1)
    exchange(first_buf, EX_FIRST)
    adam(groups[1][0] + 1, groups[1][1])
    sq_buf[0, linear] = packed(row_sums(*groups[1], lambda group: 32 * (sub % 4) + group - groups[1][0]))
    adam(groups[2][0], groups[2][0] + 1)
    exchange(sq_buf.at[0], EX_FIRST + 1)
    exchange_wait(weight_buf, ex_recv.at[EX_WEIGHT])
    weights = gathered(weight_buf)
    weight_norm = jnp.sqrt(packed_totals(weights[0:2], 0, GROUPS // 2) + packed_totals(weights[2:4], GROUPS // 2, GROUPS))
    update(0, step_rates(weight_norm, 0))
    adam(groups[2][0] + 1, groups[2][1])
    sq_buf[1, linear] = packed(row_sums(*groups[2], lambda group: 32 * (sub % 4) + group - groups[2][0]))
    rates = step_rates(weight_norm, 1)
    exchange(sq_buf.at[1], EX_FIRST + 2)
    update(1, rates)
    update(2, step_rates(weight_norm, 2))

    def arrived(sem, source, rows):
        view = params.at[rows, block(source)]
        pltpu.make_async_copy(view, view, sem).wait()
        return view

    for chunk in range(AG_CHUNKS):
        rows = ag_rows(chunk)
        view = arrived(ag_x.at[chunk], near_x, rows)
        if AG_FAR_BY_Y[chunk]:
            remote(view, view, ag_send.at[1], ag_d.at[chunk], near_y).start()
        remote(view, view, ag_send.at[2], ag_o, other).start()
        view = arrived(ag_y.at[chunk], near_y, rows)
        if not AG_FAR_BY_Y[chunk]:
            remote(view, view, ag_send.at[0], ag_d.at[chunk], near_x).start()
        remote(view, view, ag_send.at[2], ag_o, other).start()

    for chunk in range(AG_CHUNKS):
        view = arrived(ag_d.at[chunk], diag, ag_rows(chunk))
        remote(view, view, ag_send.at[2], ag_o, other).start()

    half_cols = params.at[:, pl.ds(0, DATA // 2 * COLS)]
    pltpu.make_async_copy(half_cols, half_cols, ag_o).wait()
    pltpu.make_async_copy(half_cols, half_cols, ag_send.at[2]).wait()
    for direction in range(2):
        for part in (pl.ds(0, ROWS), pl.ds(0, HALF)):
            view = params.at[part, pl.ds(0, COLS)]
            pltpu.make_async_copy(view, view, ag_send.at[direction]).wait()
    for half in range(2):
        view = params.at[pl.ds(0, HALF), pl.ds(0, 6 * COLS)]
        pltpu.make_async_copy(view, view, rs_send.at[half]).wait()
    exchange_wait(weight_buf, ex_send.at[EX_WEIGHT])
    exchange_wait(norm_buf, ex_send.at[EX_GRAD])
    exchange_wait(first_buf, ex_send.at[EX_FIRST])
    for number in range(2):
        exchange_wait(sq_buf.at[number], ex_send.at[EX_FIRST + 1 + number])


def write_out(*refs):
    count = len(refs) // 2
    sem = refs[-1]
    copies = []
    for part in range(OUT_PARTS):
        rows = pl.ds(part * (ROWS // OUT_PARTS), ROWS // OUT_PARTS)
        for source, target in zip(refs[:count], refs[count:-1]):
            copies.append(pltpu.make_async_copy(source.at[rows], target.at[rows], sem.at[len(copies)]))
    for number, copy in enumerate(copies):
        copy.start(priority=number % 2)
    for copy in copies:
        copy.wait()


def solution(mesh):
    def device_step(local_grads, master, moment_one, moment_two):
        any_spec = pl.BlockSpec(memory_space=pl.ANY)
        vmem_spec = pl.BlockSpec(memory_space=pltpu.VMEM)
        state = pltpu.VMEM((ROWS, COLS), F32)
        dma = pltpu.SemaphoreType.DMA
        results = pl.pallas_call(
            kernel,
            name="lamb",
            out_shape=(pltpu.VMEM((ROWS, DATA * COLS), BF16), state, state, state),
            in_specs=[any_spec] * 4,
            out_specs=[vmem_spec] * 4,
            scratch_shapes=[
                pltpu.VMEM((ROWS, COLS), F32),
                pltpu.VMEM((ROWS, COLS), F32),
                pltpu.VMEM((DEVICES, 4, 128), F32),
                pltpu.VMEM((DEVICES, 1, 128), F32),
                pltpu.VMEM((DEVICES, 1, 128), F32),
                pltpu.VMEM((2, DEVICES, 2, 128), F32),
                pltpu.VMEM((ROWS // 8, 8, 128), F32),
                dma((3,)),
                dma((2, RS_CHUNKS)),
                dma((2,)),
                dma((2, RS_CHUNKS)),
                dma((2,)),
                dma((5,)),
                dma((5,)),
                dma((AG_CHUNKS,)),
                dma((AG_CHUNKS,)),
                dma((AG_CHUNKS,)),
                dma,
                dma((3,)),
                pltpu.SemaphoreType.REGULAR,
            ],
            compiler_params=pltpu.CompilerParams(collective_id=0, has_side_effects=True, vmem_limit_bytes=VMEM_LIMIT),
        )(local_grads, master, moment_one, moment_two)
        results = [pltpu.with_memory_space_constraint(value, pltpu.VMEM) for value in results]
        return tuple(pl.pallas_call(
            write_out,
            name="write_out",
            out_shape=[jax.ShapeDtypeStruct(value.shape, value.dtype) for value in results],
            in_specs=[vmem_spec] * 4,
            out_specs=[any_spec] * 4,
            scratch_shapes=[dma((4 * OUT_PARTS,))],
            compiler_params=pltpu.CompilerParams(vmem_limit_bytes=VMEM_LIMIT),
        )(*results))

    state_spec = P(None, ('model', 'data'))
    return jax.shard_map(device_step, mesh=mesh, in_specs=(P('data', None, 'model'), state_spec, state_spec, state_spec), out_specs=(P(None, 'model'), state_spec, state_spec, state_spec), check_vma=False)
```
